128 devices in a mesh: seq: 16 (over x, z), head: 8 (over y, core).
Axes of the slice: x: 4, y: 4, z: 4, core: 2. Of those that a mesh axis runs over, the one named last changes fastest.
Arguments:
- latent: float32 [4096, 128], P('seq'), may hold values from -6 to 6
- w_in: bfloat16 [128, 3072], replicated, may hold values from -0.5 to 0.5
- w_query: bfloat16 [3072, 3072], P(None, 'head'), may hold values from -0.109375 to 0.109375
- w_key: bfloat16 [3072, 3072], P(None, 'head'), may hold values from -0.109375 to 0.109375
- w_value: bfloat16 [3072, 3072], P(None, 'head'), may hold values from -0.109375 to 0.109375
- w_attn_out: bfloat16 [3072, 3072], P('head'), may hold values from -0.109375 to 0.109375
- w_up: bfloat16 [3072, 12288], P('seq', 'head'), may hold values from -0.109375 to 0.109375
- w_down: bfloat16 [12288, 3072], P('head', 'seq'), may hold values from -0.0546875 to 0.0546875
- w_final: bfloat16 [3072, 256], replicated, may hold values from -0.109375 to 0.109375
- gain_attn: float32 [3072], replicated, may hold values from 0.5 to 1.5
- gain_mlp: float32 [3072], replicated, may hold values from 0.5 to 1.5
- gain_final: float32 [3072], replicated, may hold values from 0.5 to 1.5
Outputs:
- restored: float32 [4096, 128], P('seq')
The draws below stay inside these ranges and needn't reach their ends.
All inputs are finite; a program needn't handle non-finite values.
Results may differ from the reference program's by a relative error of at most 0.013.
Values may be sent and summed in bfloat16 or wider, within the bound.
A program may use at most 192 MiB of HBM per device.

```python
import jax
import jax.numpy as jnp
from jax import lax

D = 3072
HEADS = 24
HEAD_DIM = 128
FF = 12288
C = 128
ITERS = 2
LENGTH = 4096
N_HEAD = 8


def shard_levels(own_key, dims, pieces, low, top_value):
    level, own = 1.0, jax.random.fold_in(own_key, 6)
    for dim, parts in pieces:
        draws = jnp.exp(jax.random.uniform(jax.random.fold_in(own, dim), (parts,), jnp.float32, low / len(pieces), top_value / len(pieces)))
        level = level * jnp.repeat(draws, dims[dim] // parts).reshape([-1 if axis == dim else 1 for axis in range(len(dims))])
    return level


def bell_draw(stream_key, shape, deviation, limit, shards=(), dtype=jnp.bfloat16):
    result = jax.random.normal(stream_key, shape, jnp.float32) * deviation
    if len(shards) > 0:
        result = shard_levels(stream_key, shape, shards, -0.22, 0.18) * result
    return jnp.clip(result, min=-limit, max=limit).astype(dtype)


def setup_inputs(seed: int = 0) -> dict:
    seeds = jax.random.split(jax.random.key(seed), 13)
    latent = bell_draw(seeds[0], (LENGTH, C), 1.0, 6.0, ((0, 16),), jnp.float32)
    w_in = bell_draw(seeds[1], (C, D), C ** -0.5, 0.5)
    w_query = bell_draw(seeds[2], (D, HEADS * HEAD_DIM), D ** -0.5, 0.109375, ((1, 8),))
    w_key = bell_draw(seeds[3], (D, HEADS * HEAD_DIM), D ** -0.5, 0.109375, ((1, 8),))
    w_value = bell_draw(seeds[4], (D, HEADS * HEAD_DIM), D ** -0.5, 0.109375, ((1, 8),))
    w_attn_out = bell_draw(seeds[5], (HEADS * HEAD_DIM, D), (HEADS * HEAD_DIM) ** -0.5, 0.109375, ((0, 8),))
    w_up = bell_draw(seeds[6], (D, FF), D ** -0.5, 0.109375, ((0, 16), (1, 8)))
    w_down = bell_draw(seeds[7], (FF, D), FF ** -0.5, 0.0546875, ((0, 8), (1, 16)))
    w_final = bell_draw(seeds[8], (D, 2 * C), D ** -0.5, 0.109375)
    gain_attn = jnp.clip(1.0 + 0.1 * jax.random.normal(seeds[9], (D,), jnp.float32), 0.5, 1.5)
    gain_mlp = jnp.clip(1.0 + 0.1 * jax.random.normal(seeds[10], (D,), jnp.float32), 0.5, 1.5)
    gain_final = jnp.clip(1.0 + 0.1 * jax.random.normal(seeds[11], (D,), jnp.float32), 0.5, 1.5)
    return dict(latent=latent, w_in=w_in, w_query=w_query, w_key=w_key, w_value=w_value, w_attn_out=w_attn_out, w_up=w_up, w_down=w_down, w_final=w_final, gain_attn=gain_attn, gain_mlp=gain_mlp, gain_final=gain_final)


EPSILON = 1e-05

def layer_norm(stream, gain):
    center = stream - lax.optimization_barrier(jnp.mean(stream, axis=-1, keepdims=True))
    spread = lax.optimization_barrier(jnp.mean(center * center, axis=-1, keepdims=True))
    return center * lax.rsqrt(spread + EPSILON) * gain

def sinusoid(positions, model_width):
    pair_count = model_width // 2
    frequency = jnp.exp(-jnp.log(10000.0) * 2.0 * jnp.arange(pair_count).astype(jnp.float32) / model_width)
    angles = positions[:, None] * frequency[None, :]
    return jnp.concatenate([jnp.sin(angles), jnp.cos(angles)], axis=1)

def causal_attention(queries, key_rows, value_rows):
    length = queries.shape[0]
    query_heads = queries.astype(jnp.float32).reshape(length, HEADS, HEAD_DIM).transpose(1, 0, 2)
    key_heads = key_rows.astype(jnp.float32).reshape(length, HEADS, HEAD_DIM).transpose(1, 0, 2)
    value_heads = value_rows.reshape(length, HEADS, HEAD_DIM).transpose(1, 0, 2)
    visible = jnp.arange(length)[None, :] <= jnp.arange(length)[:, None]

    def one_head(operands):
        query_head, key_head, value_head = operands
        scores = jnp.dot(query_head, key_head.T, precision=lax.Precision.HIGHEST)
        weights_now = jnp.where(visible, jnp.exp(jnp.where(visible, scores, 0.0)), 0.0)
        totals = lax.optimization_barrier(jnp.sum(weights_now, axis=-1, keepdims=True))
        probs = weights_now.astype(jnp.bfloat16)
        return jnp.dot(probs, value_head, preferred_element_type=jnp.float32) / totals
    outputs = lax.map(one_head, (query_heads, key_heads, value_heads))
    return outputs.transpose(1, 0, 2).reshape(length, HEADS * HEAD_DIM).astype(jnp.bfloat16)

def grouped_sum(left, right):
    group_width = left.shape[1] // N_HEAD
    total = jnp.zeros((left.shape[0], right.shape[1]), jnp.float32)
    for group_index in range(N_HEAD):
        lower = group_index * group_width
        upper = lower + group_width
        partial_term = jnp.dot(left[:, lower:upper], right[lower:upper], preferred_element_type=jnp.float32)
        total = total + lax.optimization_barrier(partial_term.astype(jnp.bfloat16)).astype(jnp.float32)
    return total

def reference(latent, w_in, w_query, w_key, w_value, w_attn_out, w_up, w_down, w_final, gain_attn, gain_mlp, gain_final):
    length = latent.shape[0]
    positions = jnp.arange(length).astype(jnp.float32)
    embedding = sinusoid(positions, D)
    current = latent
    for step_index in range(ITERS):
        stream_in = jnp.dot(current.astype(jnp.bfloat16), w_in, preferred_element_type=jnp.float32) + embedding
        normed = layer_norm(stream_in, gain_attn).astype(jnp.bfloat16)
        queries = (jnp.dot(normed, w_query, preferred_element_type=jnp.float32) * HEAD_DIM ** (-0.5)).astype(jnp.bfloat16)
        key_rows = jnp.dot(normed, w_key, preferred_element_type=jnp.float32).astype(jnp.bfloat16)
        value_rows = jnp.dot(normed, w_value, preferred_element_type=jnp.float32).astype(jnp.bfloat16)
        attended = causal_attention(queries, key_rows, value_rows)
        stream_attn = stream_in + grouped_sum(attended, w_attn_out)
        normed_mlp = layer_norm(stream_attn, gain_mlp).astype(jnp.bfloat16)
        hidden = jax.nn.gelu(jnp.dot(normed_mlp, w_up, preferred_element_type=jnp.float32), approximate=True).astype(jnp.bfloat16)
        stream_mlp = stream_attn + grouped_sum(hidden, w_down)
        final_normed = layer_norm(stream_mlp, gain_final).astype(jnp.bfloat16)
        params_out = jnp.dot(final_normed, w_final, preferred_element_type=jnp.float32)
        shifted = jnp.concatenate([jnp.zeros((1, params_out.shape[1]), jnp.float32), params_out[:-1]], axis=0)
        current = latent * jnp.exp(jnp.tanh(shifted[:, C:])) + shifted[:, :C]
    return current[::-1]
```

```python
import functools

import jax
import jax.numpy as jnp
from jax import lax
from jax.experimental import pallas as pl
from jax.experimental.pallas import tpu as pltpu
from jax.sharding import PartitionSpec as P

D = 3072
HALF = D // 2
HEAD_DIM = 128
C = 128
ITERS = 2
EPSILON = 1e-05
KEY_BLOCK = 512
BF16 = jnp.bfloat16
F32 = jnp.float32


def split_two(value):
    high = lax.reduce_precision(value, 8, 7)
    return high.astype(BF16), (value - high).astype(BF16)


def dot(left, right):
    return jnp.dot(left, right, preferred_element_type=F32)


def dot_t(left, right):
    return lax.dot_general(left, right, (((1,), (1,)), ((), ())), preferred_element_type=F32)


def layer_norm(stream, gain):
    center = stream - jnp.mean(stream, axis=-1, keepdims=True)
    spread = jnp.mean(center * center, axis=-1, keepdims=True)
    return center * lax.rsqrt(spread + EPSILON) * gain


def frequencies():
    return jnp.exp(-jnp.log(10000.0) * 2.0 * jnp.arange(HALF).astype(F32) / D)


def embed_kernel(
    rows, turn_ref, base_ref, gain_ref, wq_ref, wk_ref, wv_ref, win_ref, gw_ref, ws_ref,
    ek_ref, ev_ref, h_ref, n_ref, eq_ref, scaled, high, low,
):
    block = pl.program_id(0)
    me = lax.axis_index("seq")
    total = jnp.zeros((rows, 1), F32)
    width = 512
    for at in range(0, HALF, width):
        cols = slice(at, at + width)
        sin_a, cos_a = turn_ref[0, 0:1, cols], turn_ref[0, 1:2, cols]
        sin_b, cos_b = base_ref[0, :, cols], base_ref[1, :, cols]
        for part, offset in (
            (sin_a * cos_b + cos_a * sin_b, 0),
            (cos_a * cos_b - sin_a * sin_b, HALF),
        ):
            into = slice(offset + at, offset + at + width)
            top = part.astype(BF16)
            high[:, into] = top
            low[:, into] = (part - top.astype(F32)).astype(BF16)
            scaled[:, into] = (part * gain_ref[:, into]).astype(BF16)
            total = total + jnp.sum(part, axis=1, keepdims=True)
    mean = total * (1.0 / D)
    ek_ref[...] = dot(scaled[...], wk_ref[...]) - mean * gw_ref[1:2, :]
    ev_ref[...] = dot(scaled[...], wv_ref[...]) - mean * gw_ref[2:3, :]
    h_ref[...] = dot_t(high[...], win_ref[...]) + dot_t(low[...], win_ref[...]) - mean * ws_ref[...]
    n_ref[...] = HALF - D * mean * mean

    @pl.when(block == me)
    def _():
        eq_ref[...] = dot(scaled[...], wq_ref[...]) - mean * gw_ref[0:1, :]


def embed_all(rows, blocks, gain, w_query, w_key, w_value, w_in, gw, w_sum):
    freq = frequencies()
    turn = (jnp.arange(blocks, dtype=F32) * rows)[:, None] * freq[None, :]
    turn = jnp.stack([jnp.sin(turn), jnp.cos(turn)], axis=1)
    base = jnp.arange(rows, dtype=F32)[:, None] * freq[None, :]
    base = jnp.stack([jnp.sin(base), jnp.cos(base)], axis=0)
    width = w_key.shape[1]
    whole = pl.BlockSpec(memory_space=pltpu.VMEM)
    length = rows * blocks
    return pl.pallas_call(
        functools.partial(embed_kernel, rows),
        grid=(blocks,),
        in_specs=[pl.BlockSpec((1, 2, HALF), lambda i: (i, 0, 0))] + [whole] * 8,
        out_specs=[
            pl.BlockSpec((rows, width), lambda i: (i, 0)),
            pl.BlockSpec((rows, width), lambda i: (i, 0)),
            pl.BlockSpec((rows, C), lambda i: (i, 0)),
            pl.BlockSpec((rows, 1), lambda i: (i, 0)),
            pl.BlockSpec((rows, width), lambda i: (0, 0)),
        ],
        out_shape=[
            jax.ShapeDtypeStruct((length, width), F32),
            jax.ShapeDtypeStruct((length, width), F32),
            jax.ShapeDtypeStruct((length, C), F32),
            jax.ShapeDtypeStruct((length, 1), F32),
            jax.ShapeDtypeStruct((rows, width), F32),
        ],
        scratch_shapes=[pltpu.VMEM((rows, D), BF16)] * 3,
        compiler_params=pltpu.CompilerParams(vmem_limit_bytes=48 << 20),
        cost_estimate=pl.CostEstimate(
            flops=2 * length * D * (2 * width + 2 * C),
            bytes_accessed=4 * length * 2 * width,
            transcendentals=0,
        ),
        name="embed_all",
    )(turn, base, gain, w_query, w_key, w_value, w_in, gw, w_sum)


def attend_kernel(
    rows, heads, x_ref, ek_ref, ev_ref, h_ref, n_ref, eq_ref, aq_ref, ak_ref, av_ref, g_ref,
    out_ref, queries, acc, sums,
):
    block = pl.program_id(0)
    me = lax.axis_index("seq")

    def scale_of(x, h, n):
        twice = jnp.concatenate([x, x], axis=1)
        quad = jnp.sum(x.astype(F32) * (dot(twice, g_ref[...]) + 2.0 * h), axis=1, keepdims=True)
        return twice, lax.rsqrt(jnp.maximum(quad + n, 0.0) * (1.0 / D) + EPSILON)

    @pl.when(block == 0)
    def _():
        own = pl.ds(pl.multiple_of(me * rows, rows), rows)
        twice, scale = scale_of(x_ref[own, :], h_ref[own, :], n_ref[own, :])
        value = (dot(twice, aq_ref[...]) + eq_ref[...]) * (scale * HEAD_DIM**-0.5)
        queries[...] = value.astype(BF16)
        acc[...] = jnp.zeros_like(acc)
        sums[...] = jnp.zeros_like(sums)

    def step(masked):
        here = pl.ds(pl.multiple_of(block * KEY_BLOCK, KEY_BLOCK), KEY_BLOCK)
        twice, scale = scale_of(x_ref[here, :], h_ref[here, :], n_ref[here, :])
        keys = ((dot(twice, ak_ref[...]) + ek_ref[...]) * scale).astype(BF16)
        values = ((dot(twice, av_ref[...]) + ev_ref[...]) * scale).astype(BF16)
        if masked:
            shape = (rows, KEY_BLOCK)
            row = me * rows + lax.broadcasted_iota(jnp.int32, shape, 0)
            col = block * KEY_BLOCK + lax.broadcasted_iota(jnp.int32, shape, 1)
            seen = col <= row
        for head in range(heads):
            cols = slice(head * HEAD_DIM, (head + 1) * HEAD_DIM)
            scores = dot_t(queries[:, cols], keys[:, cols])
            if masked:
                weights = jnp.where(seen, jnp.exp(jnp.where(seen, scores, 0.0)), 0.0)
            else:
                weights = jnp.exp(scores)
            part = weights[:, :HEAD_DIM]
            for at in range(HEAD_DIM, KEY_BLOCK, HEAD_DIM):
                part = part + weights[:, at : at + HEAD_DIM]
            sums[:, cols] += part
            acc[:, cols] += dot(weights.astype(BF16), values[:, cols])

    last = (me * rows + rows - 1) // KEY_BLOCK

    @pl.when(block < last)
    def _():
        step(False)

    @pl.when(block == last)
    def _():
        step(True)

    @pl.when(block == pl.num_programs(0) - 1)
    def _():
        for head in range(heads):
            cols = slice(head * HEAD_DIM, (head + 1) * HEAD_DIM)
            total = jnp.sum(sums[:, cols], axis=1, keepdims=True)
            out_ref[:, cols] = (acc[:, cols] / total).astype(BF16)


def attend(rows, x, ek, ev, h, n, eq, aq, ak, av, gram):
    length, width = ek.shape
    heads = width // HEAD_DIM
    whole = pl.BlockSpec(memory_space=pltpu.VMEM)
    tile = pl.BlockSpec((KEY_BLOCK, width), lambda i: (i, 0))
    return pl.pallas_call(
        functools.partial(attend_kernel, rows, heads),
        grid=(length // KEY_BLOCK,),
        in_specs=[whole, tile, tile] + [whole] * 7,
        out_specs=whole,
        out_shape=jax.ShapeDtypeStruct((rows, width), BF16),
        scratch_shapes=[
            pltpu.VMEM((rows, width), BF16),
            pltpu.VMEM((rows, width), F32),
            pltpu.VMEM((rows, width), F32),
        ],
        compiler_params=pltpu.CompilerParams(vmem_limit_bytes=40 << 20),
        cost_estimate=pl.CostEstimate(
            flops=4 * length * rows * width * 2, bytes_accessed=8 * length * width, transcendentals=0
        ),
        name="attend",
    )(x, ek, ev, h, n, eq, aq, ak, av, gram)


def per_device(
    latent, w_in, w_query, w_key, w_value, w_attn_out, w_up, w_down, w_final,
    gain_attn, gain_mlp, gain_final,
):
    seq_count, head_count = lax.axis_size("seq"), lax.axis_size("head")
    me, mine = lax.axis_index("seq"), lax.axis_index("head")
    rows = latent.shape[0]
    share = rows // head_count
    length = rows * seq_count
    first = me * rows + mine * share

    latents = lax.all_gather(latent, "seq", axis=0, tiled=True)
    up_full = lax.all_gather(w_up, "seq", axis=0, tiled=True)
    down_full = lax.all_gather(w_down.T, "seq", axis=0, tiled=True)

    w_wide = w_in.astype(F32)
    center = w_wide - jnp.mean(w_wide, axis=1, keepdims=True)
    gram = lax.dot_general(
        center, center, (((1,), (1,)), ((), ())), precision=lax.Precision.HIGHEST
    )
    gram = jnp.concatenate(split_two(gram), axis=0)
    scaled = jnp.concatenate(split_two(center * gain_attn), axis=0)
    stacks, sums = [], []
    gain_parts = jnp.concatenate(split_two(gain_attn[None, :]), axis=0)
    for weight in (w_query, w_key, w_value):
        both = dot(scaled, weight)
        stacks.append(jnp.concatenate(split_two(both[:C] + both[C:]), axis=0))
        sums.append(jnp.sum(dot(gain_parts, weight), axis=0))
    gw = jnp.stack(sums)
    w_sum = jnp.sum(w_wide, axis=1)[None, :]
    ek, ev, h, n, eq = embed_all(
        rows, seq_count, gain_attn[None, :], w_query, w_key, w_value, w_in, gw, w_sum
    )

    angles = (first + jnp.arange(share)).astype(F32)[:, None] * frequencies()[None, :]
    embedding = jnp.concatenate([jnp.sin(angles), jnp.cos(angles)], axis=1)
    ahead = lax.dynamic_slice_in_dim(
        jnp.concatenate([latents[1:], latents[:1]], axis=0), first, share, 0
    )
    x = latents.astype(BF16)
    for step_index in range(ITERS):
        own = lax.dynamic_slice_in_dim(x, first, share, 0)
        stream_in = dot(own, w_in) + embedding
        attended = attend(rows, x, ek, ev, h, n, eq, *stacks, gram)
        term = dot(attended, w_attn_out).astype(BF16)
        stream_attn = stream_in + lax.psum_scatter(
            term, "head", scatter_dimension=0, tiled=True
        ).astype(F32)
        normed = layer_norm(stream_attn, gain_mlp).astype(BF16)
        normed = lax.all_gather(normed, "head", axis=0, tiled=True)
        hidden = jax.nn.gelu(dot(normed, up_full), approximate=True).astype(BF16)
        term = dot_t(hidden, down_full).astype(BF16)
        stream_mlp = stream_attn + lax.psum_scatter(
            term, "head", scatter_dimension=0, tiled=True
        ).astype(F32)
        params = dot(layer_norm(stream_mlp, gain_final).astype(BF16), w_final)
        following = ahead * jnp.exp(jnp.tanh(params[:, C:])) + params[:, :C]
        following = lax.all_gather(following.astype(BF16), ("seq", "head"), axis=0, tiled=True)
        x = jnp.concatenate([latents[:1].astype(BF16), following[:-1]], axis=0)
    mirrored = lax.dynamic_slice_in_dim(x, (seq_count - 1 - me) * rows, rows, 0)
    return mirrored[::-1].astype(F32)


def solution(mesh):
    in_specs = (
        P("seq", None),
        P(),
        P(None, "head"),
        P(None, "head"),
        P(None, "head"),
        P("head", None),
        P("seq", "head"),
        P("head", "seq"),
        P(),
        P(),
        P(),
        P(),
    )
    return jax.shard_map(
        per_device, mesh=mesh, in_specs=in_specs, out_specs=P("seq", None), check_vma=False
    )
```

```python
import functools

import jax
import jax.numpy as jnp
from jax import lax
from jax.experimental import pallas as pl
from jax.experimental.pallas import tpu as pltpu
from jax.sharding import PartitionSpec as P

D = 3072
HALF = D // 2
HEAD_DIM = 128
C = 128
ITERS = 2
EPSILON = 1e-05
KEY_BLOCK = 512
BF16 = jnp.bfloat16
F32 = jnp.float32


def split_two(value):
    high = lax.reduce_precision(value, 8, 7)
    return high.astype(BF16), (value - high).astype(BF16)


def dot(left, right):
    return jnp.dot(left, right, preferred_element_type=F32)


def dot_t(left, right):
    return lax.dot_general(left, right, (((1,), (1,)), ((), ())), preferred_element_type=F32)


def layer_norm(stream, gain):
    center = stream - jnp.mean(stream, axis=-1, keepdims=True)
    spread = jnp.mean(center * center, axis=-1, keepdims=True)
    return center * lax.rsqrt(spread + EPSILON) * gain


def frequencies():
    return jnp.exp(-jnp.log(10000.0) * 2.0 * jnp.arange(HALF).astype(F32) / D)


def embed_kernel(
    rows, turn_ref, base_ref, gain_ref, wq_ref, wk_ref, wv_ref, win_ref, gw_ref, ws_ref,
    ek_ref, ev_ref, h_ref, n_ref, eq_ref, scaled, high, low,
):
    block = pl.program_id(0)
    me = lax.axis_index("seq")
    total = jnp.zeros((rows, 1), F32)
    width = 512
    for at in range(0, HALF, width):
        cols = slice(at, at + width)
        sin_a, cos_a = turn_ref[0, 0:1, cols], turn_ref[0, 1:2, cols]
        sin_b, cos_b = base_ref[0, :, cols], base_ref[1, :, cols]
        for part, offset in (
            (sin_a * cos_b + cos_a * sin_b, 0),
            (cos_a * cos_b - sin_a * sin_b, HALF),
        ):
            into = slice(offset + at, offset + at + width)
            top = part.astype(BF16)
            high[:, into] = top
            low[:, into] = (part - top.astype(F32)).astype(BF16)
            scaled[:, into] = (part * gain_ref[:, into]).astype(BF16)
            total = total + jnp.sum(part, axis=1, keepdims=True)
    mean = total * (1.0 / D)
    ek_ref[...] = dot(scaled[...], wk_ref[...]) - mean * gw_ref[1:2, :]
    ev_ref[...] = dot(scaled[...], wv_ref[...]) - mean * gw_ref[2:3, :]
    h_ref[...] = dot_t(high[...], win_ref[...]) + dot_t(low[...], win_ref[...]) - mean * ws_ref[...]
    n_ref[...] = HALF - D * mean * mean

    @pl.when(block == me)
    def _():
        eq_ref[...] = dot(scaled[...], wq_ref[...]) - mean * gw_ref[0:1, :]


def embed_all(rows, blocks, gain, w_query, w_key, w_value, w_in, gw, w_sum):
    freq = frequencies()
    turn = (jnp.arange(blocks, dtype=F32) * rows)[:, None] * freq[None, :]
    turn = jnp.stack([jnp.sin(turn), jnp.cos(turn)], axis=1)
    base = jnp.arange(rows, dtype=F32)[:, None] * freq[None, :]
    base = jnp.stack([jnp.sin(base), jnp.cos(base)], axis=0)
    width = w_key.shape[1]
    whole = pl.BlockSpec(memory_space=pltpu.VMEM)
    length = rows * blocks
    return pl.pallas_call(
        functools.partial(embed_kernel, rows),
        grid=(blocks,),
        in_specs=[pl.BlockSpec((1, 2, HALF), lambda i: (i, 0, 0))] + [whole] * 8,
        out_specs=[
            pl.BlockSpec((rows, width), lambda i: (i, 0)),
            pl.BlockSpec((rows, width), lambda i: (i, 0)),
            pl.BlockSpec((rows, C), lambda i: (i, 0)),
            pl.BlockSpec((rows, 1), lambda i: (i, 0)),
            pl.BlockSpec((rows, width), lambda i: (0, 0)),
        ],
        out_shape=[
            jax.ShapeDtypeStruct((length, width), F32),
            jax.ShapeDtypeStruct((length, width), F32),
            jax.ShapeDtypeStruct((length, C), F32),
            jax.ShapeDtypeStruct((length, 1), F32),
            jax.ShapeDtypeStruct((rows, width), F32),
        ],
        scratch_shapes=[pltpu.VMEM((rows, D), BF16)] * 3,
        compiler_params=pltpu.CompilerParams(vmem_limit_bytes=48 << 20),
        cost_estimate=pl.CostEstimate(
            flops=2 * length * D * (2 * width + 2 * C),
            bytes_accessed=4 * length * 2 * width,
            transcendentals=0,
        ),
        name="embed_all",
    )(turn, base, gain, w_query, w_key, w_value, w_in, gw, w_sum)


def attend_kernel(
    rows, heads, x_ref, ek_ref, ev_ref, h_ref, n_ref, eq_ref, aq_ref, ak_ref, av_ref, g_ref,
    out_ref, queries, acc, sums,
):
    block = pl.program_id(0)
    me = lax.axis_index("seq")

    def scale_of(x, h, n):
        twice = jnp.concatenate([x, x], axis=1)
        quad = jnp.sum(x.astype(F32) * (dot(twice, g_ref[...]) + 2.0 * h), axis=1, keepdims=True)
        return twice, lax.rsqrt(jnp.maximum(quad + n, 0.0) * (1.0 / D) + EPSILON)

    @pl.when(block == 0)
    def _():
        own = pl.ds(pl.multiple_of(me * rows, rows), rows)
        twice, scale = scale_of(x_ref[own, :], h_ref[own, :], n_ref[own, :])
        value = (dot(twice, aq_ref[...]) + eq_ref[...]) * (scale * HEAD_DIM**-0.5)
        queries[...] = value.astype(BF16)
        acc[...] = jnp.zeros_like(acc)
        sums[...] = jnp.zeros_like(sums)

    def step(masked):
        here = pl.ds(pl.multiple_of(block * KEY_BLOCK, KEY_BLOCK), KEY_BLOCK)
        twice, scale = scale_of(x_ref[here, :], h_ref[here, :], n_ref[here, :])
        keys = ((dot(twice, ak_ref[...]) + ek_ref[...]) * scale).astype(BF16)
        values = ((dot(twice, av_ref[...]) + ev_ref[...]) * scale).astype(BF16)
        if masked:
            shape = (rows, KEY_BLOCK)
            row = me * rows + lax.broadcasted_iota(jnp.int32, shape, 0)
            col = block * KEY_BLOCK + lax.broadcasted_iota(jnp.int32, shape, 1)
            seen = col <= row
        for head in range(heads):
            cols = slice(head * HEAD_DIM, (head + 1) * HEAD_DIM)
            scores = dot_t(queries[:, cols], keys[:, cols])
            if masked:
                weights = jnp.where(seen, jnp.exp(jnp.where(seen, scores, 0.0)), 0.0)
            else:
                weights = jnp.exp(scores)
            part = weights[:, :HEAD_DIM]
            for at in range(HEAD_DIM, KEY_BLOCK, HEAD_DIM):
                part = part + weights[:, at : at + HEAD_DIM]
            sums[:, cols] += part
            acc[:, cols] += dot(weights.astype(BF16), values[:, cols])

    last = (me * rows + rows - 1) // KEY_BLOCK

    @pl.when(block < last)
    def _():
        step(False)

    @pl.when(block == last)
    def _():
        step(True)

    @pl.when(block == pl.num_programs(0) - 1)
    def _():
        for head in range(heads):
            cols = slice(head * HEAD_DIM, (head + 1) * HEAD_DIM)
            total = jnp.sum(sums[:, cols], axis=1, keepdims=True)
            out_ref[:, cols] = (acc[:, cols] / total).astype(BF16)


def attend(rows, x, ek, ev, h, n, eq, aq, ak, av, gram):
    length, width = ek.shape
    heads = width // HEAD_DIM
    whole = pl.BlockSpec(memory_space=pltpu.VMEM)
    tile = pl.BlockSpec((KEY_BLOCK, width), lambda i: (i, 0))
    return pl.pallas_call(
        functools.partial(attend_kernel, rows, heads),
        grid=(length // KEY_BLOCK,),
        in_specs=[whole, tile, tile] + [whole] * 7,
        out_specs=whole,
        out_shape=jax.ShapeDtypeStruct((rows, width), BF16),
        scratch_shapes=[
            pltpu.VMEM((rows, width), BF16),
            pltpu.VMEM((rows, width), F32),
            pltpu.VMEM((rows, width), F32),
        ],
        compiler_params=pltpu.CompilerParams(vmem_limit_bytes=40 << 20),
        cost_estimate=pl.CostEstimate(
            flops=4 * length * rows * width * 2, bytes_accessed=8 * length * width, transcendentals=0
        ),
        name="attend",
    )(x, ek, ev, h, n, eq, aq, ak, av, gram)


MESH = pl.DeviceIdType.MESH


def seat():
    head = lax.axis_index("head")
    return lax.axis_index("seq"), lax.div(head, 2), lax.rem(head, 2)


def plus(y, by):
    return lax.rem(y + by, 4)


def greet(targets):
    barrier = pltpu.get_barrier_semaphore()
    for target in targets:
        pl.semaphore_signal(barrier, inc=1, device_id=target, device_id_type=MESH)
    pl.semaphore_wait(barrier, len(targets))


def greet_all(devices):
    seq, y, c = seat()
    place = seq * 4 + y
    barrier = pltpu.get_barrier_semaphore()
    pl.semaphore_signal(barrier, inc=1, device_id={"head": 2 * y + 1 - c}, device_id_type=MESH)

    @pl.loop(1, devices)
    def _(k):
        other = lax.rem(place + k, devices)
        pl.semaphore_signal(
            barrier, inc=1,
            device_id={"seq": lax.div(other, 4), "head": 2 * lax.rem(other, 4) + c},
            device_id_type=MESH,
        )

    pl.semaphore_wait(barrier, devices)


def spread(buffer, send, recv):
    seq, y, c = seat()
    devices = buffer.shape[0]
    place = seq * 4 + y

    @pl.loop(1, devices)
    def _(k):
        other = lax.rem(place + k, devices)
        pltpu.make_async_remote_copy(
            src_ref=buffer.at[place, c], dst_ref=buffer.at[place, c],
            send_sem=send.at[0], recv_sem=recv.at[0],
            device_id={"seq": lax.div(other, 4), "head": 2 * lax.rem(other, 4) + c},
            device_id_type=MESH,
        ).start()

    partner = {"head": 2 * y + 1 - c}
    whole = buffer.at[pl.ds(0, devices - 1), c]
    arrived = pltpu.make_async_remote_copy(
        src_ref=whole, dst_ref=whole, send_sem=send.at[0], recv_sem=recv.at[0],
        device_id=partner, device_id_type=MESH,
    )
    arrived.wait_recv()
    across = pltpu.make_async_remote_copy(
        src_ref=buffer.at[:, c], dst_ref=buffer.at[:, c], send_sem=send.at[1], recv_sem=recv.at[1],
        device_id=partner, device_id_type=MESH,
    )
    across.start()
    arrived.wait_send()
    across.wait()


def reduce_over_head(produce, meanwhile, term, taken, via_out, via_in, near, fin, send, recv):
    _, y, c = seat()
    partner, up, down = 2 * y + 1 - c, 2 * plus(y, 1) + c, 2 * plus(y, 3) + c

    def copy(src, dst, slot, head):
        return pltpu.make_async_remote_copy(
            src_ref=src, dst_ref=dst, send_sem=send.at[slot], recv_sem=recv.at[slot],
            device_id={"head": head}, device_id_type=MESH,
        )

    def pair(half, at):
        return term[half, at, c].astype(F32) + taken[half, at].astype(F32)

    gives = []
    for half in range(2):
        produce(half)
        gives.append(copy(term.at[half, :, 1 - c], taken.at[half], half, partner))
        gives[half].start()
    meanwhile()
    across, ahead, behind = plus(y, 2), plus(y, 1), plus(y, 3)
    gives[0].wait_recv()
    via_out[0] = pair(0, across).astype(BF16)
    via_0 = copy(via_out.at[0], via_in.at[0], 2, up)
    via_0.start()
    near[1, 0] = pair(0, behind).astype(BF16)
    down_0 = copy(near.at[1, 0], fin.at[1, 0], 6, down)
    down_0.start()
    gives[1].wait_recv()
    via_out[1] = pair(1, across).astype(BF16)
    via_1 = copy(via_out.at[1], via_in.at[1], 3, down)
    via_1.start()
    near[0, 1] = pair(1, ahead).astype(BF16)
    up_1 = copy(near.at[0, 1], fin.at[0, 1], 5, up)
    up_1.start()
    via_0.wait_recv()
    near[0, 0] = (pair(0, ahead) + via_in[0].astype(F32)).astype(BF16)
    up_0 = copy(near.at[0, 0], fin.at[0, 0], 4, up)
    up_0.start()
    via_1.wait_recv()
    near[1, 1] = (pair(1, behind) + via_in[1].astype(F32)).astype(BF16)
    down_1 = copy(near.at[1, 1], fin.at[1, 1], 7, down)
    down_1.start()
    sums = [pair(half, y) for half in range(2)]
    down_0.wait_recv()
    up_0.wait_recv()
    first = sums[0] + fin[0, 0].astype(F32) + fin[1, 0].astype(F32)
    up_1.wait_recv()
    down_1.wait_recv()
    second = sums[1] + fin[0, 1].astype(F32) + fin[1, 1].astype(F32)
    for done in (*gives, via_0, via_1, up_0, up_1, down_0, down_1):
        done.wait_send()
    return jnp.concatenate([first, second], axis=1)


def gather_over_head(out, send, recv):
    _, y, c = seat()
    partner, up, down = 2 * y + 1 - c, 2 * plus(y, 1) + c, 2 * plus(y, 3) + c
    across, ahead, behind = plus(y, 2), plus(y, 1), plus(y, 3)
    low, high = pl.ds(0, HALF), pl.ds(HALF, HALF)

    def copy(block, slot, head):
        return pltpu.make_async_remote_copy(
            src_ref=block, dst_ref=block, send_sem=send.at[slot], recv_sem=recv.at[slot],
            device_id={"head": head}, device_id_type=MESH,
        )

    moves = [copy(out.at[y, c], 0, up), copy(out.at[y, c], 1, down), copy(out.at[y, c], 2, partner)]
    for move in moves:
        move.start()

    def then(slot, *following):
        moves[slot].wait_recv()
        for move in following:
            move.start()
            moves.append(move)

    then(0, copy(out.at[behind, c, :, low], 3, up), copy(out.at[behind, c], 4, partner))
    then(1, copy(out.at[ahead, c, :, high], 5, down), copy(out.at[ahead, c], 6, partner))
    then(3, copy(out.at[across, c, :, low], 7, partner))
    then(5, copy(out.at[across, c, :, high], 8, partner))
    for slot in (2, 4, 6, 7, 8):
        moves[slot].wait_recv()
    for move in moves:
        move.wait_send()


def reduce_scratch(share):
    return [
        pltpu.VMEM((2, 4, 2, share, HALF), BF16),
        pltpu.VMEM((2, 4, share, HALF), BF16),
        pltpu.VMEM((2, share, HALF), BF16),
        pltpu.VMEM((2, share, HALF), BF16),
        pltpu.VMEM((2, 2, share, HALF), BF16),
        pltpu.VMEM((2, 2, share, HALF), BF16),
        pltpu.SemaphoreType.DMA((8,)),
        pltpu.SemaphoreType.DMA((8,)),
    ]


def head_neighbours():
    _, y, c = seat()
    return [{"head": 2 * y + 1 - c}, {"head": 2 * plus(y, 1) + c}, {"head": 2 * plus(y, 3) + c}]


def store_terms(term, half, at, share, value):
    for block in range(8):
        rows = value[block * share : (block + 1) * share].astype(BF16)
        term[half, block // 2, block % 2, :, at : at + value.shape[1]] = rows


def mix_kernel(
    share, x_ref, embedding_ref, win_ref, attended_ref, wo_ref, gain_ref, stream_ref, normed_ref,
    *scratch,
):
    *parts, send, recv = scratch
    greet(head_neighbours())
    term = parts[0]

    def produce(half):
        for at in range(0, HALF, 768):
            cols = slice(half * HALF + at, half * HALF + at + 768)
            store_terms(term, half, at, share, dot(attended_ref[...], wo_ref[:, cols]))

    def meanwhile():
        stream_ref[...] = dot(x_ref[...], win_ref[...]) + embedding_ref[...]

    total = reduce_over_head(produce, meanwhile, *parts)
    stream = stream_ref[...] + total
    stream_ref[...] = stream
    _, y, c = seat()
    normed_ref[y, c] = layer_norm(stream, gain_ref[...]).astype(BF16)
    gather_over_head(normed_ref, send, recv)


def mix(share, x, embedding, w_in, attended, w_attn_out, gain):
    whole = pl.BlockSpec(memory_space=pltpu.VMEM)
    return pl.pallas_call(
        functools.partial(mix_kernel, share),
        in_specs=[whole] * 6,
        out_specs=[whole] * 2,
        out_shape=[
            jax.ShapeDtypeStruct((share, D), F32),
            jax.ShapeDtypeStruct((4, 2, share, D), BF16),
        ],
        scratch_shapes=reduce_scratch(share)
        + [pltpu.SemaphoreType.DMA((9,)), pltpu.SemaphoreType.DMA((9,))],
        compiler_params=pltpu.CompilerParams(
            collective_id=1, has_side_effects=True, vmem_limit_bytes=24 << 20
        ),
        cost_estimate=pl.CostEstimate(
            flops=20_000_000_000, bytes_accessed=10_000_000, transcendentals=0
        ),
        name="mix",
    )(x, embedding, w_in, attended, w_attn_out, gain)


def mlp_kernel(
    share, last, normed_ref, both_ref, stream_ref, gain_ref, wf_ref, ahead_ref, out_ref,
    up, down, hidden, loads, *scratch,
):
    *parts, send, recv = scratch
    term = parts[0]
    seq, y, c = seat()
    ups, downs = up.shape[0], down.shape[0]
    wide, tall = up.shape[2], down.shape[1]
    fetches = [
        pltpu.make_async_copy(both_ref.at[:, pl.ds(k * wide, wide)], up.at[k], loads.at[k])
        for k in range(ups)
    ] + [
        pltpu.make_async_copy(
            both_ref.at[pl.ds(k * tall, tall), pl.ds(ups * wide, ups * wide)],
            down.at[k], loads.at[ups + k],
        )
        for k in range(downs)
    ]
    for fetch in fetches:
        fetch.start()
    if last:
        mirror = lax.axis_size("seq") - 1 - seq
        sends_edge = jnp.logical_and(mirror > 0, 2 * y + c == 7)
        keeps_edge = jnp.logical_and(mirror - 1 == seq, 2 * y + c == 7)
        waits_edge = jnp.logical_and(mirror > 0, jnp.logical_not(keeps_edge))
        barrier = pltpu.get_barrier_semaphore()
        for target in head_neighbours():
            pl.semaphore_signal(barrier, inc=1, device_id=target, device_id_type=MESH)
        for head in range(8):
            pl.semaphore_signal(
                barrier, inc=1, device_id={"seq": mirror, "head": head}, device_id_type=MESH
            )

        @pl.when(waits_edge)
        def _():
            pl.semaphore_signal(
                barrier, inc=1, device_id={"seq": mirror - 1, "head": 7}, device_id_type=MESH
            )

        @pl.when(keeps_edge)
        def _():
            pl.semaphore_wait(barrier, 18)

        @pl.when(jnp.logical_and(sends_edge, jnp.logical_not(keeps_edge)))
        def _():
            pl.semaphore_wait(barrier, 19)

        @pl.when(jnp.logical_not(sends_edge))
        def _():
            pl.semaphore_wait(barrier, 11)

    else:
        greet_all(out_ref.shape[0])

    for k in range(ups):
        fetches[k].wait()
        pre = dot(normed_ref[...], up[k])
        hidden[:, k * wide : (k + 1) * wide] = jax.nn.gelu(pre, approximate=True).astype(BF16)

    def produce(half):
        for at in range(downs // 2):
            k = half * (downs // 2) + at
            fetches[ups + k].wait()
            store_terms(term, half, at * tall, share, dot_t(hidden[...], down[k]))

    total = reduce_over_head(produce, lambda: None, *parts)
    normed = layer_norm(stream_ref[...] + total, gain_ref[...]).astype(BF16)
    params = dot(normed, wf_ref[...])
    following = ahead_ref[...] * jnp.exp(jnp.tanh(params[:, C:])) + params[:, :C]
    if not last:
        out_ref[seq * 4 + y, c] = following.astype(BF16)
        spread(out_ref, send, recv)
    else:
        block = scratch[0].at[0, 0, 0, :, pl.ds(0, C)]
        block[...] = following.astype(BF16)
        head = 2 * y + c
        moves = [
            pltpu.make_async_remote_copy(
                src_ref=block, dst_ref=out_ref.at[head], send_sem=send.at[k], recv_sem=recv.at[0],
                device_id={"seq": mirror, "head": k}, device_id_type=MESH,
            )
            for k in range(8)
        ]
        edges = [
            pltpu.make_async_remote_copy(
                src_ref=block, dst_ref=out_ref.at[8], send_sem=send.at[8 + k], recv_sem=recv.at[1],
                device_id={"seq": mirror - 1, "head": k}, device_id_type=MESH,
            )
            for k in range(8)
        ]
        for move in moves:
            move.start()

        @pl.when(sends_edge)
        def _():
            for move in edges[:7]:
                move.start()

        @pl.when(jnp.logical_and(sends_edge, jnp.logical_not(keeps_edge)))
        def _():
            edges[7].start()

        whole = out_ref.at[pl.ds(0, 8)]
        pltpu.make_async_remote_copy(
            src_ref=whole, dst_ref=whole, send_sem=send.at[0], recv_sem=recv.at[0],
            device_id={"seq": mirror, "head": 0}, device_id_type=MESH,
        ).wait_recv()

        @pl.when(waits_edge)
        def _():
            pltpu.make_async_remote_copy(
                src_ref=block, dst_ref=out_ref.at[8], send_sem=send.at[0], recv_sem=recv.at[1],
                device_id={"seq": mirror - 1, "head": 7}, device_id_type=MESH,
            ).wait_recv()

        for move in moves:
            move.wait_send()

        @pl.when(sends_edge)
        def _():
            for move in edges[:7]:
                move.wait_send()

        @pl.when(jnp.logical_and(sends_edge, jnp.logical_not(keeps_edge)))
        def _():
            edges[7].wait_send()

        @pl.when(jnp.logical_not(waits_edge))
        def _():
            out_ref[8] = following.astype(BF16)


def mlp(share, places, last, normed, both, stream, gain, w_final, ahead):
    whole = pl.BlockSpec(memory_space=pltpu.VMEM)
    rows, width = normed.shape[0], both.shape[1] // 2
    shape = (9, share, C) if last else (places, 2, share, C)
    return pl.pallas_call(
        functools.partial(mlp_kernel, share, last),
        in_specs=[whole, pl.BlockSpec(memory_space=pl.ANY)] + [whole] * 4,
        out_specs=whole,
        out_shape=jax.ShapeDtypeStruct(shape, BF16),
        scratch_shapes=[
            pltpu.VMEM((3, D, width // 3), BF16),
            pltpu.VMEM((4, D // 4, width), BF16),
            pltpu.VMEM((rows, width), BF16),
            pltpu.SemaphoreType.DMA((7,)),
        ]
        + reduce_scratch(share)
        + [pltpu.SemaphoreType.DMA((16,)), pltpu.SemaphoreType.DMA((2,))],
        compiler_params=pltpu.CompilerParams(
            collective_id=3 if last else 2, has_side_effects=True, vmem_limit_bytes=44 << 20
        ),
        cost_estimate=pl.CostEstimate(
            flops=40_000_000_000, bytes_accessed=30_000_000, transcendentals=0
        ),
        name="mlp_last" if last else "mlp",
    )(normed, both, stream, gain, w_final, ahead)


def start_kernel(share, latent_ref, out_ref, edge_ref, rows, send, recv):
    seq, y, c = seat()
    count = lax.axis_size("seq")
    greet_all(out_ref.shape[0])
    rows[...] = latent_ref[0:8, :]
    edge = pltpu.make_async_remote_copy(
        src_ref=rows, dst_ref=edge_ref, send_sem=send.at[2], recv_sem=recv.at[2],
        device_id={"seq": lax.rem(seq + count - 1, count)}, device_id_type=MESH,
    )
    edge.start()
    own = pl.ds(pl.multiple_of((2 * y + c) * share, share), share)
    out_ref[seq * 4 + y, c] = latent_ref[own, :].astype(BF16)
    spread(out_ref, send, recv)
    edge.wait()


def start(share, places, latent):
    whole = pl.BlockSpec(memory_space=pltpu.VMEM)
    return pl.pallas_call(
        functools.partial(start_kernel, share),
        in_specs=[whole],
        out_specs=[whole] * 2,
        out_shape=[
            jax.ShapeDtypeStruct((places, 2, share, C), BF16),
            jax.ShapeDtypeStruct((8, C), F32),
        ],
        scratch_shapes=[
            pltpu.VMEM((8, C), F32),
            pltpu.SemaphoreType.DMA((3,)),
            pltpu.SemaphoreType.DMA((3,)),
        ],
        compiler_params=pltpu.CompilerParams(collective_id=0, has_side_effects=True),
        cost_estimate=pl.CostEstimate(flops=10_000_000_000, bytes_accessed=2_000_000, transcendentals=0),
        name="start",
    )(latent)


def per_device(
    latent, w_in, w_query, w_key, w_value, w_attn_out, w_up, w_down, w_final,
    gain_attn, gain_mlp, gain_final,
):
    seq_count, head_count = lax.axis_size("seq"), lax.axis_size("head")
    me, mine = lax.axis_index("seq"), lax.axis_index("head")
    rows = latent.shape[0]
    share = rows // head_count
    length = rows * seq_count
    places = seq_count * head_count // 2
    first = me * rows + mine * share

    both = lax.all_gather(jnp.concatenate([w_up, w_down.T], axis=1), "seq", axis=0, tiled=True)
    gathered, edge = start(share, places, latent)
    x = gathered.reshape(length, C)

    w_wide = w_in.astype(F32)
    center = w_wide - jnp.mean(w_wide, axis=1, keepdims=True)
    gram = lax.dot_general(
        center, center, (((1,), (1,)), ((), ())), precision=lax.Precision.HIGHEST
    )
    gram = jnp.concatenate(split_two(gram), axis=0)
    scaled = jnp.concatenate(split_two(center * gain_attn), axis=0)
    stacks, sums = [], []
    gain_parts = jnp.concatenate(split_two(gain_attn[None, :]), axis=0)
    for weight in (w_query, w_key, w_value):
        product = dot(scaled, weight)
        stacks.append(jnp.concatenate(split_two(product[:C] + product[C:]), axis=0))
        sums.append(jnp.sum(dot(gain_parts, weight), axis=0))
    gw = jnp.stack(sums)
    w_sum = jnp.sum(w_wide, axis=1)[None, :]
    ek, ev, h, n, eq = embed_all(
        rows, seq_count, gain_attn[None, :], w_query, w_key, w_value, w_in, gw, w_sum
    )

    angles = (first + jnp.arange(share)).astype(F32)[:, None] * frequencies()[None, :]
    embedding = jnp.concatenate([jnp.sin(angles), jnp.cos(angles)], axis=1)
    ahead = lax.dynamic_slice_in_dim(
        jnp.concatenate([latent[1:], edge[:1]], axis=0), mine * share, share, 0
    )
    top = x[:1]
    for step_index in range(ITERS):
        own = lax.dynamic_slice_in_dim(x, first, share, 0)
        attended = attend(rows, x, ek, ev, h, n, eq, *stacks, gram)
        stream, normed = mix(
            share, own, embedding, w_in, attended, w_attn_out, gain_mlp[None, :]
        )
        last = step_index == ITERS - 1
        following = mlp(
            share, places, last, normed.reshape(rows, D), both, stream, gain_final[None, :],
            w_final, ahead,
        )
        if not last:
            x = jnp.concatenate([top, following.reshape(length, C)[:-1]], axis=0)
    edge = jnp.where(me == seq_count - 1, top, following[8, share - 1 :])
    result = jnp.concatenate([edge, following[:8].reshape(rows, C)[:-1]], axis=0)
    return result[::-1].astype(F32)


def solution(mesh):
    in_specs = (
        P("seq", None),
        P(),
        P(None, "head"),
        P(None, "head"),
        P(None, "head"),
        P("head", None),
        P("seq", "head"),
        P("head", "seq"),
        P(),
        P(),
        P(),
        P(),
    )
    return jax.shard_map(
        per_device, mesh=mesh, in_specs=in_specs, out_specs=P("seq", None), check_vma=False
    )
```

```python
import functools

import jax
import jax.numpy as jnp
from jax import lax
from jax.experimental import pallas as pl
from jax.experimental.pallas import tpu as pltpu
from jax.sharding import PartitionSpec as P

D = 3072
HALF = D // 2
HEAD_DIM = 128
C = 128
ITERS = 2
EPSILON = 1e-05
KEY_BLOCK = 512
BF16 = jnp.bfloat16
F32 = jnp.float32


def split_two(value):
    high = value.astype(BF16)
    return high, (value - high.astype(F32)).astype(BF16)


def dot(left, right):
    return jnp.dot(left, right, preferred_element_type=F32)


def dot_t(left, right):
    return lax.dot_general(left, right, (((1,), (1,)), ((), ())), preferred_element_type=F32)


def layer_norm(stream, gain):
    center = stream - jnp.mean(stream, axis=-1, keepdims=True)
    spread = jnp.mean(center * center, axis=-1, keepdims=True)
    return center * lax.rsqrt(spread + EPSILON) * gain


def frequencies():
    return jnp.exp(-jnp.log(10000.0) * 2.0 * jnp.arange(HALF).astype(F32) / D)


MESH = pl.DeviceIdType.MESH


def seat():
    head = lax.axis_index("head")
    return lax.axis_index("seq"), lax.div(head, 2), lax.rem(head, 2)


def plus(y, by):
    return lax.rem(y + by, 4)


def greet(targets):
    barrier = pltpu.get_barrier_semaphore()
    for target in targets:
        pl.semaphore_signal(barrier, inc=1, device_id=target, device_id_type=MESH)
    pl.semaphore_wait(barrier, len(targets))


def greet_all(devices, meanwhile=lambda: None):
    seq, y, c = seat()
    place = seq * 4 + y
    barrier = pltpu.get_barrier_semaphore()
    pl.semaphore_signal(barrier, inc=1, device_id={"head": 2 * y + 1 - c}, device_id_type=MESH)

    @pl.loop(1, devices)
    def _(k):
        other = lax.rem(place + k, devices)
        pl.semaphore_signal(
            barrier, inc=1,
            device_id={"seq": lax.div(other, 4), "head": 2 * lax.rem(other, 4) + c},
            device_id_type=MESH,
        )

    meanwhile()
    pl.semaphore_wait(barrier, devices)


def spread(buffer, send, recv):
    seq, y, c = seat()
    devices = buffer.shape[0]
    place = seq * 4 + y
    partner = {"head": 2 * y + 1 - c}
    whole = buffer.at[pl.ds(0, devices - 1), c]
    arrived = pltpu.make_async_remote_copy(
        src_ref=whole, dst_ref=whole, send_sem=send.at[0], recv_sem=recv.at[0],
        device_id=partner, device_id_type=MESH,
    )
    across = pltpu.make_async_remote_copy(
        src_ref=buffer.at[:, c], dst_ref=buffer.at[:, c], send_sem=send.at[1], recv_sem=recv.at[1],
        device_id=partner, device_id_type=MESH,
    )

    def begin():
        @pl.loop(1, devices)
        def _(k):
            other = lax.rem(place + k, devices)
            pltpu.make_async_remote_copy(
                src_ref=buffer.at[place, c], dst_ref=buffer.at[place, c],
                send_sem=send.at[0], recv_sem=recv.at[0],
                device_id={"seq": lax.div(other, 4), "head": 2 * lax.rem(other, 4) + c},
                device_id_type=MESH,
            ).start()

    def cross():
        arrived.wait_recv()
        across.start()

    def end():
        arrived.wait_send()
        across.wait()

    return begin, cross, end


class RingGather:
    FIRST = (0, 3, 1, 2)

    def __init__(self, own, out, local, send, recv):
        seq = lax.axis_index("seq")
        self.x, self.z = lax.div(seq, 4), lax.rem(seq, 4)
        self.own, self.out, self.send, self.recv = own, out, send, recv
        self.keep = pltpu.make_async_copy(own, out.at[seq], local)

    def place(self, half, p, q):
        x, z = (p, q) if half == 0 else (q, p)
        return plus(self.x, x) * 4 + plus(self.z, z)

    def move(self, half, slot):
        if slot < 4:
            kind, block, target = slot, None, [(1, 0), (3, 0), (1, 0), (3, 0)][slot]
            origin = [(0, 0), (0, 0), (3, 0), (1, 0)][slot]
        else:
            block, kind = divmod(slot - 4, 4)
            target = [(0, 1), (0, 3), (0, 1), (0, 3)][kind]
            origin = (self.FIRST[block], [0, 0, 3, 1][kind])
        ref = self.out.at[self.place(half, *origin), half]
        if kind >= 2:
            part = ref.shape[0] // 2
            ref = ref.at[pl.ds((kind - 2) * part, part)]
        source = self.own.at[half] if origin == (0, 0) else ref
        return pltpu.make_async_remote_copy(
            src_ref=source, dst_ref=ref,
            send_sem=self.send.at[20 * half + slot], recv_sem=self.recv.at[20 * half + slot],
            device_id={"seq": self.place(half, *target)}, device_id_type=MESH,
        )

    def neighbours(self):
        return [{"seq": self.place(0, *at)} for at in ((1, 0), (3, 0), (0, 1), (0, 3))]

    def on(self, slots, *following):
        for half in range(2):
            for slot in slots:
                self.move(half, slot).wait_recv()
            for slot in following:
                self.move(half, slot).start()

    def begin(self):
        self.keep.start()
        self.on((), 0, 1)
        self.on((), 4, 5)

    def first(self):
        self.on((0,), 2, 8, 9)
        self.on((1,), 3, 12, 13)

    def second(self):
        self.on((4,), 6)
        self.on((5,), 7)
        self.on((2, 3), 16, 17)

    def third(self):
        for block in (1, 2):
            self.on((4 + 4 * block,), 6 + 4 * block)
            self.on((5 + 4 * block,), 7 + 4 * block)

    def fourth(self):
        self.on((16,), 18)
        self.on((17,), 19)

    def end(self):
        self.on((6, 7, 10, 11, 14, 15, 18, 19))
        self.keep.wait()
        for half in range(2):
            for slot in range(20):
                self.move(half, slot).wait_send()


def first_kernel(
    rows, latent_ref, turn_ref, fine_a, fine_b, gain_ref, wq_ref, wk_ref, wv_ref, win_ref, up_ref,
    kv_ref, h_ref, n_ref, eq_ref, aq_ref, akv_ref, g_ref, x_out, edge_out, full_ref,
    x_ref, edge_ref, shard, scaled_0, scaled_1, high_0, high_1, mean_0, mean_1, base, wkv, gw, wsum, edge_rows,
    loads, xsend, xrecv, local, gsend, grecv,
):
    step, steps = pl.program_id(0), pl.num_programs(0)
    seq, y, c = seat()
    width = wk_ref.shape[1]
    fetches = [
        pltpu.make_async_copy(ref, wkv.at[:, pl.ds(k * width, width)], loads.at[k])
        for k, ref in enumerate((wk_ref, wv_ref))
    ]
    begin, cross, end = spread(x_ref, xsend, xrecv)
    count = lax.axis_size("seq")
    edge = pltpu.make_async_remote_copy(
        src_ref=edge_rows, dst_ref=edge_ref, send_sem=xsend.at[2], recv_sem=xrecv.at[2],
        device_id={"seq": lax.rem(seq + count - 1, count)}, device_id_type=MESH,
    )
    ring = RingGather(shard, full_ref, local, gsend, grecv)
    fetches.append(pltpu.make_async_copy(up_ref, shard, loads.at[2]))

    def fill(block, scaled, high, mean):
        total = jnp.zeros((rows, 1), F32)
        wide = 512
        for at in range(0, HALF, wide):
            cols = slice(at, at + wide)
            sin_a, cos_a = turn_ref[block, 0:1, cols], turn_ref[block, 1:2, cols]
            sin_b, cos_b = base[0, :, cols], base[1, :, cols]
            for part, offset in (
                (sin_a * cos_b + cos_a * sin_b, 0),
                (cos_a * cos_b - sin_a * sin_b, HALF),
            ):
                into = slice(offset + at, offset + at + wide)
                high[:, into] = part.astype(BF16)
                scaled[:, into] = (part * gain_ref[:, into]).astype(BF16)
                total = total + jnp.sum(part, axis=1, keepdims=True)
        mean[...] = total * (1.0 / D)

    def tables():
        edge_rows[...] = latent_ref[0:8, :]
        own = pl.ds(pl.multiple_of((2 * y + c) * (rows // 8), rows // 8), rows // 8)
        x_ref[seq * 4 + y, c] = latent_ref[own, :].astype(BF16)

        @pl.loop(0, rows // 16)
        def _(k):
            sin_a, cos_a = fine_a[k, 0:1, :], fine_a[k, 1:2, :]
            sin_b, cos_b = fine_b[0], fine_b[1]
            into = pl.ds(pl.multiple_of(k * 16, 16), 16)
            base[0, into, :] = sin_a * cos_b + cos_a * sin_b
            base[1, into, :] = cos_a * cos_b - sin_a * sin_b

        wsum[...] = dot_t(jnp.ones((16, D), BF16), win_ref[...])
        gain = gain_ref[...]
        high = gain.astype(BF16).astype(F32)
        line = lax.broadcasted_iota(jnp.int32, (16, D), 0)
        both = jnp.where(line == 0, high, jnp.where(line == 1, gain - high, 0.0)).astype(BF16)
        for fetch in fetches:
            fetch.wait()
        gw[:, 0:width] = dot(both, wq_ref[...])
        gw[:, width:] = dot(both, wkv[...])
        gw[0:1, :] = jnp.sum(gw[...], axis=0, keepdims=True)

    @pl.when(step == 0)
    def _():
        for fetch in fetches:
            fetch.start()
        greet_all(x_ref.shape[0], tables)
        begin()
        edge.start()
        ring.begin()
        fill(0, scaled_0, high_0, mean_0)

    def work(scaled, high, mean, others):
        value = mean[...]
        kv_ref[...] = dot(scaled[...], wkv[...]) - value * gw[0:1, width:]
        h_ref[...] = dot_t(high[...], win_ref[...]) - value * wsum[0:1, :]
        n_ref[...] = HALF - D * value * value
        fill(jnp.minimum(step + 1, steps - 1), *others)

        @pl.when(step == seq)
        def _():
            eq_ref[...] = dot(scaled[...], wq_ref[...]) - value * gw[0:1, 0:width]

    even, odd = (scaled_0, high_0, mean_0), (scaled_1, high_1, mean_1)

    @pl.when(lax.rem(step, 2) == 0)
    def _():
        work(*even, odd)

    @pl.when(lax.rem(step, 2) == 1)
    def _():
        work(*odd, even)

    @pl.when(step == 3)
    def _():
        cross()

    @pl.when(step == 5)
    def _():
        ring.first()

    @pl.when(step == 11)
    def _():
        ring.second()

    @pl.when(step == steps - 1)
    def _():
        ring.third()
        wide = win_ref[...].astype(F32)
        center = wide - jnp.mean(wide, axis=1, keepdims=True)
        high, low = split_two(center * gain_ref[...])
        scaled_0[0:C, :] = high
        scaled_0[C : 2 * C, :] = low
        for into, weight in ((aq_ref, wq_ref), (akv_ref, wkv)):
            both = dot(scaled_0[0 : 2 * C, :], weight[...])
            high, low = split_two(both[:C] + both[C:])
            into[0:C, :] = high
            into[C : 2 * C, :] = low
        ring.fourth()
        high, low = split_two(center)
        high_0[0:C, :] = high
        high_1[0:C, :] = low
        high, low = high_0[0:C, :], high_1[0:C, :]
        high, low = split_two(dot_t(high, high) + dot_t(high, low) + dot_t(low, high))
        g_ref[0:C, :] = high
        g_ref[C : 2 * C, :] = low
        end()
        edge.wait()
        x_out[...] = x_ref[...]
        edge_out[...] = edge_ref[...]
        ring.end()


def ring_scratch():
    return [
        pltpu.SemaphoreType.DMA,
        pltpu.SemaphoreType.DMA((40,)),
        pltpu.SemaphoreType.DMA((40,)),
    ]


def first(rows, blocks, places, latent, gain, w_query, w_key, w_value, w_in, up):
    freq = frequencies()
    scale = jnp.array([rows, 16.0, 1.0], F32)[:, None] * jnp.arange(16, dtype=F32)[None, :]
    angles = scale[:, :, None] * freq[None, None, :]
    sines, cosines = jnp.sin(angles), jnp.cos(angles)
    turn = jnp.stack([sines[0], cosines[0]], axis=1)
    fine_a = jnp.stack([sines[1], cosines[1]], axis=1)
    fine_b = jnp.stack([sines[2], cosines[2]], axis=0)
    return first_call(rows, blocks, places, latent, turn, fine_a, fine_b, gain, w_query, w_key,
                      w_value, w_in, up)


def first_call(rows, blocks, places, latent, turn, fine_a, fine_b, gain, w_query, w_key, w_value,
               w_in, up):
    width = w_key.shape[1]
    length = rows * blocks
    whole = pl.BlockSpec(memory_space=pltpu.VMEM)
    far = pl.BlockSpec(memory_space=pl.ANY)
    return pl.pallas_call(
        functools.partial(first_kernel, rows),
        grid=(blocks,),
        in_specs=[whole] * 6 + [far, far, whole, far],
        out_specs=[
            pl.BlockSpec((rows, 2 * width), lambda i: (i, 0)),
            pl.BlockSpec((rows, C), lambda i: (i, 0)),
            pl.BlockSpec((rows, 1), lambda i: (i, 0)),
        ]
        + [whole] * 6
        + [far],
        out_shape=[
            jax.ShapeDtypeStruct((length, 2 * width), F32),
            jax.ShapeDtypeStruct((length, C), F32),
            jax.ShapeDtypeStruct((length, 1), F32),
            jax.ShapeDtypeStruct((rows, width), F32),
            jax.ShapeDtypeStruct((2 * C, width), BF16),
            jax.ShapeDtypeStruct((2 * C, 2 * width), BF16),
            jax.ShapeDtypeStruct((2 * C, C), BF16),
            jax.ShapeDtypeStruct((places, 2, rows // 8, C), BF16),
            jax.ShapeDtypeStruct((8, C), F32),
            jax.ShapeDtypeStruct((blocks, *up.shape), BF16),
        ],
        scratch_shapes=[
            pltpu.VMEM((places, 2, rows // 8, C), BF16),
            pltpu.VMEM((8, C), F32),
            pltpu.VMEM(up.shape, BF16),
        ]
        + [pltpu.VMEM((rows, D), BF16)] * 4
        + [pltpu.VMEM((rows, 1), F32)] * 2
        + [
            pltpu.VMEM((2, rows, HALF), F32),
            pltpu.VMEM((D, 2 * width), BF16),
            pltpu.VMEM((16, 3 * width), F32),
            pltpu.VMEM((16, C), F32),
            pltpu.VMEM((8, C), F32),
            pltpu.SemaphoreType.DMA((3,)),
            pltpu.SemaphoreType.DMA((3,)),
            pltpu.SemaphoreType.DMA((3,)),
        ]
        + ring_scratch(),
        compiler_params=pltpu.CompilerParams(
            collective_id=0, has_side_effects=True, vmem_limit_bytes=44 << 20
        ),
        cost_estimate=pl.CostEstimate(
            flops=60_000_000_000, bytes_accessed=40_000_000, transcendentals=0
        ),
        name="first",
    )(latent, turn, fine_a, fine_b, gain, w_query, w_key, w_value, w_in, up)


def reduce_over_head(produce, meanwhile, term, taken, via_out, via_in, near, fin, send, recv):
    _, y, c = seat()
    partner, up, down = 2 * y + 1 - c, 2 * plus(y, 1) + c, 2 * plus(y, 3) + c

    def copy(src, dst, slot, head):
        return pltpu.make_async_remote_copy(
            src_ref=src, dst_ref=dst, send_sem=send.at[slot], recv_sem=recv.at[slot],
            device_id={"head": head}, device_id_type=MESH,
        )

    def pair(half, at):
        return term[half, at, c].astype(F32) + taken[half, at].astype(F32)

    gives = []
    for half in range(2):
        produce(half)
        gives.append(copy(term.at[half, :, 1 - c], taken.at[half], half, partner))
        gives[half].start()
    meanwhile()
    across, ahead, behind = plus(y, 2), plus(y, 1), plus(y, 3)
    gives[0].wait_recv()
    via_out[0] = pair(0, across).astype(BF16)
    via_0 = copy(via_out.at[0], via_in.at[0], 2, up)
    via_0.start()
    near[1, 0] = pair(0, behind).astype(BF16)
    down_0 = copy(near.at[1, 0], fin.at[1, 0], 6, down)
    down_0.start()
    gives[1].wait_recv()
    via_out[1] = pair(1, across).astype(BF16)
    via_1 = copy(via_out.at[1], via_in.at[1], 3, down)
    via_1.start()
    near[0, 1] = pair(1, ahead).astype(BF16)
    up_1 = copy(near.at[0, 1], fin.at[0, 1], 5, up)
    up_1.start()
    via_0.wait_recv()
    near[0, 0] = (pair(0, ahead) + via_in[0].astype(F32)).astype(BF16)
    up_0 = copy(near.at[0, 0], fin.at[0, 0], 4, up)
    up_0.start()
    via_1.wait_recv()
    near[1, 1] = (pair(1, behind) + via_in[1].astype(F32)).astype(BF16)
    down_1 = copy(near.at[1, 1], fin.at[1, 1], 7, down)
    down_1.start()
    sums = [pair(half, y) for half in range(2)]
    down_0.wait_recv()
    up_0.wait_recv()
    first = sums[0] + fin[0, 0].astype(F32) + fin[1, 0].astype(F32)
    up_1.wait_recv()
    down_1.wait_recv()
    second = sums[1] + fin[0, 1].astype(F32) + fin[1, 1].astype(F32)
    for done in (*gives, via_0, via_1, up_0, up_1, down_0, down_1):
        done.wait_send()
    return jnp.concatenate([first, second], axis=1)


def gather_over_head(out, send, recv, midway=lambda: None):
    _, y, c = seat()
    partner, up, down = 2 * y + 1 - c, 2 * plus(y, 1) + c, 2 * plus(y, 3) + c
    across, ahead, behind = plus(y, 2), plus(y, 1), plus(y, 3)
    low, high = pl.ds(0, HALF), pl.ds(HALF, HALF)

    def copy(block, slot, head):
        return pltpu.make_async_remote_copy(
            src_ref=block, dst_ref=block, send_sem=send.at[slot], recv_sem=recv.at[slot],
            device_id={"head": head}, device_id_type=MESH,
        )

    moves = [copy(out.at[y, c], 0, up), copy(out.at[y, c], 1, down), copy(out.at[y, c], 2, partner)]
    for move in moves:
        move.start()

    def then(slot, *following):
        moves[slot].wait_recv()
        for move in following:
            move.start()
            moves.append(move)

    then(0, copy(out.at[behind, c, :, low], 3, up), copy(out.at[behind, c], 4, partner))
    then(1, copy(out.at[ahead, c, :, high], 5, down), copy(out.at[ahead, c], 6, partner))
    midway()
    then(3, copy(out.at[across, c, :, low], 7, partner))
    then(5, copy(out.at[across, c, :, high], 8, partner))
    for slot in (2, 4, 6, 7, 8):
        moves[slot].wait_recv()
    for move in moves:
        move.wait_send()


def reduce_scratch(share):
    return [
        pltpu.VMEM((2, 4, 2, share, HALF), BF16),
        pltpu.VMEM((2, 4, share, HALF), BF16),
        pltpu.VMEM((2, share, HALF), BF16),
        pltpu.VMEM((2, share, HALF), BF16),
        pltpu.VMEM((2, 2, share, HALF), BF16),
        pltpu.VMEM((2, 2, share, HALF), BF16),
        pltpu.SemaphoreType.DMA((8,)),
        pltpu.SemaphoreType.DMA((8,)),
    ]


def head_neighbours():
    _, y, c = seat()
    return [{"head": 2 * y + 1 - c}, {"head": 2 * plus(y, 1) + c}, {"head": 2 * plus(y, 3) + c}]


def store_terms(term, half, at, share, value):
    for block in range(8):
        rows = value[block * share : (block + 1) * share].astype(BF16)
        term[half, block // 2, block % 2, :, at : at + value.shape[1]] = rows


def block_kernel(rows, heads, ringed, *refs):
    (
        x_ref, kv_ref, h_ref, n_ref, eq_ref, aq_ref, akv_ref, g_ref,
        embedding_ref, win_ref, wo_ref, gain_ref, *refs,
    ) = refs
    if ringed:
        shard_ref, stream_ref, normed_out, full_ref, *refs = refs
        *refs, shard, load, local, gsend, grecv = refs
        ring = RingGather(shard, full_ref, local, gsend, grecv)
        fetch = pltpu.make_async_copy(shard_ref, shard, load)
    else:
        stream_ref, normed_out, *refs = refs
    normed_ref, queries, acc, sums, attended, *parts, send, recv = refs
    term = parts[0]
    share = rows // 8
    width = heads * HEAD_DIM
    block = pl.program_id(0)
    me, y, c = seat()

    def scale_of(x, h, n):
        twice = jnp.concatenate([x, x], axis=1)
        quad = jnp.sum(x.astype(F32) * (dot(twice, g_ref[...]) + 2.0 * h), axis=1, keepdims=True)
        return twice, lax.rsqrt(jnp.maximum(quad + n, 0.0) * (1.0 / D) + EPSILON)

    @pl.when(block == 0)
    def _():
        if ringed:
            fetch.start()
        greet(head_neighbours() + (ring.neighbours() if ringed else []))
        if ringed:
            fetch.wait()
            ring.begin()
        own = pl.ds(pl.multiple_of(me * rows, rows), rows)
        twice, scale = scale_of(x_ref[own, :], h_ref[own, :], n_ref[own, :])
        value = (dot(twice, aq_ref[...]) + eq_ref[...]) * (scale * HEAD_DIM**-0.5)
        queries[...] = value.astype(BF16)
        acc[...] = jnp.zeros_like(acc)
        sums[...] = jnp.zeros_like(sums)

    def step(masked):
        here = pl.ds(pl.multiple_of(block * KEY_BLOCK, KEY_BLOCK), KEY_BLOCK)
        twice, scale = scale_of(x_ref[here, :], h_ref[here, :], n_ref[here, :])
        both = ((dot(twice, akv_ref[...]) + kv_ref[...]) * scale).astype(BF16)
        keys, values = both[:, :width], both[:, width:]
        if masked:
            shape = (rows, KEY_BLOCK)
            row = me * rows + lax.broadcasted_iota(jnp.int32, shape, 0)
            col = block * KEY_BLOCK + lax.broadcasted_iota(jnp.int32, shape, 1)
            seen = col <= row
        for head in range(heads):
            cols = slice(head * HEAD_DIM, (head + 1) * HEAD_DIM)
            scores = dot_t(queries[:, cols], keys[:, cols])
            if masked:
                weights = jnp.where(seen, jnp.exp(jnp.where(seen, scores, 0.0)), 0.0)
            else:
                weights = jnp.exp(scores)
            part = weights[:, :HEAD_DIM]
            for at in range(HEAD_DIM, KEY_BLOCK, HEAD_DIM):
                part = part + weights[:, at : at + HEAD_DIM]
            sums[:, cols] += part
            acc[:, cols] += dot(weights.astype(BF16), values[:, cols])

    final = (me * rows + rows - 1) // KEY_BLOCK

    @pl.when(block < final)
    def _():
        step(False)

    @pl.when(block == final)
    def _():
        step(True)

    def produce(half):
        for at in range(0, HALF, 768):
            cols = slice(half * HALF + at, half * HALF + at + 768)
            store_terms(term, half, at, share, dot(attended[...], wo_ref[:, cols]))

    def meanwhile():
        first = pl.ds(pl.multiple_of(me * rows + (2 * y + c) * share, share), share)
        stream_ref[...] = dot(x_ref[first, :], win_ref[...]) + embedding_ref[...]
        if ringed:
            ring.first()

    @pl.when(block == pl.num_programs(0) - 1)
    def _():
        for head in range(heads):
            cols = slice(head * HEAD_DIM, (head + 1) * HEAD_DIM)
            total = jnp.sum(sums[:, cols], axis=1, keepdims=True)
            attended[:, cols] = (acc[:, cols] / total).astype(BF16)
        total = reduce_over_head(produce, meanwhile, *parts)
        stream = stream_ref[...] + total
        stream_ref[...] = stream
        normed_ref[y, c] = layer_norm(stream, gain_ref[...]).astype(BF16)
        gather_over_head(normed_ref, send, recv, ring.second if ringed else lambda: None)
        normed_out[...] = normed_ref[...]
        if ringed:
            ring.third()
            ring.fourth()
            ring.end()


def block_step(rows, state, x, embedding, w_in, w_attn_out, gain, shard=None):
    kv = state[0]
    length, width = kv.shape[0], kv.shape[1] // 2
    share = rows // 8
    ringed = shard is not None
    whole = pl.BlockSpec(memory_space=pltpu.VMEM)
    far = pl.BlockSpec(memory_space=pl.ANY)
    tile = pl.BlockSpec((KEY_BLOCK, 2 * width), lambda i: (i, 0))
    more = [shard] if ringed else []
    outs = [
        jax.ShapeDtypeStruct((share, D), F32),
        jax.ShapeDtypeStruct((4, 2, share, D), BF16),
    ]
    if ringed:
        outs.append(jax.ShapeDtypeStruct((length // rows, *shard.shape), BF16))
    return pl.pallas_call(
        functools.partial(block_kernel, rows, width // HEAD_DIM, ringed),
        grid=(length // KEY_BLOCK,),
        in_specs=[whole, tile] + [whole] * 10 + [far] * ringed,
        out_specs=[whole] * 2 + [far] * ringed,
        out_shape=outs,
        scratch_shapes=[
            pltpu.VMEM((4, 2, share, D), BF16),
            pltpu.VMEM((rows, width), BF16),
            pltpu.VMEM((rows, width), F32),
            pltpu.VMEM((rows, width), F32),
            pltpu.VMEM((rows, width), BF16),
        ]
        + reduce_scratch(share)
        + [pltpu.SemaphoreType.DMA((9,)), pltpu.SemaphoreType.DMA((9,))]
        + ([pltpu.VMEM(shard.shape, BF16), pltpu.SemaphoreType.DMA] + ring_scratch() if ringed else []),
        compiler_params=pltpu.CompilerParams(
            collective_id=1 if ringed else 4, has_side_effects=True, vmem_limit_bytes=40 << 20
        ),
        cost_estimate=pl.CostEstimate(
            flops=30_000_000_000, bytes_accessed=20_000_000, transcendentals=0
        ),
        name="block_ring" if ringed else "block",
    )(x, *state, embedding, w_in, w_attn_out, gain, *more)


def mlp_kernel(
    share, last, normed_ref, up_ref, down_ref, stream_ref, gain_ref, wf_ref, ahead_ref, out_ref,
    up, down, hidden, loads, *scratch,
):
    *parts, send, recv = scratch
    term = parts[0]
    seq, y, c = seat()
    ups, downs = up.shape[0], down.shape[0]
    wide, tall = up.shape[2], down.shape[1]
    fetches = [
        pltpu.make_async_copy(up_ref.at[:, pl.ds(k * wide, wide)], up.at[k], loads.at[k])
        for k in range(ups)
    ] + [
        pltpu.make_async_copy(
            down_ref.at[pl.ds(k * tall, tall), :], down.at[k], loads.at[ups + k]
        )
        for k in range(downs)
    ]
    for fetch in fetches:
        fetch.start()
    if last:
        mirror = lax.axis_size("seq") - 1 - seq
        sends_edge = jnp.logical_and(mirror > 0, 2 * y + c == 7)
        keeps_edge = jnp.logical_and(mirror - 1 == seq, 2 * y + c == 7)
        waits_edge = jnp.logical_and(mirror > 0, jnp.logical_not(keeps_edge))
        barrier = pltpu.get_barrier_semaphore()
        for target in head_neighbours():
            pl.semaphore_signal(barrier, inc=1, device_id=target, device_id_type=MESH)
        for head in range(8):
            pl.semaphore_signal(
                barrier, inc=1, device_id={"seq": mirror, "head": head}, device_id_type=MESH
            )

        @pl.when(waits_edge)
        def _():
            pl.semaphore_signal(
                barrier, inc=1, device_id={"seq": mirror - 1, "head": 7}, device_id_type=MESH
            )

        @pl.when(keeps_edge)
        def _():
            pl.semaphore_wait(barrier, 18)

        @pl.when(jnp.logical_and(sends_edge, jnp.logical_not(keeps_edge)))
        def _():
            pl.semaphore_wait(barrier, 19)

        @pl.when(jnp.logical_not(sends_edge))
        def _():
            pl.semaphore_wait(barrier, 11)

    else:
        greet_all(out_ref.shape[0])

    for k in range(ups):
        fetches[k].wait()
        pre = dot(normed_ref[...], up[k])
        hidden[:, k * wide : (k + 1) * wide] = jax.nn.gelu(pre, approximate=True).astype(BF16)

    def produce(half):
        for at in range(downs // 2):
            k = half * (downs // 2) + at
            fetches[ups + k].wait()
            store_terms(term, half, at * tall, share, dot_t(hidden[...], down[k]))

    total = reduce_over_head(produce, lambda: None, *parts)
    normed = layer_norm(stream_ref[...] + total, gain_ref[...]).astype(BF16)
    params = dot(normed, wf_ref[...])
    following = ahead_ref[...] * jnp.exp(jnp.tanh(params[:, C:])) + params[:, :C]
    if not last:
        out_ref[seq * 4 + y, c] = following.astype(BF16)
        begin, cross, end = spread(out_ref, send, recv)
        begin()
        cross()
        end()
    else:
        block = scratch[0].at[0, 0, 0, :, pl.ds(0, C)]
        block[...] = following.astype(BF16)
        head = 2 * y + c
        moves = [
            pltpu.make_async_remote_copy(
                src_ref=block, dst_ref=out_ref.at[head], send_sem=send.at[k], recv_sem=recv.at[0],
                device_id={"seq": mirror, "head": k}, device_id_type=MESH,
            )
            for k in range(8)
        ]
        edges = [
            pltpu.make_async_remote_copy(
                src_ref=block, dst_ref=out_ref.at[8], send_sem=send.at[8 + k], recv_sem=recv.at[1],
                device_id={"seq": mirror - 1, "head": k}, device_id_type=MESH,
            )
            for k in range(8)
        ]
        for move in moves:
            move.start()

        @pl.when(sends_edge)
        def _():
            for move in edges[:7]:
                move.start()

        @pl.when(jnp.logical_and(sends_edge, jnp.logical_not(keeps_edge)))
        def _():
            edges[7].start()

        whole = out_ref.at[pl.ds(0, 8)]
        pltpu.make_async_remote_copy(
            src_ref=whole, dst_ref=whole, send_sem=send.at[0], recv_sem=recv.at[0],
            device_id={"seq": mirror, "head": 0}, device_id_type=MESH,
        ).wait_recv()

        @pl.when(waits_edge)
        def _():
            pltpu.make_async_remote_copy(
                src_ref=block, dst_ref=out_ref.at[8], send_sem=send.at[0], recv_sem=recv.at[1],
                device_id={"seq": mirror - 1, "head": 7}, device_id_type=MESH,
            ).wait_recv()

        for move in moves:
            move.wait_send()

        @pl.when(sends_edge)
        def _():
            for move in edges[:7]:
                move.wait_send()

        @pl.when(jnp.logical_and(sends_edge, jnp.logical_not(keeps_edge)))
        def _():
            edges[7].wait_send()

        @pl.when(jnp.logical_not(waits_edge))
        def _():
            out_ref[8] = following.astype(BF16)


def mlp(share, places, last, normed, up, down, stream, gain, w_final, ahead):
    whole = pl.BlockSpec(memory_space=pltpu.VMEM)
    rows, width = normed.shape[0], up.shape[1]
    shape = (9, share, C) if last else (places, 2, share, C)
    return pl.pallas_call(
        functools.partial(mlp_kernel, share, last),
        in_specs=[whole] + [pl.BlockSpec(memory_space=pl.ANY)] * 2 + [whole] * 4,
        out_specs=whole,
        out_shape=jax.ShapeDtypeStruct(shape, BF16),
        scratch_shapes=[
            pltpu.VMEM((3, D, width // 3), BF16),
            pltpu.VMEM((4, D // 4, width), BF16),
            pltpu.VMEM((rows, width), BF16),
            pltpu.SemaphoreType.DMA((7,)),
        ]
        + reduce_scratch(share)
        + [pltpu.SemaphoreType.DMA((16,)), pltpu.SemaphoreType.DMA((2,))],
        compiler_params=pltpu.CompilerParams(
            collective_id=3 if last else 2, has_side_effects=True, vmem_limit_bytes=44 << 20
        ),
        cost_estimate=pl.CostEstimate(
            flops=40_000_000_000, bytes_accessed=30_000_000, transcendentals=0
        ),
        name="mlp_last" if last else "mlp",
    )(normed, up, down, stream, gain, w_final, ahead)


def per_device(
    latent, w_in, w_query, w_key, w_value, w_attn_out, w_up, w_down, w_final,
    gain_attn, gain_mlp, gain_final,
):
    seq_count, head_count = lax.axis_size("seq"), lax.axis_size("head")
    me, mine = lax.axis_index("seq"), lax.axis_index("head")
    rows = latent.shape[0]
    share = rows // head_count
    length = rows * seq_count
    places = seq_count * head_count // 2
    start = me * rows + mine * share

    shape = (2, w_up.shape[0] // 2, w_up.shape[1])
    *state, gathered, edge, up = first(
        rows, seq_count, places, latent, gain_attn[None, :], w_query, w_key, w_value, w_in,
        w_up.reshape(shape),
    )
    up = up.reshape(D, w_up.shape[1])
    x = gathered.reshape(length, C)
    angles = (start + jnp.arange(share)).astype(F32)[:, None] * frequencies()[None, :]
    embedding = jnp.concatenate([jnp.sin(angles), jnp.cos(angles)], axis=1)
    ahead = lax.dynamic_slice_in_dim(
        jnp.concatenate([latent[1:], edge[:1]], axis=0), mine * share, share, 0
    )
    top = x[:1]
    for step_index in range(ITERS):
        last = step_index == ITERS - 1
        stream, normed, *full = block_step(
            rows, state, x, embedding, w_in, w_attn_out, gain_mlp[None, :],
            w_down.T.reshape(shape) if step_index == 0 else None,
        )
        if step_index == 0:
            down = full[0].reshape(D, w_up.shape[1])
        following = mlp(
            share, places, last, normed.reshape(rows, D), up, down, stream, gain_final[None, :],
            w_final, ahead,
        )
        if not last:
            x = jnp.concatenate([top, following.reshape(length, C)[:-1]], axis=0)
    edge = jnp.where(me == seq_count - 1, top, following[8, share - 1 :])
    result = jnp.concatenate([edge, following[:8].reshape(rows, C)[:-1]], axis=0)
    return result[::-1].astype(F32)


def solution(mesh):
    in_specs = (
        P("seq", None),
        P(),
        P(None, "head"),
        P(None, "head"),
        P(None, "head"),
        P("head", None),
        P("seq", "head"),
        P("head", "seq"),
        P(),
        P(),
        P(),
        P(),
    )
    return jax.shard_map(
        per_device, mesh=mesh, in_specs=in_specs, out_specs=P("seq", None), check_vma=False
    )
```

```python
import functools

import jax
import jax.numpy as jnp
from jax import lax
from jax.experimental import pallas as pl
from jax.experimental.pallas import tpu as pltpu
from jax.sharding import PartitionSpec as P

D = 3072
HALF = D // 2
HEAD_DIM = 128
C = 128
ITERS = 2
EPSILON = 1e-05
KEY_BLOCK = 512
BF16 = jnp.bfloat16
F32 = jnp.float32


def split_two(value):
    high = value.astype(BF16)
    return high, (value - high.astype(F32)).astype(BF16)


def dot(left, right):
    return jnp.dot(left, right, preferred_element_type=F32)


def dot_t(left, right):
    return lax.dot_general(left, right, (((1,), (1,)), ((), ())), preferred_element_type=F32)


def layer_norm(stream, gain):
    center = stream - jnp.mean(stream, axis=-1, keepdims=True)
    spread = jnp.mean(center * center, axis=-1, keepdims=True)
    return center * lax.rsqrt(spread + EPSILON) * gain


def frequencies():
    return jnp.exp(-jnp.log(10000.0) * 2.0 * jnp.arange(HALF).astype(F32) / D)


MESH = pl.DeviceIdType.MESH


def staged(pairs, sems):
    return [pltpu.make_async_copy(src, dst, sems.at[k]) for k, (src, dst) in enumerate(pairs)]


def each(action, copies):
    for copy in copies:
        getattr(copy, action)()


def buffer_like(array):
    return pltpu.VMEM(array.shape, array.dtype)


def seat():
    head = lax.axis_index("head")
    return lax.axis_index("seq"), lax.div(head, 2), lax.rem(head, 2)


def plus(y, by):
    return lax.rem(y + by, 4)


def hail(targets):
    barrier = pltpu.get_barrier_semaphore()
    for target in targets:
        pl.semaphore_signal(barrier, inc=1, device_id=target, device_id_type=MESH)


def met(targets):
    pl.semaphore_wait(pltpu.get_barrier_semaphore(), len(targets))


def greet_all(devices, meanwhile=lambda: None):
    seq, y, c = seat()
    place = seq * 4 + y
    barrier = pltpu.get_barrier_semaphore()
    pl.semaphore_signal(barrier, inc=1, device_id={"head": 2 * y + 1 - c}, device_id_type=MESH)

    @pl.loop(1, devices)
    def _(k):
        other = lax.rem(place + k, devices)
        pl.semaphore_signal(
            barrier, inc=1,
            device_id={"seq": lax.div(other, 4), "head": 2 * lax.rem(other, 4) + c},
            device_id_type=MESH,
        )

    meanwhile()
    pl.semaphore_wait(barrier, devices)


def spread(buffer, send, recv):
    seq, y, c = seat()
    devices = buffer.shape[0]
    place = seq * 4 + y
    partner = {"head": 2 * y + 1 - c}
    whole = buffer.at[pl.ds(0, devices - 1), c]
    arrived = pltpu.make_async_remote_copy(
        src_ref=whole, dst_ref=whole, send_sem=send.at[0], recv_sem=recv.at[0],
        device_id=partner, device_id_type=MESH,
    )
    across = pltpu.make_async_remote_copy(
        src_ref=buffer.at[:, c], dst_ref=buffer.at[:, c], send_sem=send.at[1], recv_sem=recv.at[1],
        device_id=partner, device_id_type=MESH,
    )

    def begin():
        @pl.loop(1, devices)
        def _(k):
            other = lax.rem(place + k, devices)
            pltpu.make_async_remote_copy(
                src_ref=buffer.at[place, c], dst_ref=buffer.at[place, c],
                send_sem=send.at[0], recv_sem=recv.at[0],
                device_id={"seq": lax.div(other, 4), "head": 2 * lax.rem(other, 4) + c},
                device_id_type=MESH,
            ).start()

    def cross():
        arrived.wait_recv()
        across.start()

    def end():
        arrived.wait_send()
        across.wait()

    return begin, cross, end


class RingGather:
    FIRST = (0, 3, 1, 2)

    def __init__(self, own, out, local, send, recv):
        seq = lax.axis_index("seq")
        self.x, self.z = lax.div(seq, 4), lax.rem(seq, 4)
        self.own, self.out, self.send, self.recv = own, out, send, recv
        self.keep = pltpu.make_async_copy(own, out.at[seq], local)

    def place(self, half, p, q):
        x, z = (p, q) if half == 0 else (q, p)
        return plus(self.x, x) * 4 + plus(self.z, z)

    def move(self, half, slot):
        if slot < 4:
            kind, block, target = slot, None, [(1, 0), (3, 0), (1, 0), (3, 0)][slot]
            origin = [(0, 0), (0, 0), (3, 0), (1, 0)][slot]
        else:
            block, kind = divmod(slot - 4, 4)
            target = [(0, 1), (0, 3), (0, 1), (0, 3)][kind]
            origin = (self.FIRST[block], [0, 0, 3, 1][kind])
        ref = self.out.at[self.place(half, *origin), half]
        if kind >= 2:
            part = ref.shape[0] // 2
            ref = ref.at[pl.ds((kind - 2) * part, part)]
        source = self.own.at[half] if origin == (0, 0) else ref
        return pltpu.make_async_remote_copy(
            src_ref=source, dst_ref=ref,
            send_sem=self.send.at[20 * half + slot], recv_sem=self.recv.at[20 * half + slot],
            device_id={"seq": self.place(half, *target)}, device_id_type=MESH,
        )

    def neighbours(self):
        return [{"seq": self.place(0, *at)} for at in ((1, 0), (3, 0), (0, 1), (0, 3))]

    def on(self, slots, *following):
        for half in range(2):
            for slot in slots:
                self.move(half, slot).wait_recv()
            for slot in following:
                self.move(half, slot).start()

    def begin(self):
        self.keep.start()
        self.on((), 0, 1)
        self.on((), 4, 5)

    def first(self):
        self.on((0,), 2, 8, 9)
        self.on((1,), 3, 12, 13)

    def second(self):
        self.on((4,), 6)
        self.on((5,), 7)

    def middle(self):
        self.on((2, 3), 16, 17)

    def third(self, block):
        self.on((4 + 4 * block,), 6 + 4 * block)
        self.on((5 + 4 * block,), 7 + 4 * block)

    def end(self):
        self.on((6, 7, 10, 11, 14, 15, 18, 19))
        self.keep.wait()
        for half in range(2):
            for slot in range(20):
                self.move(half, slot).wait_send()


def first_kernel(
    rows, latent_ref, turn_ref, fine_a, fine_b, gain_ref, wq_ref, wk_ref, wv_ref, win_ref, up_ref,
    kv_ref, h_ref, n_ref, eq_out, aq_out, akv_out, g_out, x_out, edge_out, full_ref,
    eq_ref, aq_ref, akv_ref, g_ref, x_ref, edge_ref, stores, shard, scaled_0, scaled_1, high_0, high_1, mean_0, mean_1, base, wkv, gw, wsum, edge_rows,
    loads, xsend, xrecv, local, gsend, grecv,
):
    step, steps = pl.program_id(0), pl.num_programs(0)
    seq, y, c = seat()
    width = wk_ref.shape[1]
    fetches = [
        pltpu.make_async_copy(ref, wkv.at[:, pl.ds(k * width, width)], loads.at[k])
        for k, ref in enumerate((wk_ref, wv_ref))
    ]
    begin, cross, end = spread(x_ref, xsend, xrecv)
    count = lax.axis_size("seq")
    edge = pltpu.make_async_remote_copy(
        src_ref=edge_rows, dst_ref=edge_ref, send_sem=xsend.at[2], recv_sem=xrecv.at[2],
        device_id={"seq": lax.rem(seq + count - 1, count)}, device_id_type=MESH,
    )
    ring = RingGather(shard, full_ref, local, gsend, grecv)
    fetches.append(pltpu.make_async_copy(up_ref, shard, loads.at[2]))
    results = staged(
        [
            (eq_ref, eq_out), (aq_ref, aq_out), (akv_ref, akv_out), (g_ref, g_out),
            (x_ref, x_out), (edge_ref, edge_out),
        ],
        stores,
    )

    def fill(block, scaled, high, mean):
        total = jnp.zeros((rows, 1), F32)
        wide = 512
        for at in range(0, HALF, wide):
            cols = slice(at, at + wide)
            sin_a, cos_a = turn_ref[block, 0:1, cols], turn_ref[block, 1:2, cols]
            sin_b, cos_b = base[0, :, cols], base[1, :, cols]
            for part, offset in (
                (sin_a * cos_b + cos_a * sin_b, 0),
                (cos_a * cos_b - sin_a * sin_b, HALF),
            ):
                into = slice(offset + at, offset + at + wide)
                high[:, into] = part.astype(BF16)
                scaled[:, into] = (part * gain_ref[:, into]).astype(BF16)
                total = total + jnp.sum(part, axis=1, keepdims=True)
        mean[...] = total * (1.0 / D)

    def tables():
        edge_rows[...] = latent_ref[0:8, :]
        own = pl.ds(pl.multiple_of((2 * y + c) * (rows // 8), rows // 8), rows // 8)
        x_ref[seq * 4 + y, c] = latent_ref[own, :].astype(BF16)

        @pl.loop(0, rows // 16)
        def _(k):
            sin_a, cos_a = fine_a[k, 0:1, :], fine_a[k, 1:2, :]
            sin_b, cos_b = fine_b[0], fine_b[1]
            into = pl.ds(pl.multiple_of(k * 16, 16), 16)
            base[0, into, :] = sin_a * cos_b + cos_a * sin_b
            base[1, into, :] = cos_a * cos_b - sin_a * sin_b

        wsum[...] = dot_t(jnp.ones((16, D), BF16), win_ref[...])
        gain = gain_ref[...]
        high = gain.astype(BF16).astype(F32)
        line = lax.broadcasted_iota(jnp.int32, (16, D), 0)
        both = jnp.where(line == 0, high, jnp.where(line == 1, gain - high, 0.0)).astype(BF16)
        for fetch in fetches:
            fetch.wait()
        gw[:, 0:width] = dot(both, wq_ref[...])
        gw[:, width:] = dot(both, wkv[...])
        gw[0:1, :] = jnp.sum(gw[...], axis=0, keepdims=True)

    @pl.when(step == 0)
    def _():
        for fetch in fetches:
            fetch.start()
        greet_all(x_ref.shape[0], tables)
        begin()
        edge.start()
        ring.begin()
        fill(0, scaled_0, high_0, mean_0)

    def work(scaled, high, mean, others):
        value = mean[...]
        kv_ref[...] = dot(scaled[...], wkv[...]) - value * gw[0:1, width:]
        h_ref[...] = dot_t(high[...], win_ref[...]) - value * wsum[0:1, :]
        n_ref[...] = HALF - D * value * value
        fill(jnp.minimum(step + 1, steps - 1), *others)

        @pl.when(step == seq)
        def _():
            eq_ref[...] = dot(scaled[...], wq_ref[...]) - value * gw[0:1, 0:width]

    even, odd = (scaled_0, high_0, mean_0), (scaled_1, high_1, mean_1)

    @pl.when(lax.rem(step, 2) == 0)
    def _():
        work(*even, odd)

    @pl.when(lax.rem(step, 2) == 1)
    def _():
        work(*odd, even)

    @pl.when(step == 3)
    def _():
        cross()

    for at, event in ((4, ring.first), (7, ring.second), (8, ring.middle)):
        pl.when(step == at)(event)
    for at, block in ((11, 1), (14, 2)):
        pl.when(step == at)(functools.partial(ring.third, block))

    @pl.when(step == steps - 1)
    def _():
        wide = win_ref[...].astype(F32)
        center = wide - jnp.mean(wide, axis=1, keepdims=True)
        high, low = split_two(center * gain_ref[...])
        scaled_0[0:C, :] = high
        scaled_0[C : 2 * C, :] = low
        for into, weight in ((aq_ref, wq_ref), (akv_ref, wkv)):
            both = dot(scaled_0[0 : 2 * C, :], weight[...])
            high, low = split_two(both[:C] + both[C:])
            into[0:C, :] = high
            into[C : 2 * C, :] = low
        ring.third(3)
        high, low = split_two(center)
        high_0[0:C, :] = high
        high_1[0:C, :] = low
        high, low = high_0[0:C, :], high_1[0:C, :]
        high, low = split_two(dot_t(high, high) + dot_t(high, low) + dot_t(low, high))
        g_ref[0:C, :] = high
        g_ref[C : 2 * C, :] = low
        end()
        edge.wait()
        each("start", results)
        ring.end()
        each("wait", results)


def ring_scratch():
    return [
        pltpu.SemaphoreType.DMA,
        pltpu.SemaphoreType.DMA((40,)),
        pltpu.SemaphoreType.DMA((40,)),
    ]


def first(rows, blocks, places, latent, gain, w_query, w_key, w_value, w_in, up):
    freq = frequencies()
    scale = jnp.array([rows, 16.0, 1.0], F32)[:, None] * jnp.arange(16, dtype=F32)[None, :]
    angles = scale[:, :, None] * freq[None, None, :]
    sines, cosines = jnp.sin(angles), jnp.cos(angles)
    turn = jnp.stack([sines[0], cosines[0]], axis=1)
    fine_a = jnp.stack([sines[1], cosines[1]], axis=1)
    fine_b = jnp.stack([sines[2], cosines[2]], axis=0)
    return first_call(rows, blocks, places, latent, turn, fine_a, fine_b, gain, w_query, w_key,
                      w_value, w_in, up)


def first_call(rows, blocks, places, latent, turn, fine_a, fine_b, gain, w_query, w_key, w_value,
               w_in, up):
    width = w_key.shape[1]
    length = rows * blocks
    whole = pl.BlockSpec(memory_space=pltpu.VMEM)
    far = pl.BlockSpec(memory_space=pltpu.HBM)
    return pl.pallas_call(
        functools.partial(first_kernel, rows),
        grid=(blocks,),
        in_specs=[whole] * 6 + [far, far, whole, far],
        out_specs=[
            pl.BlockSpec((rows, 2 * width), lambda i: (i, 0)),
            pl.BlockSpec((rows, C), lambda i: (i, 0)),
            pl.BlockSpec((rows, 1), lambda i: (i, 0)),
        ]
        + [far] * 7,
        out_shape=[
            jax.ShapeDtypeStruct((length, 2 * width), F32),
            jax.ShapeDtypeStruct((length, C), F32),
            jax.ShapeDtypeStruct((length, 1), F32),
            jax.ShapeDtypeStruct((rows, width), F32),
            jax.ShapeDtypeStruct((2 * C, width), BF16),
            jax.ShapeDtypeStruct((2 * C, 2 * width), BF16),
            jax.ShapeDtypeStruct((2 * C, C), BF16),
            jax.ShapeDtypeStruct((places, 2, rows // 8, C), BF16),
            jax.ShapeDtypeStruct((8, C), F32),
            jax.ShapeDtypeStruct((blocks, *up.shape), BF16),
        ],
        scratch_shapes=[
            pltpu.VMEM((rows, width), F32),
            pltpu.VMEM((2 * C, width), BF16),
            pltpu.VMEM((2 * C, 2 * width), BF16),
            pltpu.VMEM((2 * C, C), BF16),
            pltpu.VMEM((places, 2, rows // 8, C), BF16),
            pltpu.VMEM((8, C), F32),
            pltpu.SemaphoreType.DMA((6,)),
            pltpu.VMEM(up.shape, BF16),
        ]
        + [pltpu.VMEM((rows, D), BF16)] * 4
        + [pltpu.VMEM((rows, 1), F32)] * 2
        + [
            pltpu.VMEM((2, rows, HALF), F32),
            pltpu.VMEM((D, 2 * width), BF16),
            pltpu.VMEM((16, 3 * width), F32),
            pltpu.VMEM((16, C), F32),
            pltpu.VMEM((8, C), F32),
            pltpu.SemaphoreType.DMA((3,)),
            pltpu.SemaphoreType.DMA((3,)),
            pltpu.SemaphoreType.DMA((3,)),
        ]
        + ring_scratch(),
        compiler_params=pltpu.CompilerParams(
            collective_id=0, has_side_effects=True, vmem_limit_bytes=56 << 20
        ),
        cost_estimate=pl.CostEstimate(
            flops=60_000_000_000, bytes_accessed=40_000_000, transcendentals=0
        ),
        name="first",
    )(latent, turn, fine_a, fine_b, gain, w_query, w_key, w_value, w_in, up)


def reduce_over_head(produce, meanwhile, between, term, taken, via_out, via_in, near, fin, send, recv):
    _, y, c = seat()
    partner, up, down = 2 * y + 1 - c, 2 * plus(y, 1) + c, 2 * plus(y, 3) + c

    def copy(src, dst, slot, head):
        return pltpu.make_async_remote_copy(
            src_ref=src, dst_ref=dst, send_sem=send.at[slot], recv_sem=recv.at[slot],
            device_id={"head": head}, device_id_type=MESH,
        )

    def pair(half, at):
        return term[half, at, c].astype(F32) + taken[half, at].astype(F32)

    across, ahead, behind = plus(y, 2), plus(y, 1), plus(y, 3)
    gives = [copy(term.at[half, :, 1 - c], taken.at[half], half, partner) for half in range(2)]
    produce(0, 0)
    produce(0, 1)
    gives[0].start()
    produce(1, 0)
    gives[0].wait_recv()
    via_out[0] = pair(0, across).astype(BF16)
    via_0 = copy(via_out.at[0], via_in.at[0], 2, up)
    via_0.start()
    near[1, 0] = pair(0, behind).astype(BF16)
    down_0 = copy(near.at[1, 0], fin.at[1, 0], 6, down)
    down_0.start()
    produce(1, 1)
    gives[1].start()
    meanwhile()
    gives[1].wait_recv()
    via_out[1] = pair(1, across).astype(BF16)
    via_1 = copy(via_out.at[1], via_in.at[1], 3, down)
    via_1.start()
    near[0, 1] = pair(1, ahead).astype(BF16)
    up_1 = copy(near.at[0, 1], fin.at[0, 1], 5, up)
    up_1.start()
    via_0.wait_recv()
    near[0, 0] = (pair(0, ahead) + via_in[0].astype(F32)).astype(BF16)
    up_0 = copy(near.at[0, 0], fin.at[0, 0], 4, up)
    up_0.start()
    via_1.wait_recv()
    near[1, 1] = (pair(1, behind) + via_in[1].astype(F32)).astype(BF16)
    down_1 = copy(near.at[1, 1], fin.at[1, 1], 7, down)
    down_1.start()
    between()
    sums = [pair(half, y) for half in range(2)]
    down_0.wait_recv()
    up_0.wait_recv()
    first = sums[0] + fin[0, 0].astype(F32) + fin[1, 0].astype(F32)
    up_1.wait_recv()
    down_1.wait_recv()
    second = sums[1] + fin[0, 1].astype(F32) + fin[1, 1].astype(F32)
    for done in (*gives, via_0, via_1, up_0, up_1, down_0, down_1):
        done.wait_send()
    return jnp.concatenate([first, second], axis=1)


def gather_over_head(out, send, recv, midway=lambda: None):
    _, y, c = seat()
    partner, up, down = 2 * y + 1 - c, 2 * plus(y, 1) + c, 2 * plus(y, 3) + c
    across, ahead, behind = plus(y, 2), plus(y, 1), plus(y, 3)
    low, high = pl.ds(0, HALF), pl.ds(HALF, HALF)

    def copy(block, slot, head):
        return pltpu.make_async_remote_copy(
            src_ref=block, dst_ref=block, send_sem=send.at[slot], recv_sem=recv.at[slot],
            device_id={"head": head}, device_id_type=MESH,
        )

    moves = [copy(out.at[y, c], 0, up), copy(out.at[y, c], 1, down), copy(out.at[y, c], 2, partner)]
    for move in moves:
        move.start()

    def then(slot, *following):
        moves[slot].wait_recv()
        for move in following:
            move.start()
            moves.append(move)

    then(0, copy(out.at[behind, c, :, low], 3, up), copy(out.at[behind, c], 4, partner))
    then(1, copy(out.at[ahead, c, :, high], 5, down), copy(out.at[ahead, c], 6, partner))
    midway()
    then(3, copy(out.at[across, c, :, low], 7, partner))
    then(5, copy(out.at[across, c, :, high], 8, partner))
    for slot in (2, 4, 6, 7, 8):
        moves[slot].wait_recv()
    for move in moves:
        move.wait_send()


def reduce_scratch(share):
    return [
        pltpu.VMEM((2, 4, 2, share, HALF), BF16),
        pltpu.VMEM((2, 4, share, HALF), BF16),
        pltpu.VMEM((2, share, HALF), BF16),
        pltpu.VMEM((2, share, HALF), BF16),
        pltpu.VMEM((2, 2, share, HALF), BF16),
        pltpu.VMEM((2, 2, share, HALF), BF16),
        pltpu.SemaphoreType.DMA((8,)),
        pltpu.SemaphoreType.DMA((8,)),
    ]


def head_neighbours():
    _, y, c = seat()
    return [{"head": 2 * y + 1 - c}, {"head": 2 * plus(y, 1) + c}, {"head": 2 * plus(y, 3) + c}]


def store_terms(term, half, at, share, value):
    for block in range(8):
        rows = value[block * share : (block + 1) * share].astype(BF16)
        term[half, block // 2, block % 2, :, at : at + value.shape[1]] = rows


def block_kernel(rows, heads, ringed, *refs):
    kv_ref, *refs = refs
    sources, refs = refs[:11], refs[11:]
    if ringed:
        shard_ref, stream_out, normed_out, full_ref, *refs = refs
        *refs, shard, load, local, gsend, grecv = refs
        ring = RingGather(shard, full_ref, local, gsend, grecv)
        fetch = pltpu.make_async_copy(shard_ref, shard, load)
    else:
        stream_out, normed_out, *refs = refs
    places, refs, loads = refs[:11], refs[12:], refs[11]
    (
        x_ref, h_ref, n_ref, eq_ref, aq_ref, akv_ref, g_ref,
        win_ref, wo_ref, embedding_ref, gain_ref,
    ) = places
    inputs = staged(zip(sources, places), loads)
    stream_ref, normed_ref, outs, queries, acc, sums, attended, *parts, send, recv = refs
    term = parts[0]
    share = rows // 8
    width = heads * HEAD_DIM
    block = pl.program_id(0)
    me, y, c = seat()

    greeted = head_neighbours() + (ring.neighbours() if ringed else [])
    results = staged([(stream_ref, stream_out), (normed_ref, normed_out)], outs)

    def scale_of(x, h, n):
        twice = jnp.concatenate([x, x], axis=1)
        quad = jnp.sum(x.astype(F32) * (dot(twice, g_ref[...]) + 2.0 * h), axis=1, keepdims=True)
        return twice, lax.rsqrt(jnp.maximum(quad + n, 0.0) * (1.0 / D) + EPSILON)

    @pl.when(block == 0)
    def _():
        if ringed:
            fetch.start()
        each("start", inputs)
        hail(greeted)
        if ringed:
            met(greeted)
            fetch.wait()
            ring.begin()
        each("wait", inputs[:7])
        own = pl.ds(pl.multiple_of(me * rows, rows), rows)
        twice, scale = scale_of(x_ref[own, :], h_ref[own, :], n_ref[own, :])
        value = (dot(twice, aq_ref[...]) + eq_ref[...]) * (scale * HEAD_DIM**-0.5)
        queries[...] = value.astype(BF16)
        acc[...] = jnp.zeros_like(acc)
        sums[...] = jnp.zeros_like(sums)

    def step(masked):
        here = pl.ds(pl.multiple_of(block * KEY_BLOCK, KEY_BLOCK), KEY_BLOCK)
        twice, scale = scale_of(x_ref[here, :], h_ref[here, :], n_ref[here, :])
        both = ((dot(twice, akv_ref[...]) + kv_ref[...]) * scale).astype(BF16)
        keys, values = both[:, :width], both[:, width:]
        if masked:
            shape = (rows, KEY_BLOCK)
            row = me * rows + lax.broadcasted_iota(jnp.int32, shape, 0)
            col = block * KEY_BLOCK + lax.broadcasted_iota(jnp.int32, shape, 1)
            seen = col <= row
        for head in range(heads):
            cols = slice(head * HEAD_DIM, (head + 1) * HEAD_DIM)
            scores = dot_t(queries[:, cols], keys[:, cols])
            if masked:
                weights = jnp.where(seen, jnp.exp(jnp.where(seen, scores, 0.0)), 0.0)
            else:
                weights = jnp.exp(scores)
            part = weights[:, :HEAD_DIM]
            for at in range(HEAD_DIM, KEY_BLOCK, HEAD_DIM):
                part = part + weights[:, at : at + HEAD_DIM]
            sums[:, cols] += part
            acc[:, cols] += dot(weights.astype(BF16), values[:, cols])

    final = (me * rows + rows - 1) // KEY_BLOCK

    @pl.when(block < final)
    def _():
        step(False)

    @pl.when(block == final)
    def _():
        step(True)

    def produce(half, part):
        at = part * (HALF // 2)
        cols = slice(half * HALF + at, half * HALF + at + HALF // 2)
        store_terms(term, half, at, share, dot(attended[...], wo_ref[:, cols]))

    def meanwhile():
        first = pl.ds(pl.multiple_of(me * rows + (2 * y + c) * share, share), share)
        stream_ref[...] = dot(x_ref[first, :], win_ref[...]) + embedding_ref[...]

    def between():
        if ringed:
            ring.second()
            ring.middle()

    def midway():
        if ringed:
            ring.third(2)

    @pl.when(block == pl.num_programs(0) - 1)
    def _():
        for head in range(heads):
            cols = slice(head * HEAD_DIM, (head + 1) * HEAD_DIM)
            total = jnp.sum(sums[:, cols], axis=1, keepdims=True)
            attended[:, cols] = (acc[:, cols] / total).astype(BF16)
        each("wait", inputs[7:])
        if ringed:
            ring.first()
        else:
            met(greeted)
        total = reduce_over_head(produce, meanwhile, between, *parts)
        stream = stream_ref[...] + total
        stream_ref[...] = stream
        results[0].start()
        normed_ref[y, c] = layer_norm(stream, gain_ref[...]).astype(BF16)
        if ringed:
            ring.third(1)
        gather_over_head(normed_ref, send, recv, midway)
        results[1].start()
        if ringed:
            ring.third(3)
            ring.end()
        each("wait", results)


def block_step(rows, state, x, embedding, w_in, w_attn_out, gain, shard=None):
    kv = state[0]
    length, width = kv.shape[0], kv.shape[1] // 2
    share = rows // 8
    ringed = shard is not None
    far = pl.BlockSpec(memory_space=pltpu.HBM)
    tile = pl.BlockSpec((KEY_BLOCK, 2 * width), lambda i: (i, 0))
    more = [shard] if ringed else []
    sources = [x, *state[1:], w_in, w_attn_out, embedding, gain]
    outs = [
        jax.ShapeDtypeStruct((share, D), F32),
        jax.ShapeDtypeStruct((4, 2, share, D), BF16),
    ]
    if ringed:
        outs.append(jax.ShapeDtypeStruct((length // rows, *shard.shape), BF16))
    return pl.pallas_call(
        functools.partial(block_kernel, rows, width // HEAD_DIM, ringed),
        grid=(length // KEY_BLOCK,),
        in_specs=[tile] + [far] * (11 + ringed),
        out_specs=[far] * (2 + ringed),
        out_shape=outs,
        scratch_shapes=[buffer_like(source) for source in sources]
        + [
            pltpu.SemaphoreType.DMA((11,)),
            pltpu.VMEM((share, D), F32),
            pltpu.VMEM((4, 2, share, D), BF16),
            pltpu.SemaphoreType.DMA((2,)),
            pltpu.VMEM((rows, width), BF16),
            pltpu.VMEM((rows, width), F32),
            pltpu.VMEM((rows, width), F32),
            pltpu.VMEM((rows, width), BF16),
        ]
        + reduce_scratch(share)
        + [pltpu.SemaphoreType.DMA((9,)), pltpu.SemaphoreType.DMA((9,))]
        + ([pltpu.VMEM(shard.shape, BF16), pltpu.SemaphoreType.DMA] + ring_scratch() if ringed else []),
        compiler_params=pltpu.CompilerParams(
            collective_id=1 if ringed else 4, has_side_effects=True, vmem_limit_bytes=56 << 20
        ),
        cost_estimate=pl.CostEstimate(
            flops=30_000_000_000, bytes_accessed=20_000_000, transcendentals=0
        ),
        name="block_ring" if ringed else "block",
    )(kv, *sources, *more)


def mlp_kernel(
    share, last, up_ref, down_ref, *refs,
):
    sources, out_ref, refs = refs[:5], refs[5], refs[6:]
    places, (up, down, hidden, loads, smalls, *scratch) = refs[:5], refs[5:]
    normed_ref, stream_ref, gain_ref, wf_ref, ahead_ref = places
    *parts, send, recv = scratch
    term = parts[0]
    seq, y, c = seat()
    ups, downs = up.shape[0], down.shape[0]
    wide, tall = up.shape[2], down.shape[1]
    fetches = [
        pltpu.make_async_copy(up_ref.at[:, pl.ds(k * wide, wide)], up.at[k], loads.at[k])
        for k in range(ups)
    ] + [
        pltpu.make_async_copy(
            down_ref.at[pl.ds(k * tall, tall), :], down.at[k], loads.at[ups + k]
        )
        for k in range(downs)
    ]
    inputs = staged(zip(sources, places), smalls)
    inputs[0].start()
    each("start", fetches)
    each("start", inputs[1:])

    def raise_hidden():
        inputs[0].wait()
        for k in range(ups):
            fetches[k].wait()
            pre = dot(normed_ref[...], up[k])
            hidden[:, k * wide : (k + 1) * wide] = jax.nn.gelu(pre, approximate=True).astype(BF16)

    if last:
        mirror = lax.axis_size("seq") - 1 - seq
        sends_edge = jnp.logical_and(mirror > 0, 2 * y + c == 7)
        keeps_edge = jnp.logical_and(mirror - 1 == seq, 2 * y + c == 7)
        waits_edge = jnp.logical_and(mirror > 0, jnp.logical_not(keeps_edge))
        barrier = pltpu.get_barrier_semaphore()
        hail(head_neighbours() + [{"seq": mirror, "head": head} for head in range(8)])

        @pl.when(waits_edge)
        def _():
            pl.semaphore_signal(
                barrier, inc=1, device_id={"seq": mirror - 1, "head": 7}, device_id_type=MESH
            )

        raise_hidden()

        @pl.when(keeps_edge)
        def _():
            pl.semaphore_wait(barrier, 18)

        @pl.when(jnp.logical_and(sends_edge, jnp.logical_not(keeps_edge)))
        def _():
            pl.semaphore_wait(barrier, 19)

        @pl.when(jnp.logical_not(sends_edge))
        def _():
            pl.semaphore_wait(barrier, 11)

    else:
        greet_all(out_ref.shape[0], raise_hidden)

    def produce(half, part):
        k = half * (downs // 2) + part
        fetches[ups + k].wait()
        store_terms(term, half, part * tall, share, dot_t(hidden[...], down[k]))

    total = reduce_over_head(produce, lambda: None, lambda: each("wait", inputs[1:]), *parts)
    normed = layer_norm(stream_ref[...] + total, gain_ref[...]).astype(BF16)
    params = dot(normed, wf_ref[...])
    following = ahead_ref[...] * jnp.exp(jnp.tanh(params[:, C:])) + params[:, :C]
    if not last:
        out_ref[seq * 4 + y, c] = following.astype(BF16)
        begin, cross, end = spread(out_ref, send, recv)
        begin()
        cross()
        end()
    else:
        block = scratch[0].at[0, 0, 0, :, pl.ds(0, C)]
        block[...] = following.astype(BF16)
        head = 2 * y + c
        moves = [
            pltpu.make_async_remote_copy(
                src_ref=block, dst_ref=out_ref.at[head], send_sem=send.at[k], recv_sem=recv.at[0],
                device_id={"seq": mirror, "head": k}, device_id_type=MESH,
            )
            for k in range(8)
        ]
        edges = [
            pltpu.make_async_remote_copy(
                src_ref=block, dst_ref=out_ref.at[8], send_sem=send.at[8 + k], recv_sem=recv.at[1],
                device_id={"seq": mirror - 1, "head": k}, device_id_type=MESH,
            )
            for k in range(8)
        ]
        for move in moves:
            move.start()

        @pl.when(sends_edge)
        def _():
            for move in edges[:7]:
                move.start()

        @pl.when(jnp.logical_and(sends_edge, jnp.logical_not(keeps_edge)))
        def _():
            edges[7].start()

        whole = out_ref.at[pl.ds(0, 8)]
        pltpu.make_async_remote_copy(
            src_ref=whole, dst_ref=whole, send_sem=send.at[0], recv_sem=recv.at[0],
            device_id={"seq": mirror, "head": 0}, device_id_type=MESH,
        ).wait_recv()

        @pl.when(waits_edge)
        def _():
            pltpu.make_async_remote_copy(
                src_ref=block, dst_ref=out_ref.at[8], send_sem=send.at[0], recv_sem=recv.at[1],
                device_id={"seq": mirror - 1, "head": 7}, device_id_type=MESH,
            ).wait_recv()

        for move in moves:
            move.wait_send()

        @pl.when(sends_edge)
        def _():
            for move in edges[:7]:
                move.wait_send()

        @pl.when(jnp.logical_and(sends_edge, jnp.logical_not(keeps_edge)))
        def _():
            edges[7].wait_send()

        @pl.when(jnp.logical_not(waits_edge))
        def _():
            out_ref[8] = following.astype(BF16)


def mlp(share, places, last, normed, up, down, stream, gain, w_final, ahead):
    whole = pl.BlockSpec(memory_space=pltpu.VMEM)
    rows, width = normed.shape[0], up.shape[1]
    sources = [normed, stream, gain, w_final, ahead]
    shape = (9, share, C) if last else (places, 2, share, C)
    return pl.pallas_call(
        functools.partial(mlp_kernel, share, last),
        in_specs=[pl.BlockSpec(memory_space=pltpu.HBM)] * 7,
        out_specs=whole,
        out_shape=jax.ShapeDtypeStruct(shape, BF16),
        scratch_shapes=[buffer_like(source) for source in sources]
        + [
            pltpu.VMEM((3, D, width // 3), BF16),
            pltpu.VMEM((4, D // 4, width), BF16),
            pltpu.VMEM((rows, width), BF16),
            pltpu.SemaphoreType.DMA((7,)),
            pltpu.SemaphoreType.DMA((5,)),
        ]
        + reduce_scratch(share)
        + [pltpu.SemaphoreType.DMA((16,)), pltpu.SemaphoreType.DMA((2,))],
        compiler_params=pltpu.CompilerParams(
            collective_id=3 if last else 2, has_side_effects=True, vmem_limit_bytes=56 << 20
        ),
        cost_estimate=pl.CostEstimate(
            flops=40_000_000_000, bytes_accessed=30_000_000, transcendentals=0
        ),
        name="mlp_last" if last else "mlp",
    )(up, down, *sources)


def per_device(
    latent, w_in, w_query, w_key, w_value, w_attn_out, w_up, w_down, w_final,
    gain_attn, gain_mlp, gain_final,
):
    seq_count, head_count = lax.axis_size("seq"), lax.axis_size("head")
    me, mine = lax.axis_index("seq"), lax.axis_index("head")
    rows = latent.shape[0]
    share = rows // head_count
    length = rows * seq_count
    places = seq_count * head_count // 2
    start = me * rows + mine * share

    shape = (2, w_up.shape[0] // 2, w_up.shape[1])
    *state, gathered, edge, up = first(
        rows, seq_count, places, latent, gain_attn[None, :], w_query, w_key, w_value, w_in,
        w_up.reshape(shape),
    )
    up = up.reshape(D, w_up.shape[1])
    x = gathered.reshape(length, C)
    angles = (start + jnp.arange(share)).astype(F32)[:, None] * frequencies()[None, :]
    embedding = jnp.concatenate([jnp.sin(angles), jnp.cos(angles)], axis=1)
    ahead = lax.dynamic_slice_in_dim(
        jnp.concatenate([latent[1:], edge[:1]], axis=0), mine * share, share, 0
    )
    top = x[:1]
    for step_index in range(ITERS):
        last = step_index == ITERS - 1
        stream, normed, *full = block_step(
            rows, state, x, embedding, w_in, w_attn_out, gain_mlp[None, :],
            w_down.T.reshape(shape) if step_index == 0 else None,
        )
        if step_index == 0:
            down = full[0].reshape(D, w_up.shape[1])
        following = mlp(
            share, places, last, normed.reshape(rows, D), up, down, stream, gain_final[None, :],
            w_final, ahead,
        )
        if not last:
            x = jnp.concatenate([top, following.reshape(length, C)[:-1]], axis=0)
    edge = jnp.where(me == seq_count - 1, top, following[8, share - 1 :])
    result = jnp.concatenate([edge, following[:8].reshape(rows, C)[:-1]], axis=0)
    return result[::-1].astype(F32)


def solution(mesh):
    in_specs = (
        P("seq", None),
        P(),
        P(None, "head"),
        P(None, "head"),
        P(None, "head"),
        P("head", None),
        P("seq", "head"),
        P("head", "seq"),
        P(),
        P(),
        P(),
        P(),
    )
    return jax.shard_map(
        per_device, mesh=mesh, in_specs=in_specs, out_specs=P("seq", None), check_vma=False
    )
```

```python
import functools

import jax
import jax.numpy as jnp
from jax import lax
from jax.experimental import pallas as pl
from jax.experimental.pallas import tpu as pltpu
from jax.sharding import PartitionSpec as P

D = 3072
HALF = D // 2
HEAD_DIM = 128
C = 128
ITERS = 2
EPSILON = 1e-05
KEY_BLOCK = 512
BF16 = jnp.bfloat16
F32 = jnp.float32


def split_two(value):
    high = value.astype(BF16)
    return high, (value - high.astype(F32)).astype(BF16)


def dot(left, right):
    return jnp.dot(left, right, preferred_element_type=F32)


def dot_t(left, right):
    return lax.dot_general(left, right, (((1,), (1,)), ((), ())), preferred_element_type=F32)


def layer_norm(stream, gain):
    center = stream - jnp.mean(stream, axis=-1, keepdims=True)
    spread = jnp.mean(center * center, axis=-1, keepdims=True)
    return center * lax.rsqrt(spread + EPSILON) * gain


def frequencies():
    return jnp.exp(-jnp.log(10000.0) * 2.0 * jnp.arange(HALF).astype(F32) / D)


MESH = pl.DeviceIdType.MESH


def staged(pairs, sems):
    return [pltpu.make_async_copy(src, dst, sems.at[k]) for k, (src, dst) in enumerate(pairs)]


def each(action, copies):
    for copy in copies:
        getattr(copy, action)()


def buffer_like(array):
    return pltpu.VMEM(array.shape, array.dtype)


def seat():
    head = lax.axis_index("head")
    return lax.axis_index("seq"), lax.div(head, 2), lax.rem(head, 2)


def plus(y, by):
    return lax.rem(y + by, 4)


def hail(targets):
    barrier = pltpu.get_barrier_semaphore()
    for target in targets:
        pl.semaphore_signal(barrier, inc=1, device_id=target, device_id_type=MESH)


def met(targets):
    pl.semaphore_wait(pltpu.get_barrier_semaphore(), len(targets))


def hail_all(devices):
    seq, y, c = seat()
    place = seq * 4 + y
    barrier = pltpu.get_barrier_semaphore()
    pl.semaphore_signal(barrier, inc=1, device_id={"head": 2 * y + 1 - c}, device_id_type=MESH)

    @pl.loop(1, devices)
    def _(k):
        other = lax.rem(place + k, devices)
        pl.semaphore_signal(
            barrier, inc=1,
            device_id={"seq": lax.div(other, 4), "head": 2 * lax.rem(other, 4) + c},
            device_id_type=MESH,
        )


def start_peers(count):
    seq, y, c = seat()
    return (
        [{"seq": lax.rem(seq + k, count)} for k in range(1, count)]
        + [{"head": 2 * plus(y, k) + c} for k in range(1, 4)]
        + [{"head": 2 * y + 1 - c}]
    )


def start_spread(buffer, send, recv):
    seq, y, c = seat()
    count = buffer.shape[0]

    def copy(block, slot, device):
        return pltpu.make_async_remote_copy(
            src_ref=block, dst_ref=block, send_sem=send.at[slot], recv_sem=recv.at[slot],
            device_id=device, device_id_type=MESH,
        )

    partner = {"head": 2 * y + 1 - c}
    plane = copy(buffer.at[pl.ds(0, count - 1), 0, c], 0, partner)
    column = copy(buffer.at[:, pl.ds(0, 3), c], 1, partner)
    across = copy(buffer.at[:, :, c], 2, partner)

    def begin():
        @pl.loop(1, count)
        def _(k):
            copy(buffer.at[seq, y, c], 0, {"seq": lax.rem(seq + k, count)}).start()

    def columns():
        plane.wait_recv()
        for k in range(1, 4):
            copy(buffer.at[:, y, c], 1, {"head": 2 * plus(y, k) + c}).start()

    def cross():
        column.wait_recv()
        across.start()

    def end():
        plane.wait_send()
        column.wait_send()
        across.wait()

    return begin, columns, cross, end


def spread(buffer, send, recv):
    seq, y, c = seat()
    devices = buffer.shape[0]
    place = seq * 4 + y
    partner = {"head": 2 * y + 1 - c}
    whole = buffer.at[pl.ds(0, devices - 1), c]
    arrived = pltpu.make_async_remote_copy(
        src_ref=whole, dst_ref=whole, send_sem=send.at[0], recv_sem=recv.at[0],
        device_id=partner, device_id_type=MESH,
    )
    across = pltpu.make_async_remote_copy(
        src_ref=buffer.at[:, c], dst_ref=buffer.at[:, c], send_sem=send.at[1], recv_sem=recv.at[1],
        device_id=partner, device_id_type=MESH,
    )

    def begin():
        @pl.loop(1, devices)
        def _(k):
            other = lax.rem(place + k, devices)
            pltpu.make_async_remote_copy(
                src_ref=buffer.at[place, c], dst_ref=buffer.at[place, c],
                send_sem=send.at[0], recv_sem=recv.at[0],
                device_id={"seq": lax.div(other, 4), "head": 2 * lax.rem(other, 4) + c},
                device_id_type=MESH,
            ).start()

    def cross():
        arrived.wait_recv()
        across.start()

    def end():
        arrived.wait_send()
        across.wait()

    return begin, cross, end


class RingGather:
    FIRST = (0, 3, 1, 2)

    def __init__(self, own, out, local, send, recv):
        seq = lax.axis_index("seq")
        self.x, self.z = lax.div(seq, 4), lax.rem(seq, 4)
        self.own, self.out, self.send, self.recv = own, out, send, recv
        self.keep = pltpu.make_async_copy(own, out.at[seq], local)

    def place(self, half, p, q):
        x, z = (p, q) if half == 0 else (q, p)
        return plus(self.x, x) * 4 + plus(self.z, z)

    def move(self, half, slot):
        if slot < 4:
            kind, block, target = slot, None, [(1, 0), (3, 0), (1, 0), (3, 0)][slot]
            origin = [(0, 0), (0, 0), (3, 0), (1, 0)][slot]
        else:
            block, kind = divmod(slot - 4, 4)
            target = [(0, 1), (0, 3), (0, 1), (0, 3)][kind]
            origin = (self.FIRST[block], [0, 0, 3, 1][kind])
        ref = self.out.at[self.place(half, *origin), half]
        if kind >= 2:
            part = ref.shape[0] // 2
            ref = ref.at[pl.ds((kind - 2) * part, part)]
        source = self.own.at[half] if origin == (0, 0) else ref
        return pltpu.make_async_remote_copy(
            src_ref=source, dst_ref=ref,
            send_sem=self.send.at[20 * half + slot], recv_sem=self.recv.at[20 * half + slot],
            device_id={"seq": self.place(half, *target)}, device_id_type=MESH,
        )

    def neighbours(self):
        return [{"seq": self.place(0, *at)} for at in ((1, 0), (3, 0), (0, 1), (0, 3))]

    def on(self, slots, *following):
        for half in range(2):
            for slot in slots:
                self.move(half, slot).wait_recv()
            for slot in following:
                self.move(half, slot).start()

    def begin(self):
        self.keep.start()
        self.on((), 0, 1)
        self.on((), 4, 5)

    def first(self):
        self.on((0,), 2, 8, 9)
        self.on((1,), 3, 12, 13)

    def second(self):
        self.on((4,), 6)
        self.on((5,), 7)

    def middle(self):
        self.on((2, 3), 16, 17)

    def third(self, block):
        self.on((4 + 4 * block,), 6 + 4 * block)
        self.on((5 + 4 * block,), 7 + 4 * block)

    def end(self):
        self.on((6, 7, 10, 11, 14, 15, 18, 19))
        self.keep.wait()
        for half in range(2):
            for slot in range(20):
                self.move(half, slot).wait_send()


def first_kernel(
    rows, latent_ref, turn_ref, fine_a, fine_b, gain_ref, wq_ref, wk_ref, wv_ref, win_ref, up_ref,
    kv_ref, h_ref, n_ref, eq_out, aq_out, akv_out, g_out, x_out, edge_out, full_ref,
    eq_ref, aq_ref, akv_ref, g_ref, x_ref, edge_ref, stores, shard, scaled_0, scaled_1, high_0, high_1, mean_0, mean_1, base, wkv, gw, wsum, edge_rows,
    loads, xsend, xrecv, local, gsend, grecv,
):
    step, steps = pl.program_id(0), pl.num_programs(0)
    seq, y, c = seat()
    width = wk_ref.shape[1]
    fetches = [
        pltpu.make_async_copy(ref, wkv.at[:, pl.ds(k * width, width)], loads.at[k])
        for k, ref in enumerate((wk_ref, wv_ref))
    ]
    begin, columns, cross, end = start_spread(x_ref, xsend, xrecv)
    count = lax.axis_size("seq")
    edge = pltpu.make_async_remote_copy(
        src_ref=edge_rows, dst_ref=edge_ref, send_sem=xsend.at[3], recv_sem=xrecv.at[3],
        device_id={"seq": lax.rem(seq + count - 1, count)}, device_id_type=MESH,
    )
    ring = RingGather(shard, full_ref, local, gsend, grecv)
    fetches.append(pltpu.make_async_copy(up_ref, shard, loads.at[2]))
    results = staged(
        [
            (eq_ref, eq_out), (aq_ref, aq_out), (akv_ref, akv_out), (g_ref, g_out),
            (x_ref, x_out), (edge_ref, edge_out),
        ],
        stores,
    )

    def fill(block, scaled, high, mean):
        total = jnp.zeros((rows, 1), F32)
        wide = 512
        for at in range(0, HALF, wide):
            cols = slice(at, at + wide)
            sin_a, cos_a = turn_ref[block, 0:1, cols], turn_ref[block, 1:2, cols]
            sin_b, cos_b = base[0, :, cols], base[1, :, cols]
            for part, offset in (
                (sin_a * cos_b + cos_a * sin_b, 0),
                (cos_a * cos_b - sin_a * sin_b, HALF),
            ):
                into = slice(offset + at, offset + at + wide)
                high[:, into] = part.astype(BF16)
                scaled[:, into] = (part * gain_ref[:, into]).astype(BF16)
                total = total + jnp.sum(part, axis=1, keepdims=True)
        mean[...] = total * (1.0 / D)

    def rows_out():
        edge_rows[...] = latent_ref[0:8, :]
        own = pl.ds(pl.multiple_of((2 * y + c) * (rows // 8), rows // 8), rows // 8)
        x_ref[seq, y, c] = latent_ref[own, :].astype(BF16)

    def tables():
        @pl.loop(0, rows // 16)
        def _(k):
            sin_a, cos_a = fine_a[k, 0:1, :], fine_a[k, 1:2, :]
            sin_b, cos_b = fine_b[0], fine_b[1]
            into = pl.ds(pl.multiple_of(k * 16, 16), 16)
            base[0, into, :] = sin_a * cos_b + cos_a * sin_b
            base[1, into, :] = cos_a * cos_b - sin_a * sin_b

        wsum[...] = dot_t(jnp.ones((16, D), BF16), win_ref[...])
        gain = gain_ref[...]
        high = gain.astype(BF16).astype(F32)
        line = lax.broadcasted_iota(jnp.int32, (16, D), 0)
        both = jnp.where(line == 0, high, jnp.where(line == 1, gain - high, 0.0)).astype(BF16)
        for fetch in fetches[:2]:
            fetch.wait()
        gw[:, 0:width] = dot(both, wq_ref[...])
        gw[:, width:] = dot(both, wkv[...])
        gw[0:1, :] = jnp.sum(gw[...], axis=0, keepdims=True)

    @pl.when(step == 0)
    def _():
        fetches[2].start()
        peers = start_peers(count)
        hail(peers)
        rows_out()
        for fetch in fetches[:2]:
            fetch.start()
        fetches[2].wait()
        met(peers)
        ring.begin()
        begin()
        edge.start()
        tables()
        fill(0, scaled_0, high_0, mean_0)

    def work(scaled, high, mean, others):
        value = mean[...]
        kv_ref[...] = dot(scaled[...], wkv[...]) - value * gw[0:1, width:]
        h_ref[...] = dot_t(high[...], win_ref[...]) - value * wsum[0:1, :]
        n_ref[...] = HALF - D * value * value
        fill(jnp.minimum(step + 1, steps - 1), *others)

        @pl.when(step == seq)
        def _():
            eq_ref[...] = dot(scaled[...], wq_ref[...]) - value * gw[0:1, 0:width]

    even, odd = (scaled_0, high_0, mean_0), (scaled_1, high_1, mean_1)

    @pl.when(lax.rem(step, 2) == 0)
    def _():
        work(*even, odd)

    @pl.when(lax.rem(step, 2) == 1)
    def _():
        work(*odd, even)

    pl.when(step == 3)(columns)
    pl.when(step == 6)(cross)

    for at, event in ((3, ring.first), (7, ring.second), (9, ring.middle)):
        pl.when(step == at)(event)
    for at, block in ((12, 1), (15, 2)):
        pl.when(step == at)(functools.partial(ring.third, block))

    @pl.when(step == steps - 1)
    def _():
        wide = win_ref[...].astype(F32)
        center = wide - jnp.mean(wide, axis=1, keepdims=True)
        high, low = split_two(center * gain_ref[...])
        scaled_0[0:C, :] = high
        scaled_0[C : 2 * C, :] = low
        for into, weight in ((aq_ref, wq_ref), (akv_ref, wkv)):
            both = dot(scaled_0[0 : 2 * C, :], weight[...])
            high, low = split_two(both[:C] + both[C:])
            into[0:C, :] = high
            into[C : 2 * C, :] = low
        ring.third(3)
        high, low = split_two(center)
        high_0[0:C, :] = high
        high_1[0:C, :] = low
        high, low = high_0[0:C, :], high_1[0:C, :]
        high, low = split_two(dot_t(high, high) + dot_t(high, low) + dot_t(low, high))
        g_ref[0:C, :] = high
        g_ref[C : 2 * C, :] = low
        end()
        edge.wait()
        each("start", results)
        ring.end()
        each("wait", results)


def ring_scratch():
    return [
        pltpu.SemaphoreType.DMA,
        pltpu.SemaphoreType.DMA((40,)),
        pltpu.SemaphoreType.DMA((40,)),
    ]


def first(rows, blocks, places, latent, gain, w_query, w_key, w_value, w_in, up):
    freq = frequencies()
    scale = jnp.array([rows, 16.0, 1.0], F32)[:, None] * jnp.arange(16, dtype=F32)[None, :]
    angles = scale[:, :, None] * freq[None, None, :]
    sines, cosines = jnp.sin(angles), jnp.cos(angles)
    turn = jnp.stack([sines[0], cosines[0]], axis=1)
    fine_a = jnp.stack([sines[1], cosines[1]], axis=1)
    fine_b = jnp.stack([sines[2], cosines[2]], axis=0)
    return first_call(rows, blocks, places, latent, turn, fine_a, fine_b, gain, w_query, w_key,
                      w_value, w_in, up)


def first_call(rows, blocks, places, latent, turn, fine_a, fine_b, gain, w_query, w_key, w_value,
               w_in, up):
    width = w_key.shape[1]
    length = rows * blocks
    whole = pl.BlockSpec(memory_space=pltpu.VMEM)
    far = pl.BlockSpec(memory_space=pltpu.HBM)
    return pl.pallas_call(
        functools.partial(first_kernel, rows),
        grid=(blocks,),
        in_specs=[whole] * 6 + [far, far, whole, far],
        out_specs=[
            pl.BlockSpec((rows, 2 * width), lambda i: (i, 0)),
            pl.BlockSpec((rows, C), lambda i: (i, 0)),
            pl.BlockSpec((rows, 1), lambda i: (i, 0)),
        ]
        + [far] * 7,
        out_shape=[
            jax.ShapeDtypeStruct((length, 2 * width), F32),
            jax.ShapeDtypeStruct((length, C), F32),
            jax.ShapeDtypeStruct((length, 1), F32),
            jax.ShapeDtypeStruct((rows, width), F32),
            jax.ShapeDtypeStruct((2 * C, width), BF16),
            jax.ShapeDtypeStruct((2 * C, 2 * width), BF16),
            jax.ShapeDtypeStruct((2 * C, C), BF16),
            jax.ShapeDtypeStruct((blocks, 4, 2, rows // 8, C), BF16),
            jax.ShapeDtypeStruct((8, C), F32),
            jax.ShapeDtypeStruct((blocks, *up.shape), BF16),
        ],
        scratch_shapes=[
            pltpu.VMEM((rows, width), F32),
            pltpu.VMEM((2 * C, width), BF16),
            pltpu.VMEM((2 * C, 2 * width), BF16),
            pltpu.VMEM((2 * C, C), BF16),
            pltpu.VMEM((blocks, 4, 2, rows // 8, C), BF16),
            pltpu.VMEM((8, C), F32),
            pltpu.SemaphoreType.DMA((6,)),
            pltpu.VMEM(up.shape, BF16),
        ]
        + [pltpu.VMEM((rows, D), BF16)] * 4
        + [pltpu.VMEM((rows, 1), F32)] * 2
        + [
            pltpu.VMEM((2, rows, HALF), F32),
            pltpu.VMEM((D, 2 * width), BF16),
            pltpu.VMEM((16, 3 * width), F32),
            pltpu.VMEM((16, C), F32),
            pltpu.VMEM((8, C), F32),
            pltpu.SemaphoreType.DMA((3,)),
            pltpu.SemaphoreType.DMA((4,)),
            pltpu.SemaphoreType.DMA((4,)),
        ]
        + ring_scratch(),
        compiler_params=pltpu.CompilerParams(
            collective_id=0, has_side_effects=True, vmem_limit_bytes=56 << 20
        ),
        cost_estimate=pl.CostEstimate(
            flops=60_000_000_000, bytes_accessed=40_000_000, transcendentals=0
        ),
        name="first",
    )(latent, turn, fine_a, fine_b, gain, w_query, w_key, w_value, w_in, up)


def reduce_over_head(produce, meanwhile, between, term, taken, via_out, via_in, near, fin, send, recv):
    _, y, c = seat()
    partner, up, down = 2 * y + 1 - c, 2 * plus(y, 1) + c, 2 * plus(y, 3) + c

    def copy(src, dst, slot, head):
        return pltpu.make_async_remote_copy(
            src_ref=src, dst_ref=dst, send_sem=send.at[slot], recv_sem=recv.at[slot],
            device_id={"head": head}, device_id_type=MESH,
        )

    def pair(half, at):
        return term[half, at, c].astype(F32) + taken[half, at].astype(F32)

    across, ahead, behind = plus(y, 2), plus(y, 1), plus(y, 3)
    gives = [copy(term.at[half, :, 1 - c], taken.at[half], half, partner) for half in range(2)]
    produce(0, 0)
    produce(0, 1)
    gives[0].start()
    produce(1, 0)
    gives[0].wait_recv()
    via_out[0] = pair(0, across).astype(BF16)
    via_0 = copy(via_out.at[0], via_in.at[0], 2, up)
    via_0.start()
    near[1, 0] = pair(0, behind).astype(BF16)
    down_0 = copy(near.at[1, 0], fin.at[1, 0], 6, down)
    down_0.start()
    produce(1, 1)
    gives[1].start()
    meanwhile()
    gives[1].wait_recv()
    via_out[1] = pair(1, across).astype(BF16)
    via_1 = copy(via_out.at[1], via_in.at[1], 3, down)
    via_1.start()
    near[0, 1] = pair(1, ahead).astype(BF16)
    up_1 = copy(near.at[0, 1], fin.at[0, 1], 5, up)
    up_1.start()
    via_0.wait_recv()
    near[0, 0] = (pair(0, ahead) + via_in[0].astype(F32)).astype(BF16)
    up_0 = copy(near.at[0, 0], fin.at[0, 0], 4, up)
    up_0.start()
    via_1.wait_recv()
    near[1, 1] = (pair(1, behind) + via_in[1].astype(F32)).astype(BF16)
    down_1 = copy(near.at[1, 1], fin.at[1, 1], 7, down)
    down_1.start()
    between()
    sums = [pair(half, y) for half in range(2)]
    down_0.wait_recv()
    up_0.wait_recv()
    first = sums[0] + fin[0, 0].astype(F32) + fin[1, 0].astype(F32)
    up_1.wait_recv()
    down_1.wait_recv()
    second = sums[1] + fin[0, 1].astype(F32) + fin[1, 1].astype(F32)
    for done in (*gives, via_0, via_1, up_0, up_1, down_0, down_1):
        done.wait_send()
    return jnp.concatenate([first, second], axis=1)


def gather_over_head(out, send, recv, midway=lambda: None):
    _, y, c = seat()
    partner, up, down = 2 * y + 1 - c, 2 * plus(y, 1) + c, 2 * plus(y, 3) + c
    across, ahead, behind = plus(y, 2), plus(y, 1), plus(y, 3)
    low, high = pl.ds(0, HALF), pl.ds(HALF, HALF)

    def copy(block, slot, head):
        return pltpu.make_async_remote_copy(
            src_ref=block, dst_ref=block, send_sem=send.at[slot], recv_sem=recv.at[slot],
            device_id={"head": head}, device_id_type=MESH,
        )

    moves = [copy(out.at[y, c], 0, up), copy(out.at[y, c], 1, down), copy(out.at[y, c], 2, partner)]
    for move in moves:
        move.start()

    def then(slot, *following):
        moves[slot].wait_recv()
        for move in following:
            move.start()
            moves.append(move)

    then(0, copy(out.at[behind, c, :, low], 3, up), copy(out.at[behind, c], 4, partner))
    then(1, copy(out.at[ahead, c, :, high], 5, down), copy(out.at[ahead, c], 6, partner))
    midway()
    then(3, copy(out.at[across, c, :, low], 7, partner))
    then(5, copy(out.at[across, c, :, high], 8, partner))
    for slot in (2, 4, 6, 7, 8):
        moves[slot].wait_recv()
    for move in moves:
        move.wait_send()


def reduce_scratch(share):
    return [
        pltpu.VMEM((2, 4, 2, share, HALF), BF16),
        pltpu.VMEM((2, 4, share, HALF), BF16),
        pltpu.VMEM((2, share, HALF), BF16),
        pltpu.VMEM((2, share, HALF), BF16),
        pltpu.VMEM((2, 2, share, HALF), BF16),
        pltpu.VMEM((2, 2, share, HALF), BF16),
        pltpu.SemaphoreType.DMA((8,)),
        pltpu.SemaphoreType.DMA((8,)),
    ]


def head_neighbours():
    _, y, c = seat()
    return [{"head": 2 * y + 1 - c}, {"head": 2 * plus(y, 1) + c}, {"head": 2 * plus(y, 3) + c}]


def store_terms(term, half, at, share, value):
    for block in range(8):
        rows = value[block * share : (block + 1) * share].astype(BF16)
        term[half, block // 2, block % 2, :, at : at + value.shape[1]] = rows


def layer_kernel(rows, heads, last, *refs):
    ringed = not last
    kv_ref, *refs = refs
    sources, up_ref, down_ref, out, refs = refs[:14], refs[14], refs[15], refs[16], refs[17:]
    if ringed:
        full_ref, *refs = refs
    places, refs = refs[:14], refs[14:]
    loads, landing, stream_ref, normed_ref, queries, acc, sums, attended, *refs = refs
    up, down, hidden, wloads, msend, mrecv, *refs = refs
    if ringed:
        *refs, shard, load, local, gsend, grecv = refs
        ring = RingGather(shard, full_ref, local, gsend, grecv)
        fetch = pltpu.make_async_copy(down_ref, shard, load)
        down_ref = full_ref
    *parts, send, recv = refs
    (
        x_ref, h_ref, n_ref, eq_ref, aq_ref, akv_ref, g_ref,
        win_ref, wo_ref, embedding_ref, gain_ref, last_gain_ref, wf_ref, ahead_ref,
    ) = places
    inputs = staged(zip(sources, places), loads)
    wide = up.shape[2]
    ups = [
        pltpu.make_async_copy(up_ref.at[:, pl.ds(k * wide, wide)], up.at[k], wloads.at[k])
        for k in range(up.shape[0])
    ]
    downs = [
        pltpu.make_async_copy(
            down_ref.at[pl.ds(k * 4, 4)], down.at[k], wloads.at[up.shape[0] + k]
        )
        for k in range(down.shape[0])
    ]
    term = parts[0]
    share = rows // 8
    width = heads * HEAD_DIM
    block = pl.program_id(0)
    me, y, c = seat()
    if last:
        mirror = lax.axis_size("seq") - 1 - me
        sends_edge = jnp.logical_and(mirror > 0, 2 * y + c == 7)
        keeps_edge = jnp.logical_and(mirror - 1 == me, 2 * y + c == 7)
        waits_edge = jnp.logical_and(mirror > 0, jnp.logical_not(keeps_edge))

    def scale_of(x, h, n):
        twice = jnp.concatenate([x, x], axis=1)
        quad = jnp.sum(x.astype(F32) * (dot(twice, g_ref[...]) + 2.0 * h), axis=1, keepdims=True)
        return twice, lax.rsqrt(jnp.maximum(quad + n, 0.0) * (1.0 / D) + EPSILON)

    @pl.when(block == 0)
    def _():
        if ringed:
            fetch.start()
        each("start", inputs)
        each("start", ups if ringed else ups + downs)
        if last:
            hail(head_neighbours() + [{"seq": mirror, "head": head} for head in range(8)])

            @pl.when(waits_edge)
            def _():
                hail([{"seq": mirror - 1, "head": 7}])
        else:
            hail_all(landing.shape[0])
            pl.semaphore_wait(pltpu.get_barrier_semaphore(), landing.shape[0])
            fetch.wait()
            ring.begin()
        each("wait", inputs[:7])
        own = pl.ds(pl.multiple_of(me * rows, rows), rows)
        twice, scale = scale_of(x_ref[own, :], h_ref[own, :], n_ref[own, :])
        value = (dot(twice, aq_ref[...]) + eq_ref[...]) * (scale * HEAD_DIM**-0.5)
        queries[...] = value.astype(BF16)
        acc[...] = jnp.zeros_like(acc)
        sums[...] = jnp.zeros_like(sums)

    def step(masked):
        here = pl.ds(pl.multiple_of(block * KEY_BLOCK, KEY_BLOCK), KEY_BLOCK)
        twice, scale = scale_of(x_ref[here, :], h_ref[here, :], n_ref[here, :])
        both = ((dot(twice, akv_ref[...]) + kv_ref[...]) * scale).astype(BF16)
        keys, values = both[:, :width], both[:, width:]
        if masked:
            shape = (rows, KEY_BLOCK)
            row = me * rows + lax.broadcasted_iota(jnp.int32, shape, 0)
            col = block * KEY_BLOCK + lax.broadcasted_iota(jnp.int32, shape, 1)
            seen = col <= row
        for head in range(heads):
            cols = slice(head * HEAD_DIM, (head + 1) * HEAD_DIM)
            scores = dot_t(queries[:, cols], keys[:, cols])
            if masked:
                weights = jnp.where(seen, jnp.exp(jnp.where(seen, scores, 0.0)), 0.0)
            else:
                weights = jnp.exp(scores)
            part = weights[:, :HEAD_DIM]
            for at in range(HEAD_DIM, KEY_BLOCK, HEAD_DIM):
                part = part + weights[:, at : at + HEAD_DIM]
            sums[:, cols] += part
            acc[:, cols] += dot(weights.astype(BF16), values[:, cols])

    final = (me * rows + rows - 1) // KEY_BLOCK

    @pl.when(block < final)
    def _():
        step(False)

    @pl.when(block == final)
    def _():
        step(True)

    def produce(half, part):
        at = part * (HALF // 2)
        cols = slice(half * HALF + at, half * HALF + at + HALF // 2)
        store_terms(term, half, at, share, dot(attended[...], wo_ref[:, cols]))

    def meanwhile():
        first = pl.ds(pl.multiple_of(me * rows + (2 * y + c) * share, share), share)
        stream_ref[...] = dot(x_ref[first, :], win_ref[...]) + embedding_ref[...]

    def between():
        if ringed:
            ring.second()
            ring.middle()

    def midway():
        if ringed:
            ring.third(2)

    def produce_down(half, part):
        k = 2 * half + part
        downs[k].wait()
        weight = down[k].reshape(D // 4, hidden.shape[1])
        store_terms(term, half, part * (HALF // 2), share, dot_t(hidden[...], weight))

    @pl.when(block == pl.num_programs(0) - 1)
    def _():
        for head in range(heads):
            cols = slice(head * HEAD_DIM, (head + 1) * HEAD_DIM)
            total = jnp.sum(sums[:, cols], axis=1, keepdims=True)
            attended[:, cols] = (acc[:, cols] / total).astype(BF16)
        each("wait", inputs[7:])
        if ringed:
            ring.first()
        else:
            barrier = pltpu.get_barrier_semaphore()

            @pl.when(keeps_edge)
            def _():
                pl.semaphore_wait(barrier, 18)

            @pl.when(jnp.logical_and(sends_edge, jnp.logical_not(keeps_edge)))
            def _():
                pl.semaphore_wait(barrier, 19)

            @pl.when(jnp.logical_not(sends_edge))
            def _():
                pl.semaphore_wait(barrier, 11)

        total = reduce_over_head(produce, meanwhile, between, *parts)
        stream = stream_ref[...] + total
        stream_ref[...] = stream
        normed_ref[y, c] = layer_norm(stream, gain_ref[...]).astype(BF16)
        if ringed:
            ring.third(1)
        gather_over_head(normed_ref, send, recv, midway)
        if ringed:
            ring.third(3)
        for k in range(up.shape[0]):
            ups[k].wait()
            pre = dot(normed_ref[...].reshape(rows, D), up[k])
            hidden[:, k * wide : (k + 1) * wide] = jax.nn.gelu(pre, approximate=True).astype(BF16)
        if ringed:
            ring.end()
            each("start", downs)
        total = reduce_over_head(produce_down, lambda: None, lambda: None, *parts)
        normed = layer_norm(stream_ref[...] + total, last_gain_ref[...]).astype(BF16)
        params = dot(normed, wf_ref[...])
        following = ahead_ref[...] * jnp.exp(jnp.tanh(params[:, C:])) + params[:, :C]
        if last:
            finish(following, landing, term, msend, mrecv)
            out[...] = landing[...]
        else:
            landing[me * 4 + y, c] = following.astype(BF16)
            begin, cross, end = spread(landing, msend, mrecv)
            begin()
            cross()
            end()
            before = x_ref[0:16, :].astype(F32)[0:1]
            chunk = 8 * 2 * share
            line = lax.broadcasted_iota(jnp.int32, (chunk, C), 0)
            for k in range(landing.shape[0] // 8):
                value = landing[8 * k : 8 * k + 8].reshape(chunk, C).astype(F32)
                moved = jnp.where(line == 0, before, pltpu.roll(value, 1, 0))
                out[k * chunk : (k + 1) * chunk, :] = moved.astype(BF16)
                before = value[chunk - 1 :]


def finish(following, out_ref, term, send, recv):
    seq, y, c = seat()
    mirror = lax.axis_size("seq") - 1 - seq
    sends_edge = jnp.logical_and(mirror > 0, 2 * y + c == 7)
    keeps_edge = jnp.logical_and(mirror - 1 == seq, 2 * y + c == 7)
    waits_edge = jnp.logical_and(mirror > 0, jnp.logical_not(keeps_edge))
    block = term.at[0, 0, 0, :, pl.ds(0, C)]
    block[...] = following.astype(BF16)
    head = 2 * y + c
    moves = [
        pltpu.make_async_remote_copy(
            src_ref=block, dst_ref=out_ref.at[head], send_sem=send.at[k], recv_sem=recv.at[0],
            device_id={"seq": mirror, "head": k}, device_id_type=MESH,
        )
        for k in range(8)
    ]
    edges = [
        pltpu.make_async_remote_copy(
            src_ref=block, dst_ref=out_ref.at[8], send_sem=send.at[8 + k], recv_sem=recv.at[1],
            device_id={"seq": mirror - 1, "head": k}, device_id_type=MESH,
        )
        for k in range(8)
    ]
    for move in moves:
        move.start()

    @pl.when(sends_edge)
    def _():
        for move in edges[:7]:
            move.start()

    @pl.when(jnp.logical_and(sends_edge, jnp.logical_not(keeps_edge)))
    def _():
        edges[7].start()

    whole = out_ref.at[pl.ds(0, 8)]
    pltpu.make_async_remote_copy(
        src_ref=whole, dst_ref=whole, send_sem=send.at[0], recv_sem=recv.at[0],
        device_id={"seq": mirror, "head": 0}, device_id_type=MESH,
    ).wait_recv()

    @pl.when(waits_edge)
    def _():
        pltpu.make_async_remote_copy(
            src_ref=block, dst_ref=out_ref.at[8], send_sem=send.at[0], recv_sem=recv.at[1],
            device_id={"seq": mirror - 1, "head": 7}, device_id_type=MESH,
        ).wait_recv()

    for move in moves:
        move.wait_send()

    @pl.when(sends_edge)
    def _():
        for move in edges[:7]:
            move.wait_send()

    @pl.when(jnp.logical_and(sends_edge, jnp.logical_not(keeps_edge)))
    def _():
        edges[7].wait_send()

    @pl.when(jnp.logical_not(waits_edge))
    def _():
        out_ref[8] = following.astype(BF16)


def layer(rows, places, last, state, x, w_in, w_attn_out, embedding, gain, last_gain, w_final, ahead,
          up, down):
    kv = state[0]
    length, width = kv.shape[0], kv.shape[1] // 2
    share, hidden = rows // 8, up.shape[1]
    count = length // rows
    shard = (2, D // count // 2, hidden)
    far = pl.BlockSpec(memory_space=pltpu.HBM)
    tile = pl.BlockSpec((KEY_BLOCK, 2 * width), lambda i: (i, 0))
    sources = [x, *state[1:], w_in, w_attn_out, embedding, gain, last_gain, w_final, ahead]
    shape = (9, share, C) if last else (places, 2, share, C)
    outs = [jax.ShapeDtypeStruct(shape if last else (length, C), BF16)]
    if not last:
        outs.append(jax.ShapeDtypeStruct((count, *shard), BF16))
    return pl.pallas_call(
        functools.partial(layer_kernel, rows, width // HEAD_DIM, last),
        grid=(length // KEY_BLOCK,),
        in_specs=[tile] + [far] * 16,
        out_specs=[pl.BlockSpec(memory_space=pltpu.VMEM)] + [far] * (not last),
        out_shape=outs,
        scratch_shapes=[buffer_like(source) for source in sources]
        + [
            pltpu.SemaphoreType.DMA((14,)),
            pltpu.VMEM(shape, BF16),
            pltpu.VMEM((share, D), F32),
            pltpu.VMEM((4, 2, share, D), BF16),
            pltpu.VMEM((rows, width), BF16),
            pltpu.VMEM((rows, width), F32),
            pltpu.VMEM((rows, width), F32),
            pltpu.VMEM((rows, width), BF16),
            pltpu.VMEM((3, D, hidden // 3), BF16),
            pltpu.VMEM((4, count // 4, *shard), BF16),
            pltpu.VMEM((rows, hidden), BF16),
            pltpu.SemaphoreType.DMA((7,)),
            pltpu.SemaphoreType.DMA((16,)),
            pltpu.SemaphoreType.DMA((2,)),
        ]
        + reduce_scratch(share)
        + [pltpu.SemaphoreType.DMA((9,)), pltpu.SemaphoreType.DMA((9,))]
        + ([] if last else [pltpu.VMEM(shard, BF16), pltpu.SemaphoreType.DMA] + ring_scratch()),
        compiler_params=pltpu.CompilerParams(
            collective_id=2 if last else 1, has_side_effects=True, vmem_limit_bytes=60 << 20
        ),
        cost_estimate=pl.CostEstimate(
            flops=60_000_000_000, bytes_accessed=40_000_000, transcendentals=0
        ),
        name="layer_last" if last else "layer",
    )(kv, *sources, up, down)


def per_device(
    latent, w_in, w_query, w_key, w_value, w_attn_out, w_up, w_down, w_final,
    gain_attn, gain_mlp, gain_final,
):
    seq_count, head_count = lax.axis_size("seq"), lax.axis_size("head")
    me, mine = lax.axis_index("seq"), lax.axis_index("head")
    rows = latent.shape[0]
    share = rows // head_count
    length = rows * seq_count
    places = seq_count * head_count // 2
    start = me * rows + mine * share

    shape = (2, w_up.shape[0] // 2, w_up.shape[1])
    *state, gathered, edge, up = first(
        rows, seq_count, places, latent, gain_attn[None, :], w_query, w_key, w_value, w_in,
        w_up.reshape(shape),
    )
    up = up.reshape(D, w_up.shape[1])
    x = gathered.reshape(length, C)
    angles = (start + jnp.arange(share)).astype(F32)[:, None] * frequencies()[None, :]
    embedding = jnp.concatenate([jnp.sin(angles), jnp.cos(angles)], axis=1)
    ahead = lax.dynamic_slice_in_dim(
        jnp.concatenate([latent[1:], edge[:1]], axis=0), mine * share, share, 0
    )
    top = x[:1]
    down = w_down.T.reshape(shape)
    for step_index in range(ITERS):
        last = step_index == ITERS - 1
        x, *full = layer(
            rows, places, last, state, x, w_in, w_attn_out, embedding, gain_mlp[None, :],
            gain_final[None, :], w_final, ahead, up, down,
        )
        if not last:
            down = full[0]
    following = x
    edge = jnp.where(me == seq_count - 1, top, following[8, share - 1 :])
    result = jnp.concatenate([edge, following[:8].reshape(rows, C)[:-1]], axis=0)
    return result[::-1].astype(F32)


def solution(mesh):
    in_specs = (
        P("seq", None),
        P(),
        P(None, "head"),
        P(None, "head"),
        P(None, "head"),
        P("head", None),
        P("seq", "head"),
        P("head", "seq"),
        P(),
        P(),
        P(),
        P(),
    )
    return jax.shard_map(
        per_device, mesh=mesh, in_specs=in_specs, out_specs=P("seq", None), check_vma=False
    )
```

```python
import functools

import jax
import jax.numpy as jnp
import numpy as np
from jax import lax
from jax.experimental import pallas as pl
from jax.experimental.pallas import tpu as pltpu
from jax.sharding import PartitionSpec as P

D = 3072
HALF = D // 2
HEAD_DIM = 128
C = 128
ITERS = 2
EPSILON = 1e-05
KEY_BLOCK = 512
BF16 = jnp.bfloat16
F32 = jnp.float32


def split_two(value):
    high = value.astype(BF16)
    return high, (value - high.astype(F32)).astype(BF16)


def dot(left, right):
    return jnp.dot(left, right, preferred_element_type=F32)


def dot_t(left, right):
    return lax.dot_general(left, right, (((1,), (1,)), ((), ())), preferred_element_type=F32)


def layer_norm(stream, gain):
    center = stream - jnp.mean(stream, axis=-1, keepdims=True)
    spread = jnp.mean(center * center, axis=-1, keepdims=True)
    return center * lax.rsqrt(spread + EPSILON) * gain


def frequencies():
    return np.exp(-np.log(10000.0) * 2.0 * np.arange(HALF) / D).astype(np.float32)[None, :]


MESH = pl.DeviceIdType.MESH


def staged(pairs, sems):
    return [pltpu.make_async_copy(src, dst, sems.at[k]) for k, (src, dst) in enumerate(pairs)]


def each(action, copies):
    for copy in copies:
        getattr(copy, action)()


def buffer_like(array):
    return pltpu.VMEM(array.shape, array.dtype)


def seat():
    head = lax.axis_index("head")
    return lax.axis_index("seq"), lax.div(head, 2), lax.rem(head, 2)


def plus(y, by):
    return lax.rem(y + by, 4)


def hail(targets):
    barrier = pltpu.get_barrier_semaphore()
    for target in targets:
        pl.semaphore_signal(barrier, inc=1, device_id=target, device_id_type=MESH)


def met(targets):
    pl.semaphore_wait(pltpu.get_barrier_semaphore(), len(targets))


def hail_all(devices):
    seq, y, c = seat()
    place = seq * 4 + y
    barrier = pltpu.get_barrier_semaphore()
    pl.semaphore_signal(barrier, inc=1, device_id={"head": 2 * y + 1 - c}, device_id_type=MESH)

    @pl.loop(1, devices)
    def _(k):
        other = lax.rem(place + k, devices)
        pl.semaphore_signal(
            barrier, inc=1,
            device_id={"seq": lax.div(other, 4), "head": 2 * lax.rem(other, 4) + c},
            device_id_type=MESH,
        )


def start_peers(count):
    seq, y, c = seat()
    return (
        [{"seq": lax.rem(seq + k, count)} for k in range(1, count)]
        + [{"head": 2 * plus(y, k) + c} for k in range(1, 4)]
        + [{"head": 2 * y + 1 - c}]
    )


def start_spread(buffer, send, recv):
    seq, y, c = seat()
    count = buffer.shape[0]

    def copy(block, slot, device):
        return pltpu.make_async_remote_copy(
            src_ref=block, dst_ref=block, send_sem=send.at[slot], recv_sem=recv.at[slot],
            device_id=device, device_id_type=MESH,
        )

    partner = {"head": 2 * y + 1 - c}
    plane = copy(buffer.at[pl.ds(0, count - 1), 0, c], 0, partner)
    column = copy(buffer.at[:, pl.ds(0, 3), c], 1, partner)
    across = copy(buffer.at[:, :, c], 2, partner)

    def begin():
        @pl.loop(1, count)
        def _(k):
            copy(buffer.at[seq, y, c], 0, {"seq": lax.rem(seq + k, count)}).start()

    def columns():
        plane.wait_recv()
        for k in range(1, 4):
            copy(buffer.at[:, y, c], 1, {"head": 2 * plus(y, k) + c}).start()

    def cross():
        column.wait_recv()
        across.start()

    def end():
        plane.wait_send()
        column.wait_send()
        across.wait()

    return begin, columns, cross, end


def spread(buffer, send, recv):
    seq, y, c = seat()
    devices = buffer.shape[0]
    place = seq * 4 + y
    partner = {"head": 2 * y + 1 - c}
    whole = buffer.at[pl.ds(0, devices - 1), c]
    arrived = pltpu.make_async_remote_copy(
        src_ref=whole, dst_ref=whole, send_sem=send.at[0], recv_sem=recv.at[0],
        device_id=partner, device_id_type=MESH,
    )
    across = pltpu.make_async_remote_copy(
        src_ref=buffer.at[:, c], dst_ref=buffer.at[:, c], send_sem=send.at[1], recv_sem=recv.at[1],
        device_id=partner, device_id_type=MESH,
    )

    def begin():
        @pl.loop(1, devices)
        def _(k):
            other = lax.rem(place + k, devices)
            pltpu.make_async_remote_copy(
                src_ref=buffer.at[place, c], dst_ref=buffer.at[place, c],
                send_sem=send.at[0], recv_sem=recv.at[0],
                device_id={"seq": lax.div(other, 4), "head": 2 * lax.rem(other, 4) + c},
                device_id_type=MESH,
            ).start()

    def cross():
        arrived.wait_recv()
        across.start()

    def end():
        arrived.wait_send()
        across.wait()

    return begin, cross, end


class RingGather:
    FIRST = (0, 3, 1, 2)

    def __init__(self, own, out, local, send, recv):
        seq = lax.axis_index("seq")
        self.x, self.z = lax.div(seq, 4), lax.rem(seq, 4)
        self.own, self.out, self.send, self.recv = own, out, send, recv
        self.keep = pltpu.make_async_copy(own, out.at[seq], local)

    def place(self, half, p, q):
        x, z = (p, q) if half == 0 else (q, p)
        return plus(self.x, x) * 4 + plus(self.z, z)

    def move(self, half, slot):
        if slot < 4:
            kind, block, target = slot, None, [(1, 0), (3, 0), (1, 0), (3, 0)][slot]
            origin = [(0, 0), (0, 0), (3, 0), (1, 0)][slot]
        else:
            block, kind = divmod(slot - 4, 4)
            target = [(0, 1), (0, 3), (0, 1), (0, 3)][kind]
            origin = (self.FIRST[block], [0, 0, 3, 1][kind])
        ref = self.out.at[self.place(half, *origin), half]
        if kind >= 2:
            part = ref.shape[0] // 2
            ref = ref.at[pl.ds((kind - 2) * part, part)]
        source = self.own.at[half] if origin == (0, 0) else ref
        return pltpu.make_async_remote_copy(
            src_ref=source, dst_ref=ref,
            send_sem=self.send.at[20 * half + slot], recv_sem=self.recv.at[20 * half + slot],
            device_id={"seq": self.place(half, *target)}, device_id_type=MESH,
        )

    def neighbours(self):
        return [{"seq": self.place(0, *at)} for at in ((1, 0), (3, 0), (0, 1), (0, 3))]

    def on(self, slots, *following):
        for half in range(2):
            for slot in slots:
                self.move(half, slot).wait_recv()
            for slot in following:
                self.move(half, slot).start()

    def begin(self):
        self.keep.start()
        self.on((), 0, 1)
        self.on((), 4, 5)

    def first(self):
        self.on((0,), 2, 8, 9)
        self.on((1,), 3, 12, 13)

    def second(self):
        self.on((4,), 6)
        self.on((5,), 7)

    def middle(self):
        self.on((2, 3), 16, 17)

    def third(self, block):
        self.on((4 + 4 * block,), 6 + 4 * block)
        self.on((5 + 4 * block,), 7 + 4 * block)

    def end(self):
        self.on((6, 7, 10, 11, 14, 15, 18, 19))
        self.keep.wait()
        for half in range(2):
            for slot in range(20):
                self.move(half, slot).wait_send()


def first_kernel(
    rows, latent_ref, freq_ref, gain_ref, wq_ref, wk_ref, wv_ref, win_ref, up_ref,
    kv_ref, h_ref, n_ref, eq_out, aq_out, akv_out, g_out, x_out, ahead_out,
    embedding_out, full_ref, eq_ref, aq_ref, akv_ref, g_ref, x_ref, ahead_ref, embedding_ref, stores,
    edge_ref, turn_ref, fine_a, fine_b, shard, scaled_0, scaled_1, high_0, high_1, mean_0, mean_1, base, wkv, gw, wsum, edge_rows,
    loads, xsend, xrecv, local, gsend, grecv,
):
    step, steps = pl.program_id(0), pl.num_programs(0)
    seq, y, c = seat()
    width = wk_ref.shape[1]
    fetches = [
        pltpu.make_async_copy(ref, wkv.at[:, pl.ds(k * width, width)], loads.at[k])
        for k, ref in enumerate((wk_ref, wv_ref))
    ]
    begin, columns, cross, end = start_spread(x_ref, xsend, xrecv)
    count = lax.axis_size("seq")
    edge = pltpu.make_async_remote_copy(
        src_ref=edge_rows, dst_ref=edge_ref, send_sem=xsend.at[3], recv_sem=xrecv.at[3],
        device_id={"seq": lax.rem(seq + count - 1, count)}, device_id_type=MESH,
    )
    ring = RingGather(shard, full_ref, local, gsend, grecv)
    fetches.append(pltpu.make_async_copy(up_ref, shard, loads.at[2]))
    results = staged(
        [
            (eq_ref, eq_out), (aq_ref, aq_out), (akv_ref, akv_out), (g_ref, g_out),
            (x_ref, x_out), (ahead_ref, ahead_out), (embedding_ref, embedding_out),
        ],
        stores,
    )

    def fill(block, scaled, high, mean):
        total = jnp.zeros((rows, 1), F32)
        wide = 512
        for at in range(0, HALF, wide):
            cols = slice(at, at + wide)
            sin_a, cos_a = turn_ref[block, 0:1, cols], turn_ref[block, 1:2, cols]
            sin_b, cos_b = base[0, :, cols], base[1, :, cols]
            for part, offset in (
                (sin_a * cos_b + cos_a * sin_b, 0),
                (cos_a * cos_b - sin_a * sin_b, HALF),
            ):
                into = slice(offset + at, offset + at + wide)
                high[:, into] = part.astype(BF16)
                scaled[:, into] = (part * gain_ref[:, into]).astype(BF16)
                total = total + jnp.sum(part, axis=1, keepdims=True)
        mean[...] = total * (1.0 / D)

    def rows_out():
        edge_rows[...] = latent_ref[0:8, :]
        own = pl.ds(pl.multiple_of((2 * y + c) * (rows // 8), rows // 8), rows // 8)
        x_ref[seq, y, c] = latent_ref[own, :].astype(BF16)

    def tables():
        row = lax.broadcasted_iota(jnp.int32, (16, HALF), 0).astype(F32)
        angle = row * freq_ref[...]
        sines, cosines = jnp.sin(angle), jnp.cos(angle)
        fine_b[0], fine_b[1] = sines, cosines
        for table in (fine_a, turn_ref):
            for _ in range(4):
                sines, cosines = 2.0 * sines * cosines, cosines * cosines - sines * sines
            for k in range(16):
                table[k, 0:1, :] = sines[k : k + 1]
                table[k, 1:2, :] = cosines[k : k + 1]

        @pl.loop(0, rows // 16)
        def _(k):
            sin_a, cos_a = fine_a[k, 0:1, :], fine_a[k, 1:2, :]
            sin_b, cos_b = fine_b[0], fine_b[1]
            into = pl.ds(pl.multiple_of(k * 16, 16), 16)
            base[0, into, :] = sin_a * cos_b + cos_a * sin_b
            base[1, into, :] = cos_a * cos_b - sin_a * sin_b

        share = rows // 8
        own = pl.ds(pl.multiple_of((2 * y + c) * share, share), share)
        sin_a, cos_a = turn_ref[seq, 0:1, :], turn_ref[seq, 1:2, :]
        sin_b, cos_b = base[0, own, :], base[1, own, :]
        embedding_ref[:, 0:HALF] = sin_a * cos_b + cos_a * sin_b
        embedding_ref[:, HALF:] = cos_a * cos_b - sin_a * sin_b
        wsum[...] = dot_t(jnp.ones((16, D), BF16), win_ref[...])
        gain = gain_ref[...]
        high = gain.astype(BF16).astype(F32)
        line = lax.broadcasted_iota(jnp.int32, (16, D), 0)
        both = jnp.where(line == 0, high, jnp.where(line == 1, gain - high, 0.0)).astype(BF16)
        for fetch in fetches[:2]:
            fetch.wait()
        gw[:, 0:width] = dot(both, wq_ref[...])
        gw[:, width:] = dot(both, wkv[...])
        gw[0:1, :] = jnp.sum(gw[...], axis=0, keepdims=True)

    @pl.when(step == 0)
    def _():
        fetches[2].start()
        peers = start_peers(count)
        hail(peers)
        rows_out()
        for fetch in fetches[:2]:
            fetch.start()
        fetches[2].wait()
        met(peers)
        ring.begin()
        begin()
        edge.start()
        tables()
        fill(0, scaled_0, high_0, mean_0)

    def work(scaled, high, mean, others):
        value = mean[...]
        kv_ref[...] = dot(scaled[...], wkv[...]) - value * gw[0:1, width:]
        h_ref[...] = dot_t(high[...], win_ref[...]) - value * wsum[0:1, :]
        n_ref[...] = HALF - D * value * value
        fill(jnp.minimum(step + 1, steps - 1), *others)

        @pl.when(step == seq)
        def _():
            eq_ref[...] = dot(scaled[...], wq_ref[...]) - value * gw[0:1, 0:width]

    even, odd = (scaled_0, high_0, mean_0), (scaled_1, high_1, mean_1)

    @pl.when(lax.rem(step, 2) == 0)
    def _():
        work(*even, odd)

    @pl.when(lax.rem(step, 2) == 1)
    def _():
        work(*odd, even)

    pl.when(step == 3)(columns)
    pl.when(step == 6)(cross)

    for at, event in ((3, ring.first), (7, ring.second), (9, ring.middle)):
        pl.when(step == at)(event)
    for at, block in ((12, 1), (15, 2)):
        pl.when(step == at)(functools.partial(ring.third, block))

    @pl.when(step == steps - 1)
    def _():
        wide = win_ref[...].astype(F32)
        center = wide - jnp.mean(wide, axis=1, keepdims=True)
        high, low = split_two(center * gain_ref[...])
        scaled_0[0:C, :] = high
        scaled_0[C : 2 * C, :] = low
        for into, weight in ((aq_ref, wq_ref), (akv_ref, wkv)):
            both = dot(scaled_0[0 : 2 * C, :], weight[...])
            high, low = split_two(both[:C] + both[C:])
            into[0:C, :] = high
            into[C : 2 * C, :] = low
        ring.third(3)
        high, low = split_two(center)
        high_0[0:C, :] = high
        high_1[0:C, :] = low
        high, low = high_0[0:C, :], high_1[0:C, :]
        high, low = split_two(dot_t(high, high) + dot_t(high, low) + dot_t(low, high))
        g_ref[0:C, :] = high
        g_ref[C : 2 * C, :] = low
        end()
        edge.wait()
        share = rows // 8
        head = 2 * y + c
        own = latent_ref[pl.ds(pl.multiple_of(head * share, share), share), :]
        beyond = pl.multiple_of(jnp.minimum((head + 1) * share, rows - 8), 8)
        beyond = jnp.where(head == 7, edge_ref[0:1, :], latent_ref[pl.ds(beyond, 8), :][0:1])
        line = lax.broadcasted_iota(jnp.int32, (share, C), 0)
        ahead_ref[...] = jnp.where(line == share - 1, beyond, pltpu.roll(own, share - 1, 0))
        each("start", results)
        ring.end()
        each("wait", results)


def ring_scratch():
    return [
        pltpu.SemaphoreType.DMA,
        pltpu.SemaphoreType.DMA((40,)),
        pltpu.SemaphoreType.DMA((40,)),
    ]


def first(rows, blocks, places, latent, gain, w_query, w_key, w_value, w_in, up):
    width = w_key.shape[1]
    length = rows * blocks
    whole = pl.BlockSpec(memory_space=pltpu.VMEM)
    far = pl.BlockSpec(memory_space=pltpu.HBM)
    return pl.pallas_call(
        functools.partial(first_kernel, rows),
        grid=(blocks,),
        in_specs=[whole] * 4 + [far, far, whole, far],
        out_specs=[
            pl.BlockSpec((rows, 2 * width), lambda i: (i, 0)),
            pl.BlockSpec((rows, C), lambda i: (i, 0)),
            pl.BlockSpec((rows, 1), lambda i: (i, 0)),
        ]
        + [far] * 8,
        out_shape=[
            jax.ShapeDtypeStruct((length, 2 * width), F32),
            jax.ShapeDtypeStruct((length, C), F32),
            jax.ShapeDtypeStruct((length, 1), F32),
            jax.ShapeDtypeStruct((rows, width), F32),
            jax.ShapeDtypeStruct((2 * C, width), BF16),
            jax.ShapeDtypeStruct((2 * C, 2 * width), BF16),
            jax.ShapeDtypeStruct((2 * C, C), BF16),
            jax.ShapeDtypeStruct((blocks, 4, 2, rows // 8, C), BF16),
            jax.ShapeDtypeStruct((rows // 8, C), F32),
            jax.ShapeDtypeStruct((rows // 8, D), F32),
            jax.ShapeDtypeStruct((blocks, *up.shape), BF16),
        ],
        scratch_shapes=[
            pltpu.VMEM((rows, width), F32),
            pltpu.VMEM((2 * C, width), BF16),
            pltpu.VMEM((2 * C, 2 * width), BF16),
            pltpu.VMEM((2 * C, C), BF16),
            pltpu.VMEM((blocks, 4, 2, rows // 8, C), BF16),
            pltpu.VMEM((rows // 8, C), F32),
            pltpu.VMEM((rows // 8, D), F32),
            pltpu.SemaphoreType.DMA((7,)),
            pltpu.VMEM((8, C), F32),
            pltpu.VMEM((16, 2, HALF), F32),
            pltpu.VMEM((16, 2, HALF), F32),
            pltpu.VMEM((2, 16, HALF), F32),
            pltpu.VMEM(up.shape, BF16),
        ]
        + [pltpu.VMEM((rows, D), BF16)] * 4
        + [pltpu.VMEM((rows, 1), F32)] * 2
        + [
            pltpu.VMEM((2, rows, HALF), F32),
            pltpu.VMEM((D, 2 * width), BF16),
            pltpu.VMEM((16, 3 * width), F32),
            pltpu.VMEM((16, C), F32),
            pltpu.VMEM((8, C), F32),
            pltpu.SemaphoreType.DMA((3,)),
            pltpu.SemaphoreType.DMA((4,)),
            pltpu.SemaphoreType.DMA((4,)),
        ]
        + ring_scratch(),
        compiler_params=pltpu.CompilerParams(
            collective_id=0, has_side_effects=True, vmem_limit_bytes=56 << 20
        ),
        cost_estimate=pl.CostEstimate(
            flops=60_000_000_000, bytes_accessed=40_000_000, transcendentals=0
        ),
        name="first",
    )(latent, jnp.asarray(frequencies()), gain, w_query, w_key, w_value, w_in, up)


def reduce_over_head(produce, meanwhile, between, term, taken, via_out, via_in, near, fin, send, recv):
    _, y, c = seat()
    partner, up, down = 2 * y + 1 - c, 2 * plus(y, 1) + c, 2 * plus(y, 3) + c

    def copy(src, dst, slot, head):
        return pltpu.make_async_remote_copy(
            src_ref=src, dst_ref=dst, send_sem=send.at[slot], recv_sem=recv.at[slot],
            device_id={"head": head}, device_id_type=MESH,
        )

    def pair(half, at):
        return term[half, at, c].astype(F32) + taken[half, at].astype(F32)

    across, ahead, behind = plus(y, 2), plus(y, 1), plus(y, 3)
    gives = [copy(term.at[half, :, 1 - c], taken.at[half], half, partner) for half in range(2)]
    produce(0, 0)
    produce(0, 1)
    gives[0].start()
    produce(1, 0)
    gives[0].wait_recv()
    via_out[0] = pair(0, across).astype(BF16)
    via_0 = copy(via_out.at[0], via_in.at[0], 2, up)
    via_0.start()
    near[1, 0] = pair(0, behind).astype(BF16)
    down_0 = copy(near.at[1, 0], fin.at[1, 0], 6, down)
    down_0.start()
    produce(1, 1)
    gives[1].start()
    meanwhile()
    gives[1].wait_recv()
    via_out[1] = pair(1, across).astype(BF16)
    via_1 = copy(via_out.at[1], via_in.at[1], 3, down)
    via_1.start()
    near[0, 1] = pair(1, ahead).astype(BF16)
    up_1 = copy(near.at[0, 1], fin.at[0, 1], 5, up)
    up_1.start()
    via_0.wait_recv()
    near[0, 0] = (pair(0, ahead) + via_in[0].astype(F32)).astype(BF16)
    up_0 = copy(near.at[0, 0], fin.at[0, 0], 4, up)
    up_0.start()
    via_1.wait_recv()
    near[1, 1] = (pair(1, behind) + via_in[1].astype(F32)).astype(BF16)
    down_1 = copy(near.at[1, 1], fin.at[1, 1], 7, down)
    down_1.start()
    between()
    sums = [pair(half, y) for half in range(2)]
    down_0.wait_recv()
    up_0.wait_recv()
    first = sums[0] + fin[0, 0].astype(F32) + fin[1, 0].astype(F32)
    up_1.wait_recv()
    down_1.wait_recv()
    second = sums[1] + fin[0, 1].astype(F32) + fin[1, 1].astype(F32)
    for done in (*gives, via_0, via_1, up_0, up_1, down_0, down_1):
        done.wait_send()
    return jnp.concatenate([first, second], axis=1)


def gather_over_head(out, send, recv, midway=lambda: None):
    _, y, c = seat()
    partner, up, down = 2 * y + 1 - c, 2 * plus(y, 1) + c, 2 * plus(y, 3) + c
    across, ahead, behind = plus(y, 2), plus(y, 1), plus(y, 3)
    low, high = pl.ds(0, HALF), pl.ds(HALF, HALF)

    def copy(block, slot, head):
        return pltpu.make_async_remote_copy(
            src_ref=block, dst_ref=block, send_sem=send.at[slot], recv_sem=recv.at[slot],
            device_id={"head": head}, device_id_type=MESH,
        )

    moves = [copy(out.at[y, c], 0, up), copy(out.at[y, c], 1, down), copy(out.at[y, c], 2, partner)]
    for move in moves:
        move.start()

    def then(slot, *following):
        moves[slot].wait_recv()
        for move in following:
            move.start()
            moves.append(move)

    then(0, copy(out.at[behind, c, :, low], 3, up), copy(out.at[behind, c], 4, partner))
    then(1, copy(out.at[ahead, c, :, high], 5, down), copy(out.at[ahead, c], 6, partner))
    midway()
    then(3, copy(out.at[across, c, :, low], 7, partner))
    then(5, copy(out.at[across, c, :, high], 8, partner))
    for slot in (2, 4, 6, 7, 8):
        moves[slot].wait_recv()
    for move in moves:
        move.wait_send()


def reduce_scratch(share):
    return [
        pltpu.VMEM((2, 4, 2, share, HALF), BF16),
        pltpu.VMEM((2, 4, share, HALF), BF16),
        pltpu.VMEM((2, share, HALF), BF16),
        pltpu.VMEM((2, share, HALF), BF16),
        pltpu.VMEM((2, 2, share, HALF), BF16),
        pltpu.VMEM((2, 2, share, HALF), BF16),
        pltpu.SemaphoreType.DMA((8,)),
        pltpu.SemaphoreType.DMA((8,)),
    ]


def head_neighbours():
    _, y, c = seat()
    return [{"head": 2 * y + 1 - c}, {"head": 2 * plus(y, 1) + c}, {"head": 2 * plus(y, 3) + c}]


def store_terms(term, half, at, share, value):
    for block in range(8):
        rows = value[block * share : (block + 1) * share].astype(BF16)
        term[half, block // 2, block % 2, :, at : at + value.shape[1]] = rows


def layer_kernel(rows, heads, last, *refs):
    ringed = not last
    kv_ref, *refs = refs
    sources, up_ref, down_ref, out, refs = refs[:14], refs[14], refs[15], refs[16], refs[17:]
    if ringed:
        full_ref, *refs = refs
    places, refs = refs[:14], refs[14:]
    loads, landing, stream_ref, normed_ref, queries, acc, sums, attended, *refs = refs
    up, down, hidden, wloads, msend, mrecv, *refs = refs
    if ringed:
        *refs, shard, load, local, gsend, grecv = refs
        ring = RingGather(shard, full_ref, local, gsend, grecv)
        fetch = pltpu.make_async_copy(down_ref, shard, load)
        down_ref = full_ref
    *parts, send, recv = refs
    (
        x_ref, h_ref, n_ref, eq_ref, aq_ref, akv_ref, g_ref,
        win_ref, wo_ref, embedding_ref, gain_ref, last_gain_ref, wf_ref, ahead_ref,
    ) = places
    inputs = staged(zip(sources, places), loads)
    wide = up.shape[2]
    ups = [
        pltpu.make_async_copy(up_ref.at[:, pl.ds(k * wide, wide)], up.at[k], wloads.at[k])
        for k in range(up.shape[0])
    ]
    downs = [
        pltpu.make_async_copy(
            down_ref.at[pl.ds(k * 4, 4)], down.at[k], wloads.at[up.shape[0] + k]
        )
        for k in range(down.shape[0])
    ]
    term = parts[0]
    share = rows // 8
    width = heads * HEAD_DIM
    block = pl.program_id(0)
    me, y, c = seat()
    if last:
        mirror = lax.axis_size("seq") - 1 - me
        sends_edge = jnp.logical_and(mirror > 0, 2 * y + c == 7)
        keeps_edge = jnp.logical_and(mirror - 1 == me, 2 * y + c == 7)
        waits_edge = jnp.logical_and(mirror > 0, jnp.logical_not(keeps_edge))

    def scale_of(x, h, n):
        twice = jnp.concatenate([x, x], axis=1)
        quad = jnp.sum(x.astype(F32) * (dot(twice, g_ref[...]) + 2.0 * h), axis=1, keepdims=True)
        return twice, lax.rsqrt(jnp.maximum(quad + n, 0.0) * (1.0 / D) + EPSILON)

    @pl.when(block == 0)
    def _():
        if ringed:
            fetch.start()
        each("start", inputs)
        each("start", ups if ringed else ups + downs)
        if last:
            hail(head_neighbours() + [{"seq": mirror, "head": head} for head in range(8)])

            @pl.when(waits_edge)
            def _():
                hail([{"seq": mirror - 1, "head": 7}])
        else:
            hail_all(landing.shape[0])
            pl.semaphore_wait(pltpu.get_barrier_semaphore(), landing.shape[0])
            fetch.wait()
            ring.begin()
        each("wait", inputs[:7])
        own = pl.ds(pl.multiple_of(me * rows, rows), rows)
        twice, scale = scale_of(x_ref[own, :], h_ref[own, :], n_ref[own, :])
        value = (dot(twice, aq_ref[...]) + eq_ref[...]) * (scale * HEAD_DIM**-0.5)
        queries[...] = value.astype(BF16)
        acc[...] = jnp.zeros_like(acc)
        sums[...] = jnp.zeros_like(sums)

    def step(masked):
        here = pl.ds(pl.multiple_of(block * KEY_BLOCK, KEY_BLOCK), KEY_BLOCK)
        twice, scale = scale_of(x_ref[here, :], h_ref[here, :], n_ref[here, :])
        both = ((dot(twice, akv_ref[...]) + kv_ref[...]) * scale).astype(BF16)
        keys, values = both[:, :width], both[:, width:]
        if masked:
            shape = (rows, KEY_BLOCK)
            row = me * rows + lax.broadcasted_iota(jnp.int32, shape, 0)
            col = block * KEY_BLOCK + lax.broadcasted_iota(jnp.int32, shape, 1)
            seen = col <= row
        for head in range(heads):
            cols = slice(head * HEAD_DIM, (head + 1) * HEAD_DIM)
            scores = dot_t(queries[:, cols], keys[:, cols])
            if masked:
                weights = jnp.where(seen, jnp.exp(jnp.where(seen, scores, 0.0)), 0.0)
            else:
                weights = jnp.exp(scores)
            part = weights[:, :HEAD_DIM]
            for at in range(HEAD_DIM, KEY_BLOCK, HEAD_DIM):
                part = part + weights[:, at : at + HEAD_DIM]
            sums[:, cols] += part
            acc[:, cols] += dot(weights.astype(BF16), values[:, cols])

    final = (me * rows + rows - 1) // KEY_BLOCK

    @pl.when(block < final)
    def _():
        step(False)

    @pl.when(block == final)
    def _():
        step(True)

    def produce(half, part):
        at = part * (HALF // 2)
        cols = slice(half * HALF + at, half * HALF + at + HALF // 2)
        store_terms(term, half, at, share, dot(attended[...], wo_ref[:, cols]))

    def meanwhile():
        first = pl.ds(pl.multiple_of(me * rows + (2 * y + c) * share, share), share)
        stream_ref[...] = dot(x_ref[first, :], win_ref[...]) + embedding_ref[...]

    def between():
        if ringed:
            ring.second()
            ring.middle()

    def midway():
        if ringed:
            ring.third(2)

    def produce_down(half, part):
        k = 2 * half + part
        downs[k].wait()
        weight = down[k].reshape(D // 4, hidden.shape[1])
        store_terms(term, half, part * (HALF // 2), share, dot_t(hidden[...], weight))

    @pl.when(block == pl.num_programs(0) - 1)
    def _():
        for head in range(heads):
            cols = slice(head * HEAD_DIM, (head + 1) * HEAD_DIM)
            total = jnp.sum(sums[:, cols], axis=1, keepdims=True)
            attended[:, cols] = (acc[:, cols] / total).astype(BF16)
        each("wait", inputs[7:])
        if ringed:
            ring.first()
        else:
            barrier = pltpu.get_barrier_semaphore()

            @pl.when(keeps_edge)
            def _():
                pl.semaphore_wait(barrier, 18)

            @pl.when(jnp.logical_and(sends_edge, jnp.logical_not(keeps_edge)))
            def _():
                pl.semaphore_wait(barrier, 19)

            @pl.when(jnp.logical_not(sends_edge))
            def _():
                pl.semaphore_wait(barrier, 11)

        total = reduce_over_head(produce, meanwhile, between, *parts)
        stream = stream_ref[...] + total
        stream_ref[...] = stream
        normed_ref[y, c] = layer_norm(stream, gain_ref[...]).astype(BF16)
        if ringed:
            ring.third(1)
        gather_over_head(normed_ref, send, recv, midway)
        if ringed:
            ring.third(3)
        for k in range(up.shape[0]):
            ups[k].wait()
            pre = dot(normed_ref[...].reshape(rows, D), up[k])
            hidden[:, k * wide : (k + 1) * wide] = jax.nn.gelu(pre, approximate=True).astype(BF16)
        if ringed:
            ring.end()
            each("start", downs)
        total = reduce_over_head(produce_down, lambda: None, lambda: None, *parts)
        normed = layer_norm(stream_ref[...] + total, last_gain_ref[...]).astype(BF16)
        params = dot(normed, wf_ref[...])
        following = ahead_ref[...] * jnp.exp(jnp.tanh(params[:, C:])) + params[:, :C]
        if last:
            finish(following, x_ref[0:16, :][0:1], landing, term, msend, mrecv)
            count = landing.shape[0] * share
            line = lax.broadcasted_iota(jnp.int32, (rows, count), 0)
            column = lax.broadcasted_iota(jnp.int32, (rows, count), 1)
            source = jnp.where(line == rows - 1, count - 1, rows - 2 - line)
            pick = jnp.where(column == source, 1.0, 0.0).astype(BF16)
            out[...] = dot(pick, landing[...].reshape(count, C))
        else:
            landing[me * 4 + y, c] = following.astype(BF16)
            begin, cross, end = spread(landing, msend, mrecv)
            begin()
            cross()
            end()
            before = x_ref[0:16, :].astype(F32)[0:1]
            chunk = 8 * 2 * share
            line = lax.broadcasted_iota(jnp.int32, (chunk, C), 0)
            for k in range(landing.shape[0] // 8):
                value = landing[8 * k : 8 * k + 8].reshape(chunk, C).astype(F32)
                moved = jnp.where(line == 0, before, pltpu.roll(value, 1, 0))
                out[k * chunk : (k + 1) * chunk, :] = moved.astype(BF16)
                before = value[chunk - 1 :]


def finish(following, top, out_ref, term, send, recv):
    seq, y, c = seat()
    mirror = lax.axis_size("seq") - 1 - seq
    sends_edge = jnp.logical_and(mirror > 0, 2 * y + c == 7)
    keeps_edge = jnp.logical_and(mirror - 1 == seq, 2 * y + c == 7)
    waits_edge = jnp.logical_and(mirror > 0, jnp.logical_not(keeps_edge))
    block = term.at[0, 0, 0, :, pl.ds(0, C)]
    block[...] = following.astype(BF16)
    head = 2 * y + c
    moves = [
        pltpu.make_async_remote_copy(
            src_ref=block, dst_ref=out_ref.at[head], send_sem=send.at[k], recv_sem=recv.at[0],
            device_id={"seq": mirror, "head": k}, device_id_type=MESH,
        )
        for k in range(8)
    ]
    edges = [
        pltpu.make_async_remote_copy(
            src_ref=block, dst_ref=out_ref.at[8], send_sem=send.at[8 + k], recv_sem=recv.at[1],
            device_id={"seq": mirror - 1, "head": k}, device_id_type=MESH,
        )
        for k in range(8)
    ]
    for move in moves:
        move.start()

    @pl.when(sends_edge)
    def _():
        for move in edges[:7]:
            move.start()

    @pl.when(jnp.logical_and(sends_edge, jnp.logical_not(keeps_edge)))
    def _():
        edges[7].start()

    whole = out_ref.at[pl.ds(0, 8)]
    pltpu.make_async_remote_copy(
        src_ref=whole, dst_ref=whole, send_sem=send.at[0], recv_sem=recv.at[0],
        device_id={"seq": mirror, "head": 0}, device_id_type=MESH,
    ).wait_recv()

    @pl.when(waits_edge)
    def _():
        pltpu.make_async_remote_copy(
            src_ref=block, dst_ref=out_ref.at[8], send_sem=send.at[0], recv_sem=recv.at[1],
            device_id={"seq": mirror - 1, "head": 7}, device_id_type=MESH,
        ).wait_recv()

    for move in moves:
        move.wait_send()

    @pl.when(sends_edge)
    def _():
        for move in edges[:7]:
            move.wait_send()

    @pl.when(jnp.logical_and(sends_edge, jnp.logical_not(keeps_edge)))
    def _():
        edges[7].wait_send()

    @pl.when(keeps_edge)
    def _():
        out_ref[8] = following.astype(BF16)

    @pl.when(mirror == 0)
    def _():
        out_ref[8] = jnp.broadcast_to(top.astype(F32), following.shape).astype(BF16)


def layer(rows, places, last, state, x, w_in, w_attn_out, embedding, gain, last_gain, w_final, ahead,
          up, down):
    kv = state[0]
    length, width = kv.shape[0], kv.shape[1] // 2
    share, hidden = rows // 8, up.shape[1]
    count = length // rows
    shard = (2, D // count // 2, hidden)
    far = pl.BlockSpec(memory_space=pltpu.HBM)
    tile = pl.BlockSpec((KEY_BLOCK, 2 * width), lambda i: (i, 0))
    sources = [x, *state[1:], w_in, w_attn_out, embedding, gain, last_gain, w_final, ahead]
    shape = (9, share, C) if last else (places, 2, share, C)
    outs = [jax.ShapeDtypeStruct((rows, C), F32) if last else jax.ShapeDtypeStruct((length, C), BF16)]
    if not last:
        outs.append(jax.ShapeDtypeStruct((count, *shard), BF16))
    return pl.pallas_call(
        functools.partial(layer_kernel, rows, width // HEAD_DIM, last),
        grid=(length // KEY_BLOCK,),
        in_specs=[tile] + [far] * 16,
        out_specs=[pl.BlockSpec(memory_space=pltpu.VMEM)] + [far] * (not last),
        out_shape=outs,
        scratch_shapes=[buffer_like(source) for source in sources]
        + [
            pltpu.SemaphoreType.DMA((14,)),
            pltpu.VMEM(shape, BF16),
            pltpu.VMEM((share, D), F32),
            pltpu.VMEM((4, 2, share, D), BF16),
            pltpu.VMEM((rows, width), BF16),
            pltpu.VMEM((rows, width), F32),
            pltpu.VMEM((rows, width), F32),
            pltpu.VMEM((rows, width), BF16),
            pltpu.VMEM((3, D, hidden // 3), BF16),
            pltpu.VMEM((4, count // 4, *shard), BF16),
            pltpu.VMEM((rows, hidden), BF16),
            pltpu.SemaphoreType.DMA((7,)),
            pltpu.SemaphoreType.DMA((16,)),
            pltpu.SemaphoreType.DMA((2,)),
        ]
        + reduce_scratch(share)
        + [pltpu.SemaphoreType.DMA((9,)), pltpu.SemaphoreType.DMA((9,))]
        + ([] if last else [pltpu.VMEM(shard, BF16), pltpu.SemaphoreType.DMA] + ring_scratch()),
        compiler_params=pltpu.CompilerParams(
            collective_id=2 if last else 1, has_side_effects=True, vmem_limit_bytes=60 << 20
        ),
        cost_estimate=pl.CostEstimate(
            flops=60_000_000_000, bytes_accessed=40_000_000, transcendentals=0
        ),
        name="layer_last" if last else "layer",
    )(kv, *sources, up, down)


def per_device(
    latent, w_in, w_query, w_key, w_value, w_attn_out, w_up, w_down, w_final,
    gain_attn, gain_mlp, gain_final,
):
    seq_count, head_count = lax.axis_size("seq"), lax.axis_size("head")
    rows = latent.shape[0]
    length = rows * seq_count
    places = seq_count * head_count // 2

    shape = (2, w_up.shape[0] // 2, w_up.shape[1])
    *state, gathered, ahead, embedding, up = first(
        rows, seq_count, places, latent, gain_attn[None, :], w_query, w_key, w_value, w_in,
        w_up.reshape(shape),
    )
    up = up.reshape(D, w_up.shape[1])
    x = gathered.reshape(length, C)
    down = w_down.T.reshape(shape)
    for step_index in range(ITERS):
        last = step_index == ITERS - 1
        x, *full = layer(
            rows, places, last, state, x, w_in, w_attn_out, embedding, gain_mlp[None, :],
            gain_final[None, :], w_final, ahead, up, down,
        )
        if not last:
            down = full[0]
    return x


def solution(mesh):
    in_specs = (
        P("seq", None),
        P(),
        P(None, "head"),
        P(None, "head"),
        P(None, "head"),
        P("head", None),
        P("seq", "head"),
        P("head", "seq"),
        P(),
        P(),
        P(),
        P(),
    )
    return jax.shard_map(
        per_device, mesh=mesh, in_specs=in_specs, out_specs=P("seq", None), check_vma=False
    )
```

```python
import functools

import jax
import jax.numpy as jnp
import numpy as np
from jax import lax
from jax.experimental import pallas as pl
from jax.experimental.pallas import tpu as pltpu
from jax.sharding import PartitionSpec as P

D = 3072
HALF = D // 2
HEAD_DIM = 128
C = 128
ITERS = 2
EPSILON = 1e-05
KEY_BLOCKS = (512, 1024)
BF16 = jnp.bfloat16
F32 = jnp.float32


def split_two(value):
    high = value.astype(BF16)
    return high, (value - high.astype(F32)).astype(BF16)


def dot(left, right):
    return jnp.dot(left, right, preferred_element_type=F32)


def dot_t(left, right):
    return lax.dot_general(left, right, (((1,), (1,)), ((), ())), preferred_element_type=F32)


def layer_norm(stream, gain):
    center = stream - jnp.mean(stream, axis=-1, keepdims=True)
    spread = jnp.mean(center * center, axis=-1, keepdims=True)
    return center * lax.rsqrt(spread + EPSILON) * gain


def frequencies():
    return np.exp(-np.log(10000.0) * 2.0 * np.arange(HALF) / D).astype(np.float32)[None, :]


MESH = pl.DeviceIdType.MESH


def staged(pairs, sems):
    return [pltpu.make_async_copy(src, dst, sems.at[k]) for k, (src, dst) in enumerate(pairs)]


def each(action, copies):
    for copy in copies:
        getattr(copy, action)()


def buffer_like(array):
    return pltpu.VMEM(array.shape, array.dtype)


def seat():
    head = lax.axis_index("head")
    return lax.axis_index("seq"), lax.div(head, 2), lax.rem(head, 2)


def plus(y, by):
    return lax.rem(y + by, 4)


def hail(targets):
    barrier = pltpu.get_barrier_semaphore()
    for target in targets:
        pl.semaphore_signal(barrier, inc=1, device_id=target, device_id_type=MESH)


def met(targets):
    pl.semaphore_wait(pltpu.get_barrier_semaphore(), len(targets))


def hail_all(devices):
    seq, y, c = seat()
    place = seq * 4 + y
    barrier = pltpu.get_barrier_semaphore()
    pl.semaphore_signal(barrier, inc=1, device_id={"head": 2 * y + 1 - c}, device_id_type=MESH)

    @pl.loop(1, devices)
    def _(k):
        other = lax.rem(place + k, devices)
        pl.semaphore_signal(
            barrier, inc=1,
            device_id={"seq": lax.div(other, 4), "head": 2 * lax.rem(other, 4) + c},
            device_id_type=MESH,
        )


def start_peers(count):
    seq, y, c = seat()
    return (
        [{"seq": lax.rem(seq + k, count)} for k in range(1, count)]
        + [{"head": 2 * plus(y, k) + c} for k in range(1, 4)]
        + [{"head": 2 * y + 1 - c}]
    )


def start_spread(buffer, send, recv):
    seq, y, c = seat()
    count = buffer.shape[0]

    def copy(block, slot, device):
        return pltpu.make_async_remote_copy(
            src_ref=block, dst_ref=block, send_sem=send.at[slot], recv_sem=recv.at[slot],
            device_id=device, device_id_type=MESH,
        )

    partner = {"head": 2 * y + 1 - c}
    plane = copy(buffer.at[pl.ds(0, count - 1), 0, c], 0, partner)
    column = copy(buffer.at[:, pl.ds(0, 3), c], 1, partner)
    across = copy(buffer.at[:, :, c], 2, partner)

    def begin():
        @pl.loop(1, count)
        def _(k):
            copy(buffer.at[seq, y, c], 0, {"seq": lax.rem(seq + k, count)}).start()

    def columns():
        plane.wait_recv()
        for k in range(1, 4):
            copy(buffer.at[:, y, c], 1, {"head": 2 * plus(y, k) + c}).start()

    def cross():
        column.wait_recv()
        across.start()

    def end():
        plane.wait_send()
        column.wait_send()
        across.wait()

    return begin, columns, cross, end


def spread(buffer, send, recv):
    seq, y, c = seat()
    devices = buffer.shape[0]
    place = seq * 4 + y
    partner = {"head": 2 * y + 1 - c}
    whole = buffer.at[pl.ds(0, devices - 1), c]
    arrived = pltpu.make_async_remote_copy(
        src_ref=whole, dst_ref=whole, send_sem=send.at[0], recv_sem=recv.at[0],
        device_id=partner, device_id_type=MESH,
    )
    across = pltpu.make_async_remote_copy(
        src_ref=buffer.at[:, c], dst_ref=buffer.at[:, c], send_sem=send.at[1], recv_sem=recv.at[1],
        device_id=partner, device_id_type=MESH,
    )

    def begin():
        @pl.loop(1, devices)
        def _(k):
            other = lax.rem(place + k, devices)
            pltpu.make_async_remote_copy(
                src_ref=buffer.at[place, c], dst_ref=buffer.at[place, c],
                send_sem=send.at[0], recv_sem=recv.at[0],
                device_id={"seq": lax.div(other, 4), "head": 2 * lax.rem(other, 4) + c},
                device_id_type=MESH,
            ).start()

    def cross():
        arrived.wait_recv()
        across.start()

    def end():
        arrived.wait_send()
        across.wait()

    return begin, cross, end


class RingGather:
    FIRST = (0, 3, 1, 2)

    def __init__(self, own, out, local, send, recv):
        seq = lax.axis_index("seq")
        self.x, self.z = lax.div(seq, 4), lax.rem(seq, 4)
        self.own, self.out, self.send, self.recv = own, out, send, recv
        self.keep = pltpu.make_async_copy(own, out.at[seq], local)

    def place(self, half, p, q):
        x, z = (p, q) if half == 0 else (q, p)
        return plus(self.x, x) * 4 + plus(self.z, z)

    def move(self, half, slot):
        if slot < 4:
            kind, block, target = slot, None, [(1, 0), (3, 0), (1, 0), (3, 0)][slot]
            origin = [(0, 0), (0, 0), (3, 0), (1, 0)][slot]
        else:
            block, kind = divmod(slot - 4, 4)
            target = [(0, 1), (0, 3), (0, 1), (0, 3)][kind]
            origin = (self.FIRST[block], [0, 0, 3, 1][kind])
        ref = self.out.at[self.place(half, *origin), half]
        if kind >= 2:
            part = ref.shape[0] // 2
            ref = ref.at[pl.ds((kind - 2) * part, part)]
        source = self.own.at[half] if origin == (0, 0) else ref
        return pltpu.make_async_remote_copy(
            src_ref=source, dst_ref=ref,
            send_sem=self.send.at[20 * half + slot], recv_sem=self.recv.at[20 * half + slot],
            device_id={"seq": self.place(half, *target)}, device_id_type=MESH,
        )

    def neighbours(self):
        return [{"seq": self.place(0, *at)} for at in ((1, 0), (3, 0), (0, 1), (0, 3))]

    def on(self, slots, *following):
        for half in range(2):
            for slot in slots:
                self.move(half, slot).wait_recv()
            for slot in following:
                self.move(half, slot).start()

    def begin(self):
        self.keep.start()
        self.on((), 0, 1)
        self.on((), 4, 5)

    def first(self):
        self.on((0,), 2, 8, 9)
        self.on((1,), 3, 12, 13)

    def second(self):
        self.on((4,), 6)
        self.on((5,), 7)

    def middle(self):
        self.on((2, 3), 16, 17)

    def third(self, block):
        self.on((4 + 4 * block,), 6 + 4 * block)
        self.on((5 + 4 * block,), 7 + 4 * block)

    def end(self):
        self.on((6, 7, 10, 11, 14, 15, 18, 19))
        self.keep.wait()
        for half in range(2):
            for slot in range(20):
                self.move(half, slot).wait_send()


def first_kernel(
    rows, latent_ref, freq_ref, gain_ref, wq_ref, wk_ref, wv_ref, win_ref, up_ref,
    kv_ref, h_ref, n_ref, eq_out, aq_out, akv_out, g_out, x_out, ahead_out,
    embedding_out, full_ref, eq_ref, aq_ref, akv_ref, g_ref, x_ref, ahead_ref, embedding_ref, stores,
    edge_ref, turn_ref, fine_a, fine_b, shard, scaled_0, scaled_1, high_0, high_1, mean_0, mean_1, base, wkv, gw, wsum, edge_rows,
    loads, xsend, xrecv, local, gsend, grecv,
):
    step, steps = pl.program_id(0), pl.num_programs(0)
    seq, y, c = seat()
    width = wk_ref.shape[1]
    fetches = [
        pltpu.make_async_copy(ref, wkv.at[:, pl.ds(k * width, width)], loads.at[k])
        for k, ref in enumerate((wk_ref, wv_ref))
    ]
    begin, columns, cross, end = start_spread(x_ref, xsend, xrecv)
    count = lax.axis_size("seq")
    edge = pltpu.make_async_remote_copy(
        src_ref=edge_rows, dst_ref=edge_ref, send_sem=xsend.at[3], recv_sem=xrecv.at[3],
        device_id={"seq": lax.rem(seq + count - 1, count)}, device_id_type=MESH,
    )
    ring = RingGather(shard, full_ref, local, gsend, grecv)
    fetches.append(pltpu.make_async_copy(up_ref, shard, loads.at[2]))
    results = staged(
        [
            (eq_ref, eq_out), (aq_ref, aq_out), (akv_ref, akv_out), (g_ref, g_out),
            (x_ref, x_out), (ahead_ref, ahead_out), (embedding_ref, embedding_out),
        ],
        stores,
    )

    def fill(block, scaled, high, mean):
        total = jnp.zeros((rows, 1), F32)
        wide = 512
        for at in range(0, HALF, wide):
            cols = slice(at, at + wide)
            sin_a, cos_a = turn_ref[block, 0:1, cols], turn_ref[block, 1:2, cols]
            sin_b, cos_b = base[0, :, cols], base[1, :, cols]
            for part, offset in (
                (sin_a * cos_b + cos_a * sin_b, 0),
                (cos_a * cos_b - sin_a * sin_b, HALF),
            ):
                into = slice(offset + at, offset + at + wide)
                high[:, into] = part.astype(BF16)
                scaled[:, into] = (part * gain_ref[:, into]).astype(BF16)
                total = total + jnp.sum(part, axis=1, keepdims=True)
        mean[...] = total * (1.0 / D)

    def rows_out():
        edge_rows[...] = latent_ref[0:8, :]
        own = pl.ds(pl.multiple_of((2 * y + c) * (rows // 8), rows // 8), rows // 8)
        x_ref[seq, y, c] = latent_ref[own, :].astype(BF16)

    def tables():
        row = lax.broadcasted_iota(jnp.int32, (16, HALF), 0).astype(F32)
        angle = row * freq_ref[...]
        sines, cosines = jnp.sin(angle), jnp.cos(angle)
        fine_b[0], fine_b[1] = sines, cosines
        for table in (fine_a, turn_ref):
            for _ in range(4):
                sines, cosines = 2.0 * sines * cosines, cosines * cosines - sines * sines
            for k in range(16):
                table[k, 0:1, :] = sines[k : k + 1]
                table[k, 1:2, :] = cosines[k : k + 1]

        @pl.loop(0, rows // 16)
        def _(k):
            sin_a, cos_a = fine_a[k, 0:1, :], fine_a[k, 1:2, :]
            sin_b, cos_b = fine_b[0], fine_b[1]
            into = pl.ds(pl.multiple_of(k * 16, 16), 16)
            base[0, into, :] = sin_a * cos_b + cos_a * sin_b
            base[1, into, :] = cos_a * cos_b - sin_a * sin_b

        share = rows // 8
        own = pl.ds(pl.multiple_of((2 * y + c) * share, share), share)
        sin_a, cos_a = turn_ref[seq, 0:1, :], turn_ref[seq, 1:2, :]
        sin_b, cos_b = base[0, own, :], base[1, own, :]
        embedding_ref[:, 0:HALF] = sin_a * cos_b + cos_a * sin_b
        embedding_ref[:, HALF:] = cos_a * cos_b - sin_a * sin_b
        wsum[...] = dot_t(jnp.ones((16, D), BF16), win_ref[...])
        gain = gain_ref[...]
        high = gain.astype(BF16).astype(F32)
        line = lax.broadcasted_iota(jnp.int32, (16, D), 0)
        both = jnp.where(line == 0, high, jnp.where(line == 1, gain - high, 0.0)).astype(BF16)
        for fetch in fetches[:2]:
            fetch.wait()
        gw[:, 0:width] = dot(both, wq_ref[...])
        gw[:, width:] = dot(both, wkv[...])
        gw[0:1, :] = jnp.sum(gw[...], axis=0, keepdims=True)

    @pl.when(step == 0)
    def _():
        fetches[2].start()
        peers = start_peers(count)
        hail(peers)
        rows_out()
        for fetch in fetches[:2]:
            fetch.start()
        fetches[2].wait()
        met(peers)
        ring.begin()
        begin()
        edge.start()
        tables()
        fill(0, scaled_0, high_0, mean_0)

    def work(scaled, high, mean, others):
        value = mean[...]
        kv_ref[...] = dot(scaled[...], wkv[...]) - value * gw[0:1, width:]
        h_ref[...] = dot_t(high[...], win_ref[...]) - value * wsum[0:1, :]
        n_ref[...] = HALF - D * value * value
        fill(jnp.minimum(step + 1, steps - 1), *others)

        @pl.when(step == seq)
        def _():
            eq_ref[...] = dot(scaled[...], wq_ref[...]) - value * gw[0:1, 0:width]

    even, odd = (scaled_0, high_0, mean_0), (scaled_1, high_1, mean_1)

    @pl.when(lax.rem(step, 2) == 0)
    def _():
        work(*even, odd)

    @pl.when(lax.rem(step, 2) == 1)
    def _():
        work(*odd, even)

    pl.when(step == 3)(columns)
    pl.when(step == 6)(cross)

    for at, event in ((3, ring.first), (7, ring.second), (9, ring.middle)):
        pl.when(step == at)(event)
    for at, block in ((12, 1), (15, 2)):
        pl.when(step == at)(functools.partial(ring.third, block))

    @pl.when(step == steps - 1)
    def _():
        wide = win_ref[...].astype(F32)
        center = wide - jnp.mean(wide, axis=1, keepdims=True)
        high, low = split_two(center * gain_ref[...])
        scaled_0[0:C, :] = high
        scaled_0[C : 2 * C, :] = low
        for into, weight in ((aq_ref, wq_ref), (akv_ref, wkv)):
            both = dot(scaled_0[0 : 2 * C, :], weight[...])
            high, low = split_two(both[:C] + both[C:])
            into[0:C, :] = high
            into[C : 2 * C, :] = low
        ring.third(3)
        high, low = split_two(center)
        high_0[0:C, :] = high
        high_1[0:C, :] = low
        high, low = high_0[0:C, :], high_1[0:C, :]
        high, low = split_two(dot_t(high, high) + dot_t(high, low) + dot_t(low, high))
        g_ref[0:C, :] = high
        g_ref[C : 2 * C, :] = low
        end()
        edge.wait()
        share = rows // 8
        head = 2 * y + c
        own = latent_ref[pl.ds(pl.multiple_of(head * share, share), share), :]
        beyond = pl.multiple_of(jnp.minimum((head + 1) * share, rows - 8), 8)
        beyond = jnp.where(head == 7, edge_ref[0:1, :], latent_ref[pl.ds(beyond, 8), :][0:1])
        line = lax.broadcasted_iota(jnp.int32, (share, C), 0)
        ahead_ref[...] = jnp.where(line == share - 1, beyond, pltpu.roll(own, share - 1, 0))
        each("start", results)
        ring.end()
        each("wait", results)


def ring_scratch():
    return [
        pltpu.SemaphoreType.DMA,
        pltpu.SemaphoreType.DMA((40,)),
        pltpu.SemaphoreType.DMA((40,)),
    ]


def first(rows, blocks, places, latent, gain, w_query, w_key, w_value, w_in, up):
    width = w_key.shape[1]
    length = rows * blocks
    whole = pl.BlockSpec(memory_space=pltpu.VMEM)
    far = pl.BlockSpec(memory_space=pltpu.HBM)
    return pl.pallas_call(
        functools.partial(first_kernel, rows),
        grid=(blocks,),
        in_specs=[whole] * 4 + [far, far, whole, far],
        out_specs=[
            pl.BlockSpec((rows, 2 * width), lambda i: (i, 0)),
            pl.BlockSpec((rows, C), lambda i: (i, 0)),
            pl.BlockSpec((rows, 1), lambda i: (i, 0)),
        ]
        + [far] * 8,
        out_shape=[
            jax.ShapeDtypeStruct((length, 2 * width), F32),
            jax.ShapeDtypeStruct((length, C), F32),
            jax.ShapeDtypeStruct((length, 1), F32),
            jax.ShapeDtypeStruct((rows, width), F32),
            jax.ShapeDtypeStruct((2 * C, width), BF16),
            jax.ShapeDtypeStruct((2 * C, 2 * width), BF16),
            jax.ShapeDtypeStruct((2 * C, C), BF16),
            jax.ShapeDtypeStruct((blocks, 4, 2, rows // 8, C), BF16),
            jax.ShapeDtypeStruct((rows // 8, C), F32),
            jax.ShapeDtypeStruct((rows // 8, D), F32),
            jax.ShapeDtypeStruct((blocks, *up.shape), BF16),
        ],
        scratch_shapes=[
            pltpu.VMEM((rows, width), F32),
            pltpu.VMEM((2 * C, width), BF16),
            pltpu.VMEM((2 * C, 2 * width), BF16),
            pltpu.VMEM((2 * C, C), BF16),
            pltpu.VMEM((blocks, 4, 2, rows // 8, C), BF16),
            pltpu.VMEM((rows // 8, C), F32),
            pltpu.VMEM((rows // 8, D), F32),
            pltpu.SemaphoreType.DMA((7,)),
            pltpu.VMEM((8, C), F32),
            pltpu.VMEM((16, 2, HALF), F32),
            pltpu.VMEM((16, 2, HALF), F32),
            pltpu.VMEM((2, 16, HALF), F32),
            pltpu.VMEM(up.shape, BF16),
        ]
        + [pltpu.VMEM((rows, D), BF16)] * 4
        + [pltpu.VMEM((rows, 1), F32)] * 2
        + [
            pltpu.VMEM((2, rows, HALF), F32),
            pltpu.VMEM((D, 2 * width), BF16),
            pltpu.VMEM((16, 3 * width), F32),
            pltpu.VMEM((16, C), F32),
            pltpu.VMEM((8, C), F32),
            pltpu.SemaphoreType.DMA((3,)),
            pltpu.SemaphoreType.DMA((4,)),
            pltpu.SemaphoreType.DMA((4,)),
        ]
        + ring_scratch(),
        compiler_params=pltpu.CompilerParams(
            collective_id=0, has_side_effects=True, vmem_limit_bytes=56 << 20
        ),
        cost_estimate=pl.CostEstimate(
            flops=60_000_000_000, bytes_accessed=40_000_000, transcendentals=0
        ),
        name="first",
    )(latent, jnp.asarray(frequencies()), gain, w_query, w_key, w_value, w_in, up)


def reduce_over_head(produce, meanwhile, between, term, taken, via_out, via_in, near, fin, send, recv):
    _, y, c = seat()
    partner, up, down = 2 * y + 1 - c, 2 * plus(y, 1) + c, 2 * plus(y, 3) + c

    def copy(src, dst, slot, head):
        return pltpu.make_async_remote_copy(
            src_ref=src, dst_ref=dst, send_sem=send.at[slot], recv_sem=recv.at[slot],
            device_id={"head": head}, device_id_type=MESH,
        )

    def pair(half, at):
        return term[half, at, c].astype(F32) + taken[half, at].astype(F32)

    across, ahead, behind = plus(y, 2), plus(y, 1), plus(y, 3)
    gives = [copy(term.at[half, :, 1 - c], taken.at[half], half, partner) for half in range(2)]
    produce(0, 0)
    produce(0, 1)
    gives[0].start()
    produce(1, 0)
    gives[0].wait_recv()
    via_out[0] = pair(0, across).astype(BF16)
    via_0 = copy(via_out.at[0], via_in.at[0], 2, up)
    via_0.start()
    near[1, 0] = pair(0, behind).astype(BF16)
    down_0 = copy(near.at[1, 0], fin.at[1, 0], 6, down)
    down_0.start()
    produce(1, 1)
    gives[1].start()
    meanwhile()
    gives[1].wait_recv()
    via_out[1] = pair(1, across).astype(BF16)
    via_1 = copy(via_out.at[1], via_in.at[1], 3, down)
    via_1.start()
    near[0, 1] = pair(1, ahead).astype(BF16)
    up_1 = copy(near.at[0, 1], fin.at[0, 1], 5, up)
    up_1.start()
    via_0.wait_recv()
    near[0, 0] = (pair(0, ahead) + via_in[0].astype(F32)).astype(BF16)
    up_0 = copy(near.at[0, 0], fin.at[0, 0], 4, up)
    up_0.start()
    via_1.wait_recv()
    near[1, 1] = (pair(1, behind) + via_in[1].astype(F32)).astype(BF16)
    down_1 = copy(near.at[1, 1], fin.at[1, 1], 7, down)
    down_1.start()
    between()
    sums = [pair(half, y) for half in range(2)]
    down_0.wait_recv()
    up_0.wait_recv()
    first = sums[0] + fin[0, 0].astype(F32) + fin[1, 0].astype(F32)
    up_1.wait_recv()
    down_1.wait_recv()
    second = sums[1] + fin[0, 1].astype(F32) + fin[1, 1].astype(F32)
    for done in (*gives, via_0, via_1, up_0, up_1, down_0, down_1):
        done.wait_send()
    return jnp.concatenate([first, second], axis=1)


def gather_over_head(out, send, recv, midway=lambda: None):
    _, y, c = seat()
    partner, up, down = 2 * y + 1 - c, 2 * plus(y, 1) + c, 2 * plus(y, 3) + c
    across, ahead, behind = plus(y, 2), plus(y, 1), plus(y, 3)
    low, high = pl.ds(0, HALF), pl.ds(HALF, HALF)

    def copy(block, slot, head):
        return pltpu.make_async_remote_copy(
            src_ref=block, dst_ref=block, send_sem=send.at[slot], recv_sem=recv.at[slot],
            device_id={"head": head}, device_id_type=MESH,
        )

    moves = [copy(out.at[y, c], 0, up), copy(out.at[y, c], 1, down), copy(out.at[y, c], 2, partner)]
    for move in moves:
        move.start()

    def then(slot, *following):
        moves[slot].wait_recv()
        for move in following:
            move.start()
            moves.append(move)

    then(0, copy(out.at[behind, c, :, low], 3, up), copy(out.at[behind, c], 4, partner))
    then(1, copy(out.at[ahead, c, :, high], 5, down), copy(out.at[ahead, c], 6, partner))
    midway()
    then(3, copy(out.at[across, c, :, low], 7, partner))
    then(5, copy(out.at[across, c, :, high], 8, partner))
    for slot in (2, 4, 6, 7, 8):
        moves[slot].wait_recv()
    for move in moves:
        move.wait_send()


def reduce_scratch(share):
    return [
        pltpu.VMEM((2, 4, 2, share, HALF), BF16),
        pltpu.VMEM((2, 4, share, HALF), BF16),
        pltpu.VMEM((2, share, HALF), BF16),
        pltpu.VMEM((2, share, HALF), BF16),
        pltpu.VMEM((2, 2, share, HALF), BF16),
        pltpu.VMEM((2, 2, share, HALF), BF16),
        pltpu.SemaphoreType.DMA((8,)),
        pltpu.SemaphoreType.DMA((8,)),
    ]


def head_neighbours():
    _, y, c = seat()
    return [{"head": 2 * y + 1 - c}, {"head": 2 * plus(y, 1) + c}, {"head": 2 * plus(y, 3) + c}]


def store_terms(term, half, at, share, value):
    for block in range(8):
        rows = value[block * share : (block + 1) * share].astype(BF16)
        term[half, block // 2, block % 2, :, at : at + value.shape[1]] = rows


def layer_kernel(rows, heads, last, *refs):
    ringed = not last
    step_keys = KEY_BLOCKS[last]
    kv_ref, *refs = refs
    sources, up_ref, down_ref, out, refs = refs[:14], refs[14], refs[15], refs[16], refs[17:]
    if ringed:
        full_ref, *refs = refs
    places, refs = refs[:14], refs[14:]
    loads, landing, stream_ref, normed_ref, queries, acc, sums, attended, *refs = refs
    up, down, hidden, wloads, msend, mrecv, *refs = refs
    if ringed:
        *refs, shard, load, local, gsend, grecv = refs
        ring = RingGather(shard, full_ref, local, gsend, grecv)
        fetch = pltpu.make_async_copy(down_ref, shard, load)
        down_ref = full_ref
    *parts, send, recv = refs
    (
        x_ref, h_ref, n_ref, eq_ref, aq_ref, akv_ref, g_ref,
        win_ref, wo_ref, embedding_ref, gain_ref, last_gain_ref, wf_ref, ahead_ref,
    ) = places
    inputs = staged(zip(sources, places), loads)
    wide = up.shape[2]
    ups = [
        pltpu.make_async_copy(up_ref.at[:, pl.ds(k * wide, wide)], up.at[k], wloads.at[k])
        for k in range(up.shape[0])
    ]
    downs = [
        pltpu.make_async_copy(
            down_ref.at[pl.ds(k * 4, 4)], down.at[k], wloads.at[up.shape[0] + k]
        )
        for k in range(down.shape[0])
    ]
    term = parts[0]
    share = rows // 8
    width = heads * HEAD_DIM
    block = pl.program_id(0)
    me, y, c = seat()
    if last:
        mirror = lax.axis_size("seq") - 1 - me
        sends_edge = jnp.logical_and(mirror > 0, 2 * y + c == 7)
        keeps_edge = jnp.logical_and(mirror - 1 == me, 2 * y + c == 7)
        waits_edge = jnp.logical_and(mirror > 0, jnp.logical_not(keeps_edge))

    def scale_of(x, h, n):
        twice = jnp.concatenate([x, x], axis=1)
        quad = jnp.sum(x.astype(F32) * (dot(twice, g_ref[...]) + 2.0 * h), axis=1, keepdims=True)
        return twice, lax.rsqrt(jnp.maximum(quad + n, 0.0) * (1.0 / D) + EPSILON)

    @pl.when(block == 0)
    def _():
        if ringed:
            fetch.start()
        each("start", inputs)
        each("start", ups if ringed else ups + downs)
        if last:
            hail(head_neighbours() + [{"seq": mirror, "head": head} for head in range(8)])

            @pl.when(waits_edge)
            def _():
                hail([{"seq": mirror - 1, "head": 7}])
        else:
            hail_all(landing.shape[0])
            pl.semaphore_wait(pltpu.get_barrier_semaphore(), landing.shape[0])
            fetch.wait()
            ring.begin()
        each("wait", inputs[:7])
        own = pl.ds(pl.multiple_of(me * rows, rows), rows)
        twice, scale = scale_of(x_ref[own, :], h_ref[own, :], n_ref[own, :])
        value = (dot(twice, aq_ref[...]) + eq_ref[...]) * (scale * HEAD_DIM**-0.5)
        queries[...] = value.astype(BF16)
        acc[...] = jnp.zeros_like(acc)
        sums[...] = jnp.zeros_like(sums)

    def step(masked):
        here = pl.ds(pl.multiple_of(block * step_keys, step_keys), step_keys)
        twice, scale = scale_of(x_ref[here, :], h_ref[here, :], n_ref[here, :])
        both = ((dot(twice, akv_ref[...]) + kv_ref[...]) * scale).astype(BF16)
        keys, values = both[:, :width], both[:, width:]
        if masked:
            shape = (rows, step_keys)
            row = me * rows + lax.broadcasted_iota(jnp.int32, shape, 0)
            col = block * step_keys + lax.broadcasted_iota(jnp.int32, shape, 1)
            seen = col <= row
        for head in range(heads):
            cols = slice(head * HEAD_DIM, (head + 1) * HEAD_DIM)
            scores = dot_t(queries[:, cols], keys[:, cols])
            if masked:
                weights = jnp.where(seen, jnp.exp(jnp.where(seen, scores, 0.0)), 0.0)
            else:
                weights = jnp.exp(scores)
            part = weights[:, :HEAD_DIM]
            for at in range(HEAD_DIM, step_keys, HEAD_DIM):
                part = part + weights[:, at : at + HEAD_DIM]
            sums[:, cols] += part
            acc[:, cols] += dot(weights.astype(BF16), values[:, cols])

    final = (me * rows + rows - 1) // step_keys

    @pl.when(block < final)
    def _():
        step(False)

    @pl.when(block == final)
    def _():
        step(True)

    def produce(half, part):
        at = part * (HALF // 2)
        cols = slice(half * HALF + at, half * HALF + at + HALF // 2)
        store_terms(term, half, at, share, dot(attended[...], wo_ref[:, cols]))

    def meanwhile():
        first = pl.ds(pl.multiple_of(me * rows + (2 * y + c) * share, share), share)
        stream_ref[...] = dot(x_ref[first, :], win_ref[...]) + embedding_ref[...]

    def between():
        if ringed:
            ring.second()
            ring.middle()

    def midway():
        if ringed:
            ring.third(2)

    def produce_down(half, part):
        k = 2 * half + part
        downs[k].wait()
        weight = down[k].reshape(D // 4, hidden.shape[1])
        store_terms(term, half, part * (HALF // 2), share, dot_t(hidden[...], weight))

    @pl.when(block == pl.num_programs(0) - 1)
    def _():
        for head in range(heads):
            cols = slice(head * HEAD_DIM, (head + 1) * HEAD_DIM)
            total = jnp.sum(sums[:, cols], axis=1, keepdims=True)
            attended[:, cols] = (acc[:, cols] / total).astype(BF16)
        each("wait", inputs[7:])
        if ringed:
            ring.first()
        else:
            barrier = pltpu.get_barrier_semaphore()

            @pl.when(keeps_edge)
            def _():
                pl.semaphore_wait(barrier, 18)

            @pl.when(jnp.logical_and(sends_edge, jnp.logical_not(keeps_edge)))
            def _():
                pl.semaphore_wait(barrier, 19)

            @pl.when(jnp.logical_not(sends_edge))
            def _():
                pl.semaphore_wait(barrier, 11)

        total = reduce_over_head(produce, meanwhile, between, *parts)
        stream = stream_ref[...] + total
        stream_ref[...] = stream
        normed_ref[y, c] = layer_norm(stream, gain_ref[...]).astype(BF16)
        if ringed:
            ring.third(1)
        gather_over_head(normed_ref, send, recv, midway)
        if ringed:
            ring.third(3)
        for k in range(up.shape[0]):
            ups[k].wait()
            pre = dot(normed_ref[...].reshape(rows, D), up[k])
            hidden[:, k * wide : (k + 1) * wide] = jax.nn.gelu(pre, approximate=True).astype(BF16)
        if ringed:
            ring.end()
            each("start", downs)
        total = reduce_over_head(produce_down, lambda: None, lambda: None, *parts)
        normed = layer_norm(stream_ref[...] + total, last_gain_ref[...]).astype(BF16)
        params = dot(normed, wf_ref[...])
        following = ahead_ref[...] * jnp.exp(jnp.tanh(params[:, C:])) + params[:, :C]
        if last:
            finish(following, x_ref[0:16, :][0:1], landing, term, msend, mrecv)
            count = landing.shape[0] * share
            line = lax.broadcasted_iota(jnp.int32, (rows, count), 0)
            column = lax.broadcasted_iota(jnp.int32, (rows, count), 1)
            source = jnp.where(line == rows - 1, count - 1, rows - 2 - line)
            pick = jnp.where(column == source, 1.0, 0.0).astype(BF16)
            out[...] = dot(pick, landing[...].reshape(count, C)).astype(BF16)
        else:
            landing[me * 4 + y, c] = following.astype(BF16)
            begin, cross, end = spread(landing, msend, mrecv)
            begin()
            cross()
            end()
            before = x_ref[0:16, :].astype(F32)[0:1]
            chunk = 8 * 2 * share
            line = lax.broadcasted_iota(jnp.int32, (chunk, C), 0)
            for k in range(landing.shape[0] // 8):
                value = landing[8 * k : 8 * k + 8].reshape(chunk, C).astype(F32)
                moved = jnp.where(line == 0, before, pltpu.roll(value, 1, 0))
                out[k * chunk : (k + 1) * chunk, :] = moved.astype(BF16)
                before = value[chunk - 1 :]


def finish(following, top, out_ref, term, send, recv):
    seq, y, c = seat()
    mirror = lax.axis_size("seq") - 1 - seq
    sends_edge = jnp.logical_and(mirror > 0, 2 * y + c == 7)
    keeps_edge = jnp.logical_and(mirror - 1 == seq, 2 * y + c == 7)
    waits_edge = jnp.logical_and(mirror > 0, jnp.logical_not(keeps_edge))
    block = term.at[0, 0, 0, :, pl.ds(0, C)]
    block[...] = following.astype(BF16)
    head = 2 * y + c
    moves = [
        pltpu.make_async_remote_copy(
            src_ref=block, dst_ref=out_ref.at[head], send_sem=send.at[k], recv_sem=recv.at[0],
            device_id={"seq": mirror, "head": k}, device_id_type=MESH,
        )
        for k in range(8)
    ]
    edges = [
        pltpu.make_async_remote_copy(
            src_ref=block, dst_ref=out_ref.at[8], send_sem=send.at[8 + k], recv_sem=recv.at[1],
            device_id={"seq": mirror - 1, "head": k}, device_id_type=MESH,
        )
        for k in range(8)
    ]
    for move in moves:
        move.start()

    @pl.when(sends_edge)
    def _():
        for move in edges[:7]:
            move.start()

    @pl.when(jnp.logical_and(sends_edge, jnp.logical_not(keeps_edge)))
    def _():
        edges[7].start()

    whole = out_ref.at[pl.ds(0, 8)]
    pltpu.make_async_remote_copy(
        src_ref=whole, dst_ref=whole, send_sem=send.at[0], recv_sem=recv.at[0],
        device_id={"seq": mirror, "head": 0}, device_id_type=MESH,
    ).wait_recv()

    @pl.when(waits_edge)
    def _():
        pltpu.make_async_remote_copy(
            src_ref=block, dst_ref=out_ref.at[8], send_sem=send.at[0], recv_sem=recv.at[1],
            device_id={"seq": mirror - 1, "head": 7}, device_id_type=MESH,
        ).wait_recv()

    for move in moves:
        move.wait_send()

    @pl.when(sends_edge)
    def _():
        for move in edges[:7]:
            move.wait_send()

    @pl.when(jnp.logical_and(sends_edge, jnp.logical_not(keeps_edge)))
    def _():
        edges[7].wait_send()

    @pl.when(keeps_edge)
    def _():
        out_ref[8] = following.astype(BF16)

    @pl.when(mirror == 0)
    def _():
        out_ref[8] = jnp.broadcast_to(top.astype(F32), following.shape).astype(BF16)


def layer(rows, places, last, state, x, w_in, w_attn_out, embedding, gain, last_gain, w_final, ahead,
          up, down):
    kv = state[0]
    length, width = kv.shape[0], kv.shape[1] // 2
    step_keys = KEY_BLOCKS[last]
    share, hidden = rows // 8, up.shape[1]
    count = length // rows
    shard = (2, D // count // 2, hidden)
    far = pl.BlockSpec(memory_space=pltpu.HBM)
    tile = pl.BlockSpec((step_keys, 2 * width), lambda i: (i, 0))
    sources = [x, *state[1:], w_in, w_attn_out, embedding, gain, last_gain, w_final, ahead]
    shape = (9, share, C) if last else (places, 2, share, C)
    outs = [jax.ShapeDtypeStruct((rows, C), BF16) if last else jax.ShapeDtypeStruct((length, C), BF16)]
    if not last:
        outs.append(jax.ShapeDtypeStruct((count, *shard), BF16))
    return pl.pallas_call(
        functools.partial(layer_kernel, rows, width // HEAD_DIM, last),
        grid=(length // step_keys,),
        in_specs=[tile] + [far] * 16,
        out_specs=[pl.BlockSpec(memory_space=pltpu.VMEM)] + [far] * (not last),
        out_shape=outs,
        scratch_shapes=[buffer_like(source) for source in sources]
        + [
            pltpu.SemaphoreType.DMA((14,)),
            pltpu.VMEM(shape, BF16),
            pltpu.VMEM((share, D), F32),
            pltpu.VMEM((4, 2, share, D), BF16),
            pltpu.VMEM((rows, width), BF16),
            pltpu.VMEM((rows, width), F32),
            pltpu.VMEM((rows, width), F32),
            pltpu.VMEM((rows, width), BF16),
            pltpu.VMEM((3, D, hidden // 3), BF16),
            pltpu.VMEM((4, count // 4, *shard), BF16),
            pltpu.VMEM((rows, hidden), BF16),
            pltpu.SemaphoreType.DMA((7,)),
            pltpu.SemaphoreType.DMA((16,)),
            pltpu.SemaphoreType.DMA((2,)),
        ]
        + reduce_scratch(share)
        + [pltpu.SemaphoreType.DMA((9,)), pltpu.SemaphoreType.DMA((9,))]
        + ([] if last else [pltpu.VMEM(shard, BF16), pltpu.SemaphoreType.DMA] + ring_scratch()),
        compiler_params=pltpu.CompilerParams(
            collective_id=2 if last else 1, has_side_effects=True, vmem_limit_bytes=60 << 20,
        ),
        cost_estimate=pl.CostEstimate(
            flops=60_000_000_000, bytes_accessed=40_000_000, transcendentals=0
        ),
        name="layer_last" if last else "layer",
    )(kv, *sources, up, down)


def per_device(
    latent, w_in, w_query, w_key, w_value, w_attn_out, w_up, w_down, w_final,
    gain_attn, gain_mlp, gain_final,
):
    seq_count, head_count = lax.axis_size("seq"), lax.axis_size("head")
    rows = latent.shape[0]
    length = rows * seq_count
    places = seq_count * head_count // 2

    shape = (2, w_up.shape[0] // 2, w_up.shape[1])
    *state, gathered, ahead, embedding, up = first(
        rows, seq_count, places, latent, gain_attn[None, :], w_query, w_key, w_value, w_in,
        w_up.reshape(shape),
    )
    up = up.reshape(D, w_up.shape[1])
    x = gathered.reshape(length, C)
    down = w_down.T.reshape(shape)
    for step_index in range(ITERS):
        last = step_index == ITERS - 1
        x, *full = layer(
            rows, places, last, state, x, w_in, w_attn_out, embedding, gain_mlp[None, :],
            gain_final[None, :], w_final, ahead, up, down,
        )
        if not last:
            down = full[0]
    return x.astype(F32)


def solution(mesh):
    in_specs = (
        P("seq", None),
        P(),
        P(None, "head"),
        P(None, "head"),
        P(None, "head"),
        P("head", None),
        P("seq", "head"),
        P("head", "seq"),
        P(),
        P(),
        P(),
        P(),
    )
    return jax.shard_map(
        per_device, mesh=mesh, in_specs=in_specs, out_specs=P("seq", None), check_vma=False
    )
```

```python
import functools

import jax
import jax.numpy as jnp
import numpy as np
from jax import lax
from jax.experimental import pallas as pl
from jax.experimental.pallas import tpu as pltpu
from jax.sharding import PartitionSpec as P

D = 3072
HALF = D // 2
HEAD_DIM = 128
C = 128
ITERS = 2
EPSILON = 1e-05
KEY_BLOCKS = (512, 1024)
BF16 = jnp.bfloat16
F32 = jnp.float32


def split_two(value):
    high = value.astype(BF16)
    return high, (value - high.astype(F32)).astype(BF16)


def dot(left, right):
    return jnp.dot(left, right, preferred_element_type=F32)


def dot_t(left, right):
    return lax.dot_general(left, right, (((1,), (1,)), ((), ())), preferred_element_type=F32)


def layer_norm(stream, gain):
    center = stream - jnp.mean(stream, axis=-1, keepdims=True)
    spread = jnp.mean(center * center, axis=-1, keepdims=True)
    return center * lax.rsqrt(spread + EPSILON) * gain


def frequencies():
    return np.exp(-np.log(10000.0) * 2.0 * np.arange(HALF) / D).astype(np.float32)[None, :]


MESH = pl.DeviceIdType.MESH


def staged(pairs, sems):
    return [pltpu.make_async_copy(src, dst, sems.at[k]) for k, (src, dst) in enumerate(pairs)]


def each(action, copies):
    for copy in copies:
        getattr(copy, action)()


def buffer_like(array):
    return pltpu.VMEM(array.shape, array.dtype)


def seat():
    head = lax.axis_index("head")
    return lax.axis_index("seq"), lax.div(head, 2), lax.rem(head, 2)


def plus(y, by):
    return lax.rem(y + by, 4)


def hail(targets):
    barrier = pltpu.get_barrier_semaphore()
    for target in targets:
        pl.semaphore_signal(barrier, inc=1, device_id=target, device_id_type=MESH)


def met(targets):
    pl.semaphore_wait(pltpu.get_barrier_semaphore(), len(targets))


def hail_all(devices):
    seq, y, c = seat()
    place = seq * 4 + y
    barrier = pltpu.get_barrier_semaphore()
    pl.semaphore_signal(barrier, inc=1, device_id={"head": 2 * y + 1 - c}, device_id_type=MESH)

    @pl.loop(1, devices)
    def _(k):
        other = lax.rem(place + k, devices)
        pl.semaphore_signal(
            barrier, inc=1,
            device_id={"seq": lax.div(other, 4), "head": 2 * lax.rem(other, 4) + c},
            device_id_type=MESH,
        )


def start_peers(count):
    seq, y, c = seat()
    return (
        [{"seq": lax.rem(seq + k, count)} for k in range(1, count)]
        + [{"head": 2 * plus(y, k) + c} for k in range(1, 4)]
        + [{"head": 2 * y + 1 - c}]
    )


def start_spread(buffer, send, recv):
    seq, y, c = seat()
    count = buffer.shape[0]

    def copy(block, slot, device):
        return pltpu.make_async_remote_copy(
            src_ref=block, dst_ref=block, send_sem=send.at[slot], recv_sem=recv.at[slot],
            device_id=device, device_id_type=MESH,
        )

    partner = {"head": 2 * y + 1 - c}
    plane = copy(buffer.at[pl.ds(0, count - 1), 0, c], 0, partner)
    column = copy(buffer.at[:, pl.ds(0, 3), c], 1, partner)
    across = copy(buffer.at[:, :, c], 2, partner)

    def begin():
        @pl.loop(1, count)
        def _(k):
            copy(buffer.at[seq, y, c], 0, {"seq": lax.rem(seq + k, count)}).start()

    def columns():
        plane.wait_recv()
        for k in range(1, 4):
            copy(buffer.at[:, y, c], 1, {"head": 2 * plus(y, k) + c}).start()

    def cross():
        column.wait_recv()
        across.start()

    def end():
        plane.wait_send()
        column.wait_send()
        across.wait()

    return begin, columns, cross, end


def spread(buffer, send, recv):
    seq, y, c = seat()
    devices = buffer.shape[0]
    place = seq * 4 + y
    partner = {"head": 2 * y + 1 - c}
    whole = buffer.at[pl.ds(0, devices - 1), c]
    arrived = pltpu.make_async_remote_copy(
        src_ref=whole, dst_ref=whole, send_sem=send.at[0], recv_sem=recv.at[0],
        device_id=partner, device_id_type=MESH,
    )
    across = pltpu.make_async_remote_copy(
        src_ref=buffer.at[:, c], dst_ref=buffer.at[:, c], send_sem=send.at[1], recv_sem=recv.at[1],
        device_id=partner, device_id_type=MESH,
    )

    def begin():
        @pl.loop(1, devices)
        def _(k):
            other = lax.rem(place + k, devices)
            pltpu.make_async_remote_copy(
                src_ref=buffer.at[place, c], dst_ref=buffer.at[place, c],
                send_sem=send.at[0], recv_sem=recv.at[0],
                device_id={"seq": lax.div(other, 4), "head": 2 * lax.rem(other, 4) + c},
                device_id_type=MESH,
            ).start()

    def cross():
        arrived.wait_recv()
        across.start()
        across.wait_recv()

    def end():
        arrived.wait_send()
        across.wait_send()

    return begin, cross, end


class RingGather:
    FIRST = (0, 3, 1, 2)

    def __init__(self, own, out, local, send, recv):
        seq = lax.axis_index("seq")
        self.x, self.z = lax.div(seq, 4), lax.rem(seq, 4)
        self.own, self.out, self.send, self.recv = own, out, send, recv
        self.keep = pltpu.make_async_copy(own, out.at[seq], local)

    def place(self, half, p, q):
        x, z = (p, q) if half == 0 else (q, p)
        return plus(self.x, x) * 4 + plus(self.z, z)

    def move(self, half, slot):
        if slot < 4:
            kind, block, target = slot, None, [(1, 0), (3, 0), (1, 0), (3, 0)][slot]
            origin = [(0, 0), (0, 0), (3, 0), (1, 0)][slot]
        else:
            block, kind = divmod(slot - 4, 4)
            target = [(0, 1), (0, 3), (0, 1), (0, 3)][kind]
            origin = (self.FIRST[block], [0, 0, 3, 1][kind])
        ref = self.out.at[self.place(half, *origin), half]
        if kind >= 2:
            part = ref.shape[0] // 2
            ref = ref.at[pl.ds((kind - 2) * part, part)]
        source = self.own.at[half] if origin == (0, 0) else ref
        return pltpu.make_async_remote_copy(
            src_ref=source, dst_ref=ref,
            send_sem=self.send.at[20 * half + slot], recv_sem=self.recv.at[20 * half + slot],
            device_id={"seq": self.place(half, *target)}, device_id_type=MESH,
        )

    def neighbours(self):
        return [{"seq": self.place(0, *at)} for at in ((1, 0), (3, 0), (0, 1), (0, 3))]

    def on(self, slots, *following):
        for half in range(2):
            for slot in slots:
                self.move(half, slot).wait_recv()
            for slot in following:
                self.move(half, slot).start()

    def begin(self):
        self.keep.start()
        self.on((), 0, 1)
        self.on((), 4, 5)

    def first(self):
        self.on((0,), 2, 8, 9)
        self.on((1,), 3, 12, 13)

    def second(self):
        self.on((4,), 6)
        self.on((5,), 7)

    def middle(self):
        self.on((2, 3), 16, 17)

    def third(self, block):
        self.on((4 + 4 * block,), 6 + 4 * block)
        self.on((5 + 4 * block,), 7 + 4 * block)

    def end(self):
        self.arrive()
        self.flush()

    def arrive(self):
        self.on((6, 7, 10, 11, 14, 15, 18, 19))
        self.keep.wait()

    def flush(self):
        for half in range(2):
            for slot in range(20):
                self.move(half, slot).wait_send()


def first_kernel(
    rows, latent_ref, freq_ref, gain_ref, wq_ref, wk_ref, wv_ref, win_ref, up_ref,
    kv_ref, h_ref, n_ref, eq_out, aq_out, akv_out, g_out, x_out, ahead_out,
    embedding_out, full_ref, eq_ref, aq_ref, akv_ref, g_ref, x_ref, ahead_ref, embedding_ref, stores,
    edge_ref, turn_ref, fine_a, fine_b, shard, scaled_0, scaled_1, high_0, high_1, mean_0, mean_1, base, wkv, gw, wsum, edge_rows,
    loads, xsend, xrecv, local, gsend, grecv,
):
    step, steps = pl.program_id(0), pl.num_programs(0)
    seq, y, c = seat()
    width = wk_ref.shape[1]
    fetches = [
        pltpu.make_async_copy(ref, wkv.at[:, pl.ds(k * width, width)], loads.at[k])
        for k, ref in enumerate((wk_ref, wv_ref))
    ]
    begin, columns, cross, end = start_spread(x_ref, xsend, xrecv)
    count = lax.axis_size("seq")
    edge = pltpu.make_async_remote_copy(
        src_ref=edge_rows, dst_ref=edge_ref, send_sem=xsend.at[3], recv_sem=xrecv.at[3],
        device_id={"seq": lax.rem(seq + count - 1, count)}, device_id_type=MESH,
    )
    ring = RingGather(shard, full_ref, local, gsend, grecv)
    fetches.append(pltpu.make_async_copy(up_ref, shard, loads.at[2]))
    results = staged(
        [
            (eq_ref, eq_out), (aq_ref, aq_out), (akv_ref, akv_out), (g_ref, g_out),
            (x_ref, x_out), (ahead_ref, ahead_out), (embedding_ref, embedding_out),
        ],
        stores,
    )

    def fill(block, scaled, high, mean):
        total = jnp.zeros((rows, 1), F32)
        wide = 512
        for at in range(0, HALF, wide):
            cols = slice(at, at + wide)
            sin_a, cos_a = turn_ref[block, 0:1, cols], turn_ref[block, 1:2, cols]
            sin_b, cos_b = base[0, :, cols], base[1, :, cols]
            for part, offset in (
                (sin_a * cos_b + cos_a * sin_b, 0),
                (cos_a * cos_b - sin_a * sin_b, HALF),
            ):
                into = slice(offset + at, offset + at + wide)
                high[:, into] = part.astype(BF16)
                scaled[:, into] = (part * gain_ref[:, into]).astype(BF16)
                total = total + jnp.sum(part, axis=1, keepdims=True)
        mean[...] = total * (1.0 / D)

    def rows_out():
        edge_rows[...] = latent_ref[0:8, :]
        own = pl.ds(pl.multiple_of((2 * y + c) * (rows // 8), rows // 8), rows // 8)
        x_ref[seq, y, c] = latent_ref[own, :].astype(BF16)

    def tables():
        row = lax.broadcasted_iota(jnp.int32, (16, HALF), 0).astype(F32)
        angle = row * freq_ref[...]
        sines, cosines = jnp.sin(angle), jnp.cos(angle)
        fine_b[0], fine_b[1] = sines, cosines
        for table in (fine_a, turn_ref):
            for _ in range(4):
                sines, cosines = 2.0 * sines * cosines, cosines * cosines - sines * sines
            for k in range(16):
                table[k, 0:1, :] = sines[k : k + 1]
                table[k, 1:2, :] = cosines[k : k + 1]

        @pl.loop(0, rows // 16)
        def _(k):
            sin_a, cos_a = fine_a[k, 0:1, :], fine_a[k, 1:2, :]
            sin_b, cos_b = fine_b[0], fine_b[1]
            into = pl.ds(pl.multiple_of(k * 16, 16), 16)
            base[0, into, :] = sin_a * cos_b + cos_a * sin_b
            base[1, into, :] = cos_a * cos_b - sin_a * sin_b

        share = rows // 8
        own = pl.ds(pl.multiple_of((2 * y + c) * share, share), share)
        sin_a, cos_a = turn_ref[seq, 0:1, :], turn_ref[seq, 1:2, :]
        sin_b, cos_b = base[0, own, :], base[1, own, :]
        embedding_ref[:, 0:HALF] = sin_a * cos_b + cos_a * sin_b
        embedding_ref[:, HALF:] = cos_a * cos_b - sin_a * sin_b
        wsum[...] = dot_t(jnp.ones((16, D), BF16), win_ref[...])
        gain = gain_ref[...]
        high = gain.astype(BF16).astype(F32)
        line = lax.broadcasted_iota(jnp.int32, (16, D), 0)
        both = jnp.where(line == 0, high, jnp.where(line == 1, gain - high, 0.0)).astype(BF16)
        for fetch in fetches[:2]:
            fetch.wait()
        gw[:, 0:width] = dot(both, wq_ref[...])
        gw[:, width:] = dot(both, wkv[...])
        gw[0:1, :] = jnp.sum(gw[...], axis=0, keepdims=True)

    @pl.when(step == 0)
    def _():
        fetches[2].start()
        peers = start_peers(count)
        hail(peers)
        rows_out()
        for fetch in fetches[:2]:
            fetch.start()
        fetches[2].wait()
        met(peers)
        ring.begin()
        begin()
        edge.start()
        tables()
        fill(0, scaled_0, high_0, mean_0)

    def work(scaled, high, mean, others):
        value = mean[...]
        kv_ref[...] = dot(scaled[...], wkv[...]) - value * gw[0:1, width:]
        h_ref[...] = dot_t(high[...], win_ref[...]) - value * wsum[0:1, :]
        n_ref[...] = HALF - D * value * value
        fill(jnp.minimum(step + 1, steps - 1), *others)

        @pl.when(step == seq)
        def _():
            eq_ref[...] = dot(scaled[...], wq_ref[...]) - value * gw[0:1, 0:width]

    even, odd = (scaled_0, high_0, mean_0), (scaled_1, high_1, mean_1)

    @pl.when(lax.rem(step, 2) == 0)
    def _():
        work(*even, odd)

    @pl.when(lax.rem(step, 2) == 1)
    def _():
        work(*odd, even)

    pl.when(step == 3)(columns)
    pl.when(step == 6)(cross)

    for at, event in ((3, ring.first), (7, ring.second), (9, ring.middle)):
        pl.when(step == at)(event)
    for at, block in ((12, 1), (15, 2)):
        pl.when(step == at)(functools.partial(ring.third, block))

    @pl.when(step == steps - 1)
    def _():
        wide = win_ref[...].astype(F32)
        center = wide - jnp.mean(wide, axis=1, keepdims=True)
        high, low = split_two(center * gain_ref[...])
        scaled_0[0:C, :] = high
        scaled_0[C : 2 * C, :] = low
        for into, weight in ((aq_ref, wq_ref), (akv_ref, wkv)):
            both = dot(scaled_0[0 : 2 * C, :], weight[...])
            high, low = split_two(both[:C] + both[C:])
            into[0:C, :] = high
            into[C : 2 * C, :] = low
        ring.third(3)
        high, low = split_two(center)
        high_0[0:C, :] = high
        high_1[0:C, :] = low
        high, low = high_0[0:C, :], high_1[0:C, :]
        high, low = split_two(dot_t(high, high) + dot_t(high, low) + dot_t(low, high))
        g_ref[0:C, :] = high
        g_ref[C : 2 * C, :] = low
        end()
        edge.wait()
        share = rows // 8
        head = 2 * y + c
        own = latent_ref[pl.ds(pl.multiple_of(head * share, share), share), :]
        beyond = pl.multiple_of(jnp.minimum((head + 1) * share, rows - 8), 8)
        beyond = jnp.where(head == 7, edge_ref[0:1, :], latent_ref[pl.ds(beyond, 8), :][0:1])
        line = lax.broadcasted_iota(jnp.int32, (share, C), 0)
        ahead_ref[...] = jnp.where(line == share - 1, beyond, pltpu.roll(own, share - 1, 0))
        each("start", results)
        ring.end()
        each("wait", results)


def ring_scratch():
    return [
        pltpu.SemaphoreType.DMA,
        pltpu.SemaphoreType.DMA((40,)),
        pltpu.SemaphoreType.DMA((40,)),
    ]


def first(rows, blocks, places, latent, gain, w_query, w_key, w_value, w_in, up):
    width = w_key.shape[1]
    length = rows * blocks
    whole = pl.BlockSpec(memory_space=pltpu.VMEM)
    far = pl.BlockSpec(memory_space=pltpu.HBM)
    return pl.pallas_call(
        functools.partial(first_kernel, rows),
        grid=(blocks,),
        in_specs=[whole] * 4 + [far, far, whole, far],
        out_specs=[
            pl.BlockSpec((rows, 2 * width), lambda i: (i, 0)),
            pl.BlockSpec((rows, C), lambda i: (i, 0)),
            pl.BlockSpec((rows, 1), lambda i: (i, 0)),
        ]
        + [far] * 8,
        out_shape=[
            jax.ShapeDtypeStruct((length, 2 * width), F32),
            jax.ShapeDtypeStruct((length, C), F32),
            jax.ShapeDtypeStruct((length, 1), F32),
            jax.ShapeDtypeStruct((rows, width), F32),
            jax.ShapeDtypeStruct((2 * C, width), BF16),
            jax.ShapeDtypeStruct((2 * C, 2 * width), BF16),
            jax.ShapeDtypeStruct((2 * C, C), BF16),
            jax.ShapeDtypeStruct((blocks, 4, 2, rows // 8, C), BF16),
            jax.ShapeDtypeStruct((rows // 8, C), F32),
            jax.ShapeDtypeStruct((rows // 8, D), F32),
            jax.ShapeDtypeStruct((blocks, *up.shape), BF16),
        ],
        scratch_shapes=[
            pltpu.VMEM((rows, width), F32),
            pltpu.VMEM((2 * C, width), BF16),
            pltpu.VMEM((2 * C, 2 * width), BF16),
            pltpu.VMEM((2 * C, C), BF16),
            pltpu.VMEM((blocks, 4, 2, rows // 8, C), BF16),
            pltpu.VMEM((rows // 8, C), F32),
            pltpu.VMEM((rows // 8, D), F32),
            pltpu.SemaphoreType.DMA((7,)),
            pltpu.VMEM((8, C), F32),
            pltpu.VMEM((16, 2, HALF), F32),
            pltpu.VMEM((16, 2, HALF), F32),
            pltpu.VMEM((2, 16, HALF), F32),
            pltpu.VMEM(up.shape, BF16),
        ]
        + [pltpu.VMEM((rows, D), BF16)] * 4
        + [pltpu.VMEM((rows, 1), F32)] * 2
        + [
            pltpu.VMEM((2, rows, HALF), F32),
            pltpu.VMEM((D, 2 * width), BF16),
            pltpu.VMEM((16, 3 * width), F32),
            pltpu.VMEM((16, C), F32),
            pltpu.VMEM((8, C), F32),
            pltpu.SemaphoreType.DMA((3,)),
            pltpu.SemaphoreType.DMA((4,)),
            pltpu.SemaphoreType.DMA((4,)),
        ]
        + ring_scratch(),
        compiler_params=pltpu.CompilerParams(
            collective_id=0, has_side_effects=True, vmem_limit_bytes=56 << 20
        ),
        cost_estimate=pl.CostEstimate(
            flops=60_000_000_000, bytes_accessed=40_000_000, transcendentals=0
        ),
        name="first",
    )(latent, jnp.asarray(frequencies()), gain, w_query, w_key, w_value, w_in, up)


def reduce_over_head(produce, meanwhile, between, term, taken, via_out, via_in, near, fin, send, recv):
    _, y, c = seat()
    partner, up, down = 2 * y + 1 - c, 2 * plus(y, 1) + c, 2 * plus(y, 3) + c

    def copy(src, dst, slot, head):
        return pltpu.make_async_remote_copy(
            src_ref=src, dst_ref=dst, send_sem=send.at[slot], recv_sem=recv.at[slot],
            device_id={"head": head}, device_id_type=MESH,
        )

    def pair(half, at):
        return term[half, at, c].astype(F32) + taken[half, at].astype(F32)

    across, ahead, behind = plus(y, 2), plus(y, 1), plus(y, 3)
    gives = [copy(term.at[half, :, 1 - c], taken.at[half], half, partner) for half in range(2)]
    produce(0, 0)
    produce(0, 1)
    gives[0].start()
    produce(1, 0)
    gives[0].wait_recv()
    via_out[0] = pair(0, across).astype(BF16)
    via_0 = copy(via_out.at[0], via_in.at[0], 2, up)
    via_0.start()
    near[1, 0] = pair(0, behind).astype(BF16)
    down_0 = copy(near.at[1, 0], fin.at[1, 0], 6, down)
    down_0.start()
    produce(1, 1)
    gives[1].start()
    meanwhile()
    gives[1].wait_recv()
    via_out[1] = pair(1, across).astype(BF16)
    via_1 = copy(via_out.at[1], via_in.at[1], 3, down)
    via_1.start()
    near[0, 1] = pair(1, ahead).astype(BF16)
    up_1 = copy(near.at[0, 1], fin.at[0, 1], 5, up)
    up_1.start()
    via_0.wait_recv()
    near[0, 0] = (pair(0, ahead) + via_in[0].astype(F32)).astype(BF16)
    up_0 = copy(near.at[0, 0], fin.at[0, 0], 4, up)
    up_0.start()
    via_1.wait_recv()
    near[1, 1] = (pair(1, behind) + via_in[1].astype(F32)).astype(BF16)
    down_1 = copy(near.at[1, 1], fin.at[1, 1], 7, down)
    down_1.start()
    between()
    sums = [pair(half, y) for half in range(2)]
    down_0.wait_recv()
    up_0.wait_recv()
    first = sums[0] + fin[0, 0].astype(F32) + fin[1, 0].astype(F32)
    up_1.wait_recv()
    down_1.wait_recv()
    second = sums[1] + fin[0, 1].astype(F32) + fin[1, 1].astype(F32)
    for done in (*gives, via_0, via_1, up_0, up_1, down_0, down_1):
        done.wait_send()
    return jnp.concatenate([first, second], axis=1)


def gather_over_head(out, send, recv, midway=lambda: None):
    _, y, c = seat()
    partner, up, down = 2 * y + 1 - c, 2 * plus(y, 1) + c, 2 * plus(y, 3) + c
    across, ahead, behind = plus(y, 2), plus(y, 1), plus(y, 3)
    low, high = pl.ds(0, HALF), pl.ds(HALF, HALF)

    def copy(block, slot, head):
        return pltpu.make_async_remote_copy(
            src_ref=block, dst_ref=block, send_sem=send.at[slot], recv_sem=recv.at[slot],
            device_id={"head": head}, device_id_type=MESH,
        )

    moves = [copy(out.at[y, c], 0, up), copy(out.at[y, c], 1, down), copy(out.at[y, c], 2, partner)]
    for move in moves:
        move.start()

    def then(slot, *following):
        moves[slot].wait_recv()
        for move in following:
            move.start()
            moves.append(move)

    then(0, copy(out.at[behind, c, :, low], 3, up), copy(out.at[behind, c], 4, partner))
    then(1, copy(out.at[ahead, c, :, high], 5, down), copy(out.at[ahead, c], 6, partner))
    midway()
    then(3, copy(out.at[across, c, :, low], 7, partner))
    then(5, copy(out.at[across, c, :, high], 8, partner))
    for slot in (2, 4, 6, 7, 8):
        moves[slot].wait_recv()
    for move in moves:
        move.wait_send()


def reduce_scratch(share):
    return [
        pltpu.VMEM((2, 4, 2, share, HALF), BF16),
        pltpu.VMEM((2, 4, share, HALF), BF16),
        pltpu.VMEM((2, share, HALF), BF16),
        pltpu.VMEM((2, share, HALF), BF16),
        pltpu.VMEM((2, 2, share, HALF), BF16),
        pltpu.VMEM((2, 2, share, HALF), BF16),
        pltpu.SemaphoreType.DMA((8,)),
        pltpu.SemaphoreType.DMA((8,)),
    ]


def head_neighbours():
    _, y, c = seat()
    return [{"head": 2 * y + 1 - c}, {"head": 2 * plus(y, 1) + c}, {"head": 2 * plus(y, 3) + c}]


def store_terms(term, half, at, share, value):
    for block in range(8):
        rows = value[block * share : (block + 1) * share].astype(BF16)
        term[half, block // 2, block % 2, :, at : at + value.shape[1]] = rows


def layer_kernel(rows, heads, last, *refs):
    ringed = not last
    step_keys = KEY_BLOCKS[last]
    kv_ref, *refs = refs
    sources, up_ref, down_ref, out, refs = refs[:14], refs[14], refs[15], refs[16], refs[17:]
    if ringed:
        full_ref, *refs = refs
    places, refs = refs[:14], refs[14:]
    loads, landing, stream_ref, normed_ref, queries, acc, sums, attended, *refs = refs
    up, down, hidden, wloads, msend, mrecv, *refs = refs
    if ringed:
        *refs, shard, load, local, gsend, grecv = refs
        ring = RingGather(shard, full_ref, local, gsend, grecv)
        fetch = pltpu.make_async_copy(down_ref, shard, load)
        down_ref = full_ref
    *parts, send, recv = refs
    (
        x_ref, h_ref, n_ref, eq_ref, aq_ref, akv_ref, g_ref,
        win_ref, wo_ref, embedding_ref, gain_ref, last_gain_ref, wf_ref, ahead_ref,
    ) = places
    inputs = staged(zip(sources, places), loads)
    wide = up.shape[2]
    ups = [
        pltpu.make_async_copy(up_ref.at[:, pl.ds(k * wide, wide)], up.at[k], wloads.at[k])
        for k in range(up.shape[0])
    ]
    downs = [
        pltpu.make_async_copy(
            down_ref.at[pl.ds(k * 4, 4)], down.at[k], wloads.at[up.shape[0] + k]
        )
        for k in range(down.shape[0])
    ]
    term = parts[0]
    share = rows // 8
    width = heads * HEAD_DIM
    block = pl.program_id(0)
    me, y, c = seat()
    if last:
        mirror = lax.axis_size("seq") - 1 - me
        sends_edge = jnp.logical_and(mirror > 0, 2 * y + c == 7)
        keeps_edge = jnp.logical_and(mirror - 1 == me, 2 * y + c == 7)
        waits_edge = jnp.logical_and(mirror > 0, jnp.logical_not(keeps_edge))

    def scale_of(x, h, n):
        twice = jnp.concatenate([x, x], axis=1)
        quad = jnp.sum(x.astype(F32) * (dot(twice, g_ref[...]) + 2.0 * h), axis=1, keepdims=True)
        return twice, lax.rsqrt(jnp.maximum(quad + n, 0.0) * (1.0 / D) + EPSILON)

    @pl.when(block == 0)
    def _():
        if ringed:
            fetch.start()
        each("start", inputs)
        each("start", ups if ringed else ups + downs)
        if last:
            hail(head_neighbours() + [{"seq": mirror, "head": head} for head in range(8)])

            @pl.when(waits_edge)
            def _():
                hail([{"seq": mirror - 1, "head": 7}])
        else:
            hail_all(landing.shape[0])
            pl.semaphore_wait(pltpu.get_barrier_semaphore(), landing.shape[0])
            fetch.wait()
            ring.begin()
        each("wait", inputs[:7])
        own = pl.ds(pl.multiple_of(me * rows, rows), rows)
        twice, scale = scale_of(x_ref[own, :], h_ref[own, :], n_ref[own, :])
        value = (dot(twice, aq_ref[...]) + eq_ref[...]) * (scale * HEAD_DIM**-0.5)
        queries[...] = value.astype(BF16)
        acc[...] = jnp.zeros_like(acc)
        sums[...] = jnp.zeros_like(sums)

    def step(masked):
        here = pl.ds(pl.multiple_of(block * step_keys, step_keys), step_keys)
        twice, scale = scale_of(x_ref[here, :], h_ref[here, :], n_ref[here, :])
        both = ((dot(twice, akv_ref[...]) + kv_ref[...]) * scale).astype(BF16)
        keys, values = both[:, :width], both[:, width:]
        if masked:
            shape = (rows, step_keys)
            row = me * rows + lax.broadcasted_iota(jnp.int32, shape, 0)
            col = block * step_keys + lax.broadcasted_iota(jnp.int32, shape, 1)
            seen = col <= row
        for head in range(heads):
            cols = slice(head * HEAD_DIM, (head + 1) * HEAD_DIM)
            scores = dot_t(queries[:, cols], keys[:, cols])
            if masked:
                weights = jnp.where(seen, jnp.exp(jnp.where(seen, scores, 0.0)), 0.0)
            else:
                weights = jnp.exp(scores)
            part = weights[:, :HEAD_DIM]
            for at in range(HEAD_DIM, step_keys, HEAD_DIM):
                part = part + weights[:, at : at + HEAD_DIM]
            sums[:, cols] += part
            acc[:, cols] += dot(weights.astype(BF16), values[:, cols])

    final = (me * rows + rows - 1) // step_keys

    @pl.when(block < final)
    def _():
        step(False)

    @pl.when(block == final)
    def _():
        step(True)

    def produce(half, part):
        at = part * (HALF // 2)
        cols = slice(half * HALF + at, half * HALF + at + HALF // 2)
        store_terms(term, half, at, share, dot(attended[...], wo_ref[:, cols]))

    def meanwhile():
        first = pl.ds(pl.multiple_of(me * rows + (2 * y + c) * share, share), share)
        stream_ref[...] = dot(x_ref[first, :], win_ref[...]) + embedding_ref[...]

    def between():
        if ringed:
            ring.second()
            ring.middle()

    def midway():
        if ringed:
            ring.third(2)

    def produce_down(half, part):
        k = 2 * half + part
        downs[k].wait()
        weight = down[k].reshape(D // 4, hidden.shape[1])
        store_terms(term, half, part * (HALF // 2), share, dot_t(hidden[...], weight))

    @pl.when(block == pl.num_programs(0) - 1)
    def _():
        for head in range(heads):
            cols = slice(head * HEAD_DIM, (head + 1) * HEAD_DIM)
            total = jnp.sum(sums[:, cols], axis=1, keepdims=True)
            attended[:, cols] = (acc[:, cols] / total).astype(BF16)
        each("wait", inputs[7:])
        if ringed:
            ring.first()
        else:
            barrier = pltpu.get_barrier_semaphore()

            @pl.when(keeps_edge)
            def _():
                pl.semaphore_wait(barrier, 18)

            @pl.when(jnp.logical_and(sends_edge, jnp.logical_not(keeps_edge)))
            def _():
                pl.semaphore_wait(barrier, 19)

            @pl.when(jnp.logical_not(sends_edge))
            def _():
                pl.semaphore_wait(barrier, 11)

        total = reduce_over_head(produce, meanwhile, between, *parts)
        stream = stream_ref[...] + total
        stream_ref[...] = stream
        normed_ref[y, c] = layer_norm(stream, gain_ref[...]).astype(BF16)
        if ringed:
            ring.third(1)
        gather_over_head(normed_ref, send, recv, midway)
        if ringed:
            ring.third(3)
        for k in range(up.shape[0]):
            ups[k].wait()
            pre = dot(normed_ref[...].reshape(rows, D), up[k])
            hidden[:, k * wide : (k + 1) * wide] = jax.nn.gelu(pre, approximate=True).astype(BF16)
        if ringed:
            ring.arrive()
            each("start", downs)
        total = reduce_over_head(produce_down, lambda: None, lambda: None, *parts)
        normed = layer_norm(stream_ref[...] + total, last_gain_ref[...]).astype(BF16)
        params = dot(normed, wf_ref[...])
        following = ahead_ref[...] * jnp.exp(jnp.tanh(params[:, C:])) + params[:, :C]
        if last:
            finish(following, x_ref[0:16, :][0:1], landing, term, msend, mrecv)
            count = landing.shape[0] * share
            line = lax.broadcasted_iota(jnp.int32, (rows, count), 0)
            column = lax.broadcasted_iota(jnp.int32, (rows, count), 1)
            source = jnp.where(line == rows - 1, count - 1, rows - 2 - line)
            pick = jnp.where(column == source, 1.0, 0.0).astype(BF16)
            out[...] = dot(pick, landing[...].reshape(count, C)).astype(BF16)
        else:
            landing[me * 4 + y, c] = following.astype(BF16)
            begin, cross, end = spread(landing, msend, mrecv)
            begin()
            cross()
            before = x_ref[0:16, :].astype(F32)[0:1]
            chunk = 8 * 2 * share
            line = lax.broadcasted_iota(jnp.int32, (chunk, C), 0)
            for k in range(landing.shape[0] // 8):
                value = landing[8 * k : 8 * k + 8].reshape(chunk, C).astype(F32)
                moved = jnp.where(line == 0, before, pltpu.roll(value, 1, 0))
                out[k * chunk : (k + 1) * chunk, :] = moved.astype(BF16)
                before = value[chunk - 1 :]
            end()
            ring.flush()


def finish(following, top, out_ref, term, send, recv):
    seq, y, c = seat()
    mirror = lax.axis_size("seq") - 1 - seq
    sends_edge = jnp.logical_and(mirror > 0, 2 * y + c == 7)
    keeps_edge = jnp.logical_and(mirror - 1 == seq, 2 * y + c == 7)
    waits_edge = jnp.logical_and(mirror > 0, jnp.logical_not(keeps_edge))
    block = term.at[0, 0, 0, :, pl.ds(0, C)]
    block[...] = following.astype(BF16)
    head = 2 * y + c
    moves = [
        pltpu.make_async_remote_copy(
            src_ref=block, dst_ref=out_ref.at[head], send_sem=send.at[k], recv_sem=recv.at[0],
            device_id={"seq": mirror, "head": k}, device_id_type=MESH,
        )
        for k in range(8)
    ]
    edges = [
        pltpu.make_async_remote_copy(
            src_ref=block, dst_ref=out_ref.at[8], send_sem=send.at[8 + k], recv_sem=recv.at[1],
            device_id={"seq": mirror - 1, "head": k}, device_id_type=MESH,
        )
        for k in range(8)
    ]
    for move in moves:
        move.start()

    @pl.when(sends_edge)
    def _():
        for move in edges[:7]:
            move.start()

    @pl.when(jnp.logical_and(sends_edge, jnp.logical_not(keeps_edge)))
    def _():
        edges[7].start()

    whole = out_ref.at[pl.ds(0, 8)]
    pltpu.make_async_remote_copy(
        src_ref=whole, dst_ref=whole, send_sem=send.at[0], recv_sem=recv.at[0],
        device_id={"seq": mirror, "head": 0}, device_id_type=MESH,
    ).wait_recv()

    @pl.when(waits_edge)
    def _():
        pltpu.make_async_remote_copy(
            src_ref=block, dst_ref=out_ref.at[8], send_sem=send.at[0], recv_sem=recv.at[1],
            device_id={"seq": mirror - 1, "head": 7}, device_id_type=MESH,
        ).wait_recv()

    for move in moves:
        move.wait_send()

    @pl.when(sends_edge)
    def _():
        for move in edges[:7]:
            move.wait_send()

    @pl.when(jnp.logical_and(sends_edge, jnp.logical_not(keeps_edge)))
    def _():
        edges[7].wait_send()

    @pl.when(keeps_edge)
    def _():
        out_ref[8] = following.astype(BF16)

    @pl.when(mirror == 0)
    def _():
        out_ref[8] = jnp.broadcast_to(top.astype(F32), following.shape).astype(BF16)


def layer(rows, places, last, state, x, w_in, w_attn_out, embedding, gain, last_gain, w_final, ahead,
          up, down):
    kv = state[0]
    length, width = kv.shape[0], kv.shape[1] // 2
    step_keys = KEY_BLOCKS[last]
    share, hidden = rows // 8, up.shape[1]
    count = length // rows
    shard = (2, D // count // 2, hidden)
    far = pl.BlockSpec(memory_space=pltpu.HBM)
    tile = pl.BlockSpec((step_keys, 2 * width), lambda i: (i, 0))
    sources = [x, *state[1:], w_in, w_attn_out, embedding, gain, last_gain, w_final, ahead]
    shape = (9, share, C) if last else (places, 2, share, C)
    outs = [jax.ShapeDtypeStruct((rows, C), BF16) if last else jax.ShapeDtypeStruct((length, C), BF16)]
    if not last:
        outs.append(jax.ShapeDtypeStruct((count, *shard), BF16))
    return pl.pallas_call(
        functools.partial(layer_kernel, rows, width // HEAD_DIM, last),
        grid=(length // step_keys,),
        in_specs=[tile] + [far] * 16,
        out_specs=[pl.BlockSpec(memory_space=pltpu.VMEM)] + [far] * (not last),
        out_shape=outs,
        scratch_shapes=[buffer_like(source) for source in sources]
        + [
            pltpu.SemaphoreType.DMA((14,)),
            pltpu.VMEM(shape, BF16),
            pltpu.VMEM((share, D), F32),
            pltpu.VMEM((4, 2, share, D), BF16),
            pltpu.VMEM((rows, width), BF16),
            pltpu.VMEM((rows, width), F32),
            pltpu.VMEM((rows, width), F32),
            pltpu.VMEM((rows, width), BF16),
            pltpu.VMEM((3, D, hidden // 3), BF16),
            pltpu.VMEM((4, count // 4, *shard), BF16),
            pltpu.VMEM((rows, hidden), BF16),
            pltpu.SemaphoreType.DMA((7,)),
            pltpu.SemaphoreType.DMA((16,)),
            pltpu.SemaphoreType.DMA((2,)),
        ]
        + reduce_scratch(share)
        + [pltpu.SemaphoreType.DMA((9,)), pltpu.SemaphoreType.DMA((9,))]
        + ([] if last else [pltpu.VMEM(shard, BF16), pltpu.SemaphoreType.DMA] + ring_scratch()),
        compiler_params=pltpu.CompilerParams(
            collective_id=2 if last else 1, has_side_effects=True, vmem_limit_bytes=60 << 20,
        ),
        cost_estimate=pl.CostEstimate(
            flops=60_000_000_000, bytes_accessed=40_000_000, transcendentals=0
        ),
        name="layer_last" if last else "layer",
    )(kv, *sources, up, down)


def per_device(
    latent, w_in, w_query, w_key, w_value, w_attn_out, w_up, w_down, w_final,
    gain_attn, gain_mlp, gain_final,
):
    seq_count, head_count = lax.axis_size("seq"), lax.axis_size("head")
    rows = latent.shape[0]
    length = rows * seq_count
    places = seq_count * head_count // 2

    shape = (2, w_up.shape[0] // 2, w_up.shape[1])
    *state, gathered, ahead, embedding, up = first(
        rows, seq_count, places, latent, gain_attn[None, :], w_query, w_key, w_value, w_in,
        w_up.reshape(shape),
    )
    up = up.reshape(D, w_up.shape[1])
    x = gathered.reshape(length, C)
    down = w_down.T.reshape(shape)
    for step_index in range(ITERS):
        last = step_index == ITERS - 1
        x, *full = layer(
            rows, places, last, state, x, w_in, w_attn_out, embedding, gain_mlp[None, :],
            gain_final[None, :], w_final, ahead, up, down,
        )
        if not last:
            down = full[0]
    return x.astype(F32)


def solution(mesh):
    in_specs = (
        P("seq", None),
        P(),
        P(None, "head"),
        P(None, "head"),
        P(None, "head"),
        P("head", None),
        P("seq", "head"),
        P("head", "seq"),
        P(),
        P(),
        P(),
        P(),
    )
    return jax.shard_map(
        per_device, mesh=mesh, in_specs=in_specs, out_specs=P("seq", None), check_vma=False
    )
```
